16 devices in a mesh: dp: 16 (over z, y, x, core).
Axes of the slice: x: 2, y: 2, z: 2, core: 2. Of those that a mesh axis runs over, the one named last changes fastest.
Arguments:
- w_in0: float32 [1024, 512], replicated
- w_short: float32 [1024, 2048], replicated
- w_in: float32 [1, 2048, 512], replicated
- w_mid: float32 [2, 3, 3, 512, 512], replicated
- w_out: float32 [2, 512, 2048], replicated
- w_fc: float32 [2048, 1000], replicated
- w_bn: float32 [16384], replicated
- w_bias: float32 [1000], replicated
- g_in0: float32 [16, 1024, 512], P('dp')
- g_short: float32 [16, 1024, 2048], P('dp')
- g_in: float32 [16, 1, 2048, 512], P('dp')
- g_mid: float32 [16, 2, 3, 3, 512, 512], P('dp')
- g_out: float32 [16, 2, 512, 2048], P('dp')
- g_bn: float32 [16, 16384], P('dp')
- pooled: bfloat16 [16384, 2048], P('dp')
- dlogits: bfloat16 [16384, 1000], P('dp')
- v_in0: float32 [524288], P('dp')
- v_short: float32 [2097152], P('dp')
- v_in: float32 [1, 1048576], P(None, 'dp')
- v_mid: float32 [2, 2359296], P(None, 'dp')
- v_out: float32 [2, 1048576], P(None, 'dp')
- v_fc: float32 [2048000], P('dp')
- v_bn: float32 [16384], P('dp')
- v_bias: float32 [1008], P('dp')
- learn_rate: float32 [], replicated
Outputs:
- output 1: float32 [1024, 512], replicated
- output 2: float32 [1024, 2048], replicated
- output 3: float32 [1, 2048, 512], replicated
- output 4: float32 [2, 3, 3, 512, 512], replicated
- output 5: float32 [2, 512, 2048], replicated
- output 6: float32 [2048, 1000], replicated
- output 7: float32 [16384], replicated
- output 8: float32 [1000], replicated
- output 9: bfloat16 [1024, 512], replicated
- output 10: bfloat16 [1024, 2048], replicated
- output 11: bfloat16 [1, 2048, 512], replicated
- output 12: bfloat16 [2, 3, 3, 512, 512], replicated
- output 13: bfloat16 [2, 512, 2048], replicated
- output 14: bfloat16 [2048, 1000], replicated
- output 15: float32 [524288], P('dp')
- output 16: float32 [2097152], P('dp')
- output 17: float32 [1, 1048576], P(None, 'dp')
- output 18: float32 [2, 2359296], P(None, 'dp')
- output 19: float32 [2, 1048576], P(None, 'dp')
- output 20: float32 [2048000], P('dp')
- output 21: float32 [16384], P('dp')
- output 22: float32 [1008], P('dp')
All inputs are finite; a program needn't handle non-finite values.
Results may differ from the reference program's by a relative error of at most 0.001.
Values sent between devices are 32-bit elements.
A program may use at most 1 GiB of HBM per device.

```python
import math
import jax
import jax.numpy as jnp

C_IN = 1024
C_MID = 512
C_OUT = 2048
BLOCKS = 2
CLASSES = 1000
LOCAL_BATCH = 1024
DEVICES = 16
BN_LEN = 16384
BIAS_PAD = 1008

ROWS = DEVICES * LOCAL_BATCH
MOMENTUM = 0.9
TRUST_COEF = 0.001
DECAY = 0.0001


def draw_stack(key, count, shape, fan_in):
    keys = jax.random.split(key, 6)
    scale = fan_in ** -0.5
    ones = (1,) * len(shape)
    size = math.prod(shape)
    weight = scale * jax.random.normal(keys[0], (count,) + shape, jnp.float32)
    ratio = 1e-4 * 2.0 ** jax.random.uniform(keys[1], (1, count) + ones, jnp.float32, 0.0, 4.0)
    slope = jax.random.uniform(keys[5], (1, count) + ones, jnp.float32, 1.5, 3.0)
    place = (jnp.arange(size, dtype=jnp.float32) / size - 0.5).reshape((1, 1) + shape)
    ramp = 2.0 ** (slope * place)
    noise = jax.random.normal(keys[2], (DEVICES, count) + shape, jnp.float32)
    dev_mean = jax.random.normal(keys[3], (DEVICES, count) + ones, jnp.float32)
    gradient = scale * ratio * ramp * (math.sqrt(DEVICES) * noise + dev_mean)
    moment = 0.03 * scale * jax.random.normal(keys[4], (count, size), jnp.float32)
    return weight, gradient, moment


def setup_inputs(seed: int = 0) -> dict:
    keys = jax.random.split(jax.random.key(seed), 17)
    w_in0, g_in0, v_in0 = draw_stack(keys[0], 1, (C_IN, C_MID), C_IN)
    w_short, g_short, v_short = draw_stack(keys[1], 1, (C_IN, C_OUT), C_IN)
    w_in, g_in, v_in = draw_stack(keys[2], BLOCKS - 1, (C_OUT, C_MID), C_OUT)
    w_mid, g_mid, v_mid = draw_stack(keys[3], BLOCKS, (3, 3, C_MID, C_MID), 9 * C_MID)
    w_out, g_out, v_out = draw_stack(keys[4], BLOCKS, (C_MID, C_OUT), C_MID)
    fc_scale = C_OUT ** -0.5
    w_fc = fc_scale * jax.random.normal(keys[5], (C_OUT, CLASSES), jnp.float32)
    v_fc = 0.03 * fc_scale * jax.random.normal(keys[6], (C_OUT * CLASSES,), jnp.float32)
    pooled = jnp.abs(jax.random.normal(keys[7], (ROWS, C_OUT), jnp.float32))
    dev_shift = 0.2 * jax.random.normal(keys[8], (DEVICES, 1, CLASSES), jnp.float32)
    dlogits = 0.1 * (jax.random.normal(keys[9], (DEVICES, LOCAL_BATCH, CLASSES), jnp.float32) + dev_shift)
    bias_scale = 0.1 * (ROWS ** -0.5 + 0.2 * DEVICES ** -0.5)
    w_bias = 300.0 * bias_scale * jax.random.normal(keys[10], (CLASSES,), jnp.float32)
    v_bias = 20.0 * bias_scale * jax.random.normal(keys[11], (BIAS_PAD,), jnp.float32)
    w_bn = 0.5 + 0.5 * jax.random.normal(keys[12], (BN_LEN,), jnp.float32)
    bn_noise = jax.random.normal(keys[13], (DEVICES, BN_LEN), jnp.float32)
    bn_shift = jax.random.normal(keys[14], (DEVICES, 1), jnp.float32)
    g_bn = 0.001 * (math.sqrt(DEVICES) * bn_noise + bn_shift)
    v_bn = 0.03 * jax.random.normal(keys[15], (BN_LEN,), jnp.float32)
    learn_rate = jax.random.uniform(keys[16], (), jnp.float32, 10.0, 30.0)
    return {
        'w_in0': w_in0[0], 'w_short': w_short[0], 'w_in': w_in, 'w_mid': w_mid, 'w_out': w_out,
        'w_fc': w_fc, 'w_bn': w_bn, 'w_bias': w_bias,
        'g_in0': g_in0[:, 0], 'g_short': g_short[:, 0], 'g_in': g_in, 'g_mid': g_mid, 'g_out': g_out,
        'g_bn': g_bn,
        'pooled': pooled.astype(jnp.bfloat16),
        'dlogits': dlogits.reshape(ROWS, CLASSES).astype(jnp.bfloat16),
        'v_in0': v_in0[0], 'v_short': v_short[0], 'v_in': v_in, 'v_mid': v_mid, 'v_out': v_out,
        'v_fc': v_fc, 'v_bn': v_bn, 'v_bias': v_bias,
        'learn_rate': learn_rate,
    }


def lars_step(weight, gradient, moment, learn_rate):
    count = moment.shape[0]
    w_flat = weight.reshape(count, -1)
    g_flat = gradient.reshape(count, -1)
    w_norm = jnp.sqrt(jnp.sum(w_flat * w_flat, axis=1, keepdims=True))
    g_norm = jnp.sqrt(jnp.sum(g_flat * g_flat, axis=1, keepdims=True))
    trust = jnp.where((w_norm > 0) & (g_norm > 0), TRUST_COEF * w_norm / (g_norm + DECAY * w_norm), 1.0)
    moment_new = MOMENTUM * moment + learn_rate * trust * (g_flat + DECAY * w_flat)
    return (w_flat - moment_new).reshape(weight.shape), moment_new


def reference(w_in0, w_short, w_in, w_mid, w_out, w_fc, w_bn, w_bias,
              g_in0, g_short, g_in, g_mid, g_out, g_bn, pooled, dlogits,
              v_in0, v_short, v_in, v_mid, v_out, v_fc, v_bn, v_bias, learn_rate):
    fc_grad = jnp.dot(pooled.T, dlogits, preferred_element_type=jnp.float32) / ROWS
    bias_grad = jnp.sum(dlogits.astype(jnp.float32), axis=0) / ROWS
    kernels = [
        (w_in0, jnp.mean(g_in0, axis=0), v_in0),
        (w_short, jnp.mean(g_short, axis=0), v_short),
        (w_in, jnp.mean(g_in, axis=0), v_in),
        (w_mid, jnp.mean(g_mid, axis=0), v_mid),
        (w_out, jnp.mean(g_out, axis=0), v_out),
        (w_fc, fc_grad, v_fc),
    ]
    new_w = []
    new_v = []
    for weight, gradient, moment in kernels:
        w_next, moment_next = lars_step(weight, gradient, moment.reshape(-1, moment.shape[-1]), learn_rate)
        new_w.append(w_next)
        new_v.append(moment_next.reshape(moment.shape))
    bn_moment = MOMENTUM * v_bn + learn_rate * jnp.mean(g_bn, axis=0)
    bias_moment = MOMENTUM * v_bias + learn_rate * jnp.pad(bias_grad, (0, BIAS_PAD - CLASSES))
    w_bn_new = w_bn - bn_moment
    w_bias_new = w_bias - bias_moment[:CLASSES]
    return (new_w[0], new_w[1], new_w[2], new_w[3], new_w[4], new_w[5], w_bn_new, w_bias_new,
            new_w[0].astype(jnp.bfloat16), new_w[1].astype(jnp.bfloat16), new_w[2].astype(jnp.bfloat16),
            new_w[3].astype(jnp.bfloat16), new_w[4].astype(jnp.bfloat16), new_w[5].astype(jnp.bfloat16),
            new_v[0], new_v[1], new_v[2], new_v[3], new_v[4], new_v[5], bn_moment, bias_moment)
```

```python
import functools
import jax
import jax.numpy as jnp
from jax import lax
from jax.experimental import pallas as pl
from jax.experimental.pallas import tpu as pltpu
from jax.sharding import PartitionSpec as P

MOMENTUM = 0.9
TRUST_COEF = 0.001
DECAY = 0.0001

MESH = pl.DeviceIdType.MESH
F32 = jnp.float32
DEV = 16
U = 32
CW = 512
NCH = 48
NSLOT = 12
FC0 = 40
STARTS = (0, 9, 18, 26, 30, 34, 38, 40)
MID, SHORT, OUT = (2, DEV, 288, CW), (DEV, 64, 2048), (2, DEV, U, 2048)
INN, IN0 = (DEV, 128, CW), (DEV, 64, CW)
LANES = 128
SPLIT = 34
L1, L2, L3, L4 = 2, 5, 8, 10
AG0 = 48
M0, M1, M2, M3, M4 = 1, 3, 6, 10, 14
NSEND = 16


def tensor_of(c):
    t = 0
    for first in STARTS[1:]:
        t = t + jnp.where(c >= first, 1, 0)
    return t


def chunk_views(c, refs, fn):
    mid, short, out, inn, in0, fc = refs

    def rows(x):
        return pl.ds(pl.multiple_of(x * U, U), U)

    def cols(x):
        return pl.ds(pl.multiple_of(x * CW, CW), CW)

    def whole(ref):
        return [(ref, lambda dst: dst)]

    def strip(i):
        return lambda dst: dst.at[:, pl.ds(128 * i, 128)]

    @pl.when(c < 18)
    def _():
        fn(lambda p: whole(mid.at[c // 9, p, rows(c % 9), :]))

    @pl.when((c >= 18) & (c < 26))
    def _():
        fn(lambda p: whole(short.at[p, rows((c - 18) // 4), cols((c - 18) % 4)]))

    @pl.when((c >= 26) & (c < 34))
    def _():
        fn(lambda p: whole(out.at[(c - 26) // 4, p, :, cols((c - 26) % 4)]))

    @pl.when((c >= 34) & (c < 38))
    def _():
        fn(lambda p: whole(inn.at[p, rows(c - 34), :]))

    @pl.when((c >= 38) & (c < 40))
    def _():
        fn(lambda p: whole(in0.at[p, rows(c - 38), :]))

    if fc is not None:
        @pl.when(c >= FC0)
        def _():
            fn(lambda p: [(fc.at[rows(4 * (c - FC0) + i), pl.ds(pl.multiple_of(p * 128, 128), 128)], strip(i))
                          for i in range(4)])


def comm_kernel(lr_ref, gm, gs, go, gi, g0, gf, wm, ws, wo, wi, w0, wf, vm, vs, vo, vi, v0, vf,
                small_g, small_w, small_v,
                o_ref, vn_ref, so_ref, sv_ref,
                acc, rd, r1, r2, r3, grad, wbuf, vbuf, wnew, vnew, sums, nb, tr, sb, snew, svnew,
                load_sem, ds_sem, dr_sem, s1_sem, p1_sem, s2_sem, p2_sem, s3_sem, p3_sem,
                w_sem, v_sem, sm_send, sm_recv, so_send, so_recv, nb_send, nb_recv, loc_sem, vn_sem, misc_sem,
                a1_sem, a2_sem, a3_sem, ad_sem, as_sem,
                cd_sem, c1_sem, c2_sem, c3_sem):
    me = lax.axis_index('dp')
    core = me % 2
    chip = me // 2
    partner = me + 1 - 2 * core

    send_sems = (ds_sem, s1_sem, s2_sem, s3_sem)
    recv_sems = (dr_sem, p1_sem, p2_sem, p3_sem)
    ag_sems = (a1_sem, a2_sem, a3_sem)
    credits = (None, c1_sem, c2_sem, c3_sem)

    def order(c):
        steps = []
        for i in range(3):
            d = (c + i) % 3
            weight = 1 + d + (d * (d - 1)) // 2
            steps.append(weight * (1 - 2 * ((chip // weight) % 2)))
        return steps

    def remote(src, dst, send, recv, dev):
        return pltpu.make_async_remote_copy(src_ref=src, dst_ref=dst, send_sem=send, recv_sem=recv,
                                            device_id=(dev,), device_id_type=MESH)

    def local(src, dst, sem):
        return pltpu.make_async_copy(src, dst, sem)

    def units(n):
        return o_ref.at[0, pl.ds(0, n)]

    def drain(n, sem):
        local(units(n), units(n), sem).wait()

    def signal(sem, dev):
        pl.semaphore_signal(sem, inc=1, device_id=(dev,), device_id_type=MESH)

    barrier = pltpu.get_barrier_semaphore()

    def ring(d, _):
        signal(barrier, (me + d) % DEV)
        return 0
    lax.fori_loop(1, DEV, ring, 0)
    pl.semaphore_wait(barrier, DEV - 1)

    def small_out(d, _):
        dev = (me + d) % DEV
        remote(small_g.at[dev], sb.at[me], sm_send, sm_recv, dev).start()
        return 0

    def load_state(c, _):
        def weight(view):
            for src, part in view(me):
                local(src, part(wbuf.at[c]), w_sem).start()

        def moment(view):
            for src, part in view(0):
                local(src, part(vbuf.at[c]), v_sem).start()
        chunk_views(c, (wm, ws, wo, wi, w0, None), weight)
        chunk_views(c, (vm, vs, vo, vi, v0, vf), moment)
        return 0

    def fc_weights():
        lane = pl.ds(pl.multiple_of(me * 128, 128), 128)
        for b in range(31):
            local(wf.at[pl.ds(b * U, U), lane], wbuf.at[FC0 + b // 4, :, pl.ds(b % 4 * 128, 128)], w_sem).start()
        local(wf.at[pl.ds(992, 8), lane], wbuf.at[NCH - 1, pl.ds(0, 8), pl.ds(384, 128)], w_sem).start()
        wbuf[NCH - 1, 8:32, 384:512] = jnp.zeros((24, 128), F32)

    def weights_wait():
        first = pl.ds(0, NCH - 1)
        local(wbuf.at[first], wbuf.at[first], w_sem).wait()
        for part in (wbuf.at[NCH - 1, :, pl.ds(0, 384)], wbuf.at[NCH - 1, pl.ds(0, 8), pl.ds(384, 128)]):
            local(part, part, w_sem).wait()

    def sent(slot):
        for level in range(4):
            drain(8 >> level, send_sems[level].at[slot])

    def rs_start(c):
        slot = c % NSLOT

        @pl.when(c >= NSLOT)
        def _():
            sent(slot)
            pl.semaphore_wait(cd_sem, 1)
        x1, x2, x3 = order(c)
        chips = [chip + (q // 4) * x1 + ((q // 2) % 2) * x2 + (q % 2) * x3 for q in range(8)]

        def go_all(view):
            for q in (4, 5, 6, 7, 0, 1, 2, 3):
                for src, part in view(2 * chips[q] + 1 - core):
                    remote(src, part(rd.at[slot, q]), ds_sem.at[slot], dr_sem.at[slot], partner).start()
                for src, part in view(2 * chips[q] + core):
                    local(src, part(acc.at[slot, q]), load_sem.at[slot]).start()
        chunk_views(c, (gm, gs, go, gi, g0, gf), go_all)

    def rs_fold(c, level):
        slot, half = c % NSLOT, 4 >> level
        came, going = (rd, r1, r2, r3)[level:level + 2]
        dev = 2 * (chip + order(c)[level]) + core
        if level == 0:
            drain(8, load_sem.at[slot])
        drain(2 * half, recv_sems[level].at[slot])
        acc[slot, half:2 * half] = acc[slot, half:2 * half] + came[slot, half:2 * half]

        @pl.when(c >= NSLOT)
        def _():
            pl.semaphore_wait(credits[level + 1].at[c % 3], 1)
        remote(acc.at[slot, pl.ds(half, half)], going.at[slot], send_sems[level + 1].at[slot],
               recv_sems[level + 1].at[slot], dev).start()
        acc[slot, 0:half] = acc[slot, 0:half] + came[slot, 0:half]
        give_credit(c, level)

    def give_credit(c, level):
        @pl.when(c + NSLOT < NCH)
        def _():
            if level == 0:
                signal(cd_sem, partner)
            else:
                signal(credits[level].at[c % 3], 2 * (chip + order(c)[level - 1]) + core)

    def fold(x):
        y = jnp.sum(x * x, axis=0, keepdims=True)
        return sum(y[:, i:i + LANES] for i in range(0, CW, LANES))

    def rs_end(c):
        slot = c % NSLOT
        drain(1, p3_sem.at[slot])
        scale = jnp.where(c >= FC0, 1.0 / 16384.0, 1.0 / 16.0).astype(F32)
        g = (acc[slot, 0] + r3[slot, 0]) * scale
        grad[c] = g
        t = tensor_of(c)
        sums[pl.ds(t, 1), :] = sums[pl.ds(t, 1), :] + fold(g)
        give_credit(c, 3)

    def weight_sums(c, _):
        t = tensor_of(c)
        sums[pl.ds(8 + t, 1), :] = sums[pl.ds(8 + t, 1), :] + fold(wbuf[c])
        return 0

    def norms_out(n):
        nb[n, me] = sums[...]

        def send(d, _):
            dev = (me + d) % DEV
            remote(nb.at[n, me], nb.at[n, me], nb_send.at[n], nb_recv.at[n], dev).start()
            return 0
        lax.fori_loop(1, DEV, send, 0)

    def norms_in(n):
        local(nb.at[n, pl.ds(0, DEV - 1)], nb.at[n, pl.ds(0, DEV - 1)], nb_recv.at[n]).wait()
        local(nb.at[n, pl.ds(0, DEV - 1)], nb.at[n, pl.ds(0, DEV - 1)], nb_send.at[n]).wait()
        total = jnp.sum(nb[n], axis=0)
        norm = jnp.sqrt(jnp.broadcast_to(jnp.sum(total, axis=1, keepdims=True), (16, 128)))
        g_norm, w_norm = norm[0:8], norm[8:16]
        ratio = jnp.where((w_norm > 0) & (g_norm > 0), TRUST_COEF * w_norm / (g_norm + DECAY * w_norm), 1.0)
        tr[...] = lr_ref[0, 0] * ratio

    def update(a):
        rate = tr[pl.ds(tensor_of(a), 1), :]
        for i in range(4):
            s = slice(128 * i, 128 * i + 128)
            w = wbuf[a, :, s]
            v = MOMENTUM * vbuf[a, :, s] + rate * (grad[a, :, s] + DECAY * w)
            vnew[a, :, s] = v
            wnew[a, :, s] = w - v

    def ag_send(src, a, p, recv, dev):
        remote(src, o_ref.at[a, p], as_sem.at[a % NSEND], recv.at[a], dev).start()

    def ids(a):
        x1, x2, x3 = order(a)
        return [me + 2 * ((q % 2) * x1 + ((q // 2) % 2) * x2 + (q // 4) * x3) for q in range(8)]

    def ag_pass(a, n):
        e = ids(a)
        level = n.bit_length() - 1
        held = [wnew.at[a]] + [o_ref.at[a, p] for p in e[1:n]]
        if n > 1:
            drain(n // 2, ag_sems[level - 1].at[a])
        if n < 8:
            for q in range(n):
                ag_send(held[q], a, e[q], ag_sems[level], e[n])
        for q in range(n // 2, n):
            ag_send(held[q], a, e[q], ad_sem, partner)

    def ag_first(a):
        @pl.when(a >= NSEND)
        def _():
            drain(15, as_sem.at[a % NSEND])
        ag_pass(a, 1)
        local(wnew.at[a], o_ref.at[a, me], loc_sem).start()
        local(vnew.at[a], vn_ref.at[a], vn_sem).start()

    def ag_end(a):
        drain(8, ad_sem.at[a])

    def stage(s, lag, fn):
        c = s - lag

        @pl.when((c >= 0) & (c < NCH))
        def _():
            fn(c)

    def rs_rest(s):
        stage(s, L4, rs_end)
        for level, lag in ((2, L3), (1, L2), (0, L1)):
            stage(s, lag, functools.partial(rs_fold, level=level))

    def rs_step(s, _):
        rs_rest(s)
        stage(s, 0, rs_start)
        return 0

    def ag_step(s):
        stage(s, AG0 + M4, ag_end)
        for n, lag in ((8, M3), (4, M2), (2, M1)):
            stage(s, AG0 + lag, functools.partial(ag_pass, n=n))
        stage(s, AG0 + M0, ag_first)
        stage(s, AG0, update)

    def both_step(s, _):
        rs_rest(s)
        ag_step(s)
        return 0

    def last_step(s, _):
        ag_step(s)
        return 0

    lax.fori_loop(0, 2, rs_step, 0)
    lax.fori_loop(1, DEV, small_out, 0)
    sums[...] = jnp.zeros_like(sums)
    own = local(small_g.at[me], sb.at[me], misc_sem)
    own.start()
    lax.fori_loop(0, NCH, load_state, 0)
    fc_weights()
    lax.fori_loop(2, 10, rs_step, 0)

    own.wait()
    local(sb.at[pl.ds(0, DEV - 1)], sb.at[pl.ds(0, DEV - 1)], sm_recv).wait()
    local(sb.at[pl.ds(0, DEV - 1)], sb.at[pl.ds(0, DEV - 1)], sm_send).wait()
    row = lax.broadcasted_iota(jnp.int32, (16, 128), 0)
    small = jnp.sum(sb[...], axis=0) * jnp.where(row < 8, 1.0 / 16.0, 1.0 / 16384.0)
    sv = MOMENTUM * small_v[...] + lr_ref[0, 0] * small
    svnew[...] = sv
    snew[...] = small_w[...] - sv

    lax.fori_loop(10, 14, rs_step, 0)

    def small_back(d, _):
        dev = (me + d) % DEV
        remote(snew, so_ref.at[me], so_send, so_recv, dev).start()
        return 0
    lax.fori_loop(1, DEV, small_back, 0)
    own_s = local(snew, so_ref.at[me], misc_sem)
    own_s.start()
    own_v = local(svnew, sv_ref, w_sem)

    weights_wait()
    local(vbuf, vbuf, v_sem).wait()
    own_v.start()
    lax.fori_loop(0, NCH, weight_sums, 0)

    lax.fori_loop(14, SPLIT + L4, rs_step, 0)
    norms_out(0)
    lax.fori_loop(SPLIT + L4, AG0, rs_step, 0)
    norms_in(0)
    lax.fori_loop(AG0, NCH + L4, both_step, 0)
    norms_out(1)
    lax.fori_loop(NCH + L4, NCH + L4 + 4, last_step, 0)
    norms_in(1)
    lax.fori_loop(NCH + L4 + 4, AG0 + M4 + NCH, last_step, 0)

    def rest(c, _):
        sent(c % NSLOT)
        return 0
    lax.fori_loop(NCH - NSLOT, NCH, rest, 0)

    def rest_ag(a, _):
        drain(15, as_sem.at[a % NSEND])
        return 0
    lax.fori_loop(NCH - NSEND, NCH, rest_ag, 0)
    own_s.wait()
    own_v.wait()
    local(so_ref.at[pl.ds(0, DEV - 1)], so_ref.at[pl.ds(0, DEV - 1)], so_recv).wait()
    local(so_ref.at[pl.ds(0, DEV - 1)], so_ref.at[pl.ds(0, DEV - 1)], so_send).wait()
    local(wnew, wnew, loc_sem).wait()
    local(vnew, vn_ref, vn_sem).wait()


def run_comm(lr, grads, weights, moments, small_g, small_w, small_v):
    unit = (U, CW)
    anyspec = pl.BlockSpec(memory_space=pl.ANY)
    vspec = pl.BlockSpec(memory_space=pltpu.VMEM)
    dma = pltpu.SemaphoreType.DMA
    reg = pltpu.SemaphoreType.REGULAR
    slots = [dma((NSLOT,))] * 9
    return pl.pallas_call(
        comm_kernel,
        out_shape=[jax.ShapeDtypeStruct((NCH, DEV) + unit, F32), jax.ShapeDtypeStruct((NCH,) + unit, F32),
                   jax.ShapeDtypeStruct((DEV, 16, 128), F32), jax.ShapeDtypeStruct((16, 128), F32)],
        in_specs=[pl.BlockSpec(memory_space=pltpu.SMEM)] + [anyspec] * 19 + [vspec] * 2,
        out_specs=[anyspec] * 4,
        scratch_shapes=[
            pltpu.VMEM((NSLOT, 8) + unit, F32), pltpu.VMEM((NSLOT, 8) + unit, F32),
            pltpu.VMEM((NSLOT, 4) + unit, F32), pltpu.VMEM((NSLOT, 2) + unit, F32),
            pltpu.VMEM((NSLOT, 1) + unit, F32)]
        + [pltpu.VMEM((NCH,) + unit, F32)] * 5
        + [pltpu.VMEM((16, 128), F32), pltpu.VMEM((2, DEV, 16, 128), F32), pltpu.VMEM((8, 128), F32),
           pltpu.VMEM((DEV, 16, 128), F32), pltpu.VMEM((16, 128), F32), pltpu.VMEM((16, 128), F32)]
        + slots
        + [dma, dma, dma, dma, dma, dma, dma((2,)), dma((2,)), dma, dma, dma]
        + [dma((NCH,))] * 4 + [dma((NSEND,))]
        + [reg, reg((3,)), reg((3,)), reg((3,))],
        compiler_params=pltpu.CompilerParams(collective_id=0, has_side_effects=True,
                                             vmem_limit_bytes=56 * 1024 * 1024),
        name='lars_comm',
    )(lr, *grads, *weights, *moments, small_g, small_w, small_v)


NBUF = 6
AHEAD = 3


def write_kernel(o_ref, om, os_, oo, oi, o0, of, bm, bs, bo, bi, b0, bf,
                 buf, bbuf, fbuf, fbbuf, in_sem, f_sem, b_sem):
    def view(c, refs):
        m, s, o, i, z = refs
        if c < 18:
            return m.at[c // 9, :, pl.ds(c % 9 * U, U), :]
        if c < 26:
            return s.at[:, pl.ds((c - 18) // 4 * U, U), pl.ds((c - 18) % 4 * CW, CW)]
        if c < 34:
            return o.at[(c - 26) // 4, :, :, pl.ds((c - 26) % 4 * CW, CW)]
        if c < 38:
            return i.at[:, pl.ds((c - 34) * U, U), :]
        return z.at[:, pl.ds((c - 38) * U, U), :]

    def load(i):
        return [pltpu.make_async_copy(o_ref.at[i], buf.at[i % NBUF], in_sem.at[i % NBUF])]

    def stores(i):
        slot = i % NBUF
        if i < FC0:
            pairs = [(buf.at[slot], view(i, (om, os_, oo, oi, o0))), (bbuf.at[slot], view(i, (bm, bs, bo, bi, b0)))]
        else:
            size = 128 if i < NCH - 1 else 104
            have, want = pl.ds(0, size), pl.ds(128 * (i - FC0), size)
            pairs = [(fbuf.at[i % 4, have], of.at[want]), (fbbuf.at[i % 4, have], bf.at[want])]
        return [pltpu.make_async_copy(*pairs[0], f_sem.at[slot]), pltpu.make_async_copy(*pairs[1], b_sem.at[slot])]

    for i in range(AHEAD):
        for d in load(i):
            d.start()
    waited = 0
    for i in range(NCH):
        slot = i % NBUF
        for d in load(i):
            d.wait()
        if i < FC0:
            def cast(p, _):
                bbuf[slot, p] = buf[slot, p].astype(jnp.bfloat16)
                return 0
            lax.fori_loop(0, DEV, cast, 0)
        else:
            while waited <= i - 4:
                for d in stores(waited):
                    d.wait()
                waited += 1
            for p in range(DEV):
                for r in range(4):
                    x = buf[slot, p, :, 128 * r:128 * r + 128]
                    fbuf[i % 4, U * r:U * r + U, 128 * p:128 * p + 128] = x
                    fbbuf[i % 4, U * r:U * r + U, 128 * p:128 * p + 128] = x.astype(jnp.bfloat16)
        for d in stores(i):
            d.start()
        nxt = i + AHEAD
        if nxt < NCH:
            while waited <= nxt - NBUF:
                for d in stores(waited):
                    d.wait()
                waited += 1
            for d in load(nxt):
                d.start()
    while waited < NCH:
        for d in stores(waited):
            d.wait()
        waited += 1


def run_write(o):
    anyspec = pl.BlockSpec(memory_space=pl.ANY)
    shapes = [MID, SHORT, OUT, INN, IN0, (1000, 2048)]
    dma = pltpu.SemaphoreType.DMA
    return pl.pallas_call(
        write_kernel,
        out_shape=[jax.ShapeDtypeStruct(s, F32) for s in shapes]
        + [jax.ShapeDtypeStruct(s, jnp.bfloat16) for s in shapes],
        in_specs=[anyspec],
        out_specs=[anyspec] * 12,
        scratch_shapes=[
            pltpu.VMEM((NBUF, DEV, U, CW), F32), pltpu.VMEM((NBUF, DEV, U, CW), jnp.bfloat16),
            pltpu.VMEM((4, 128, 2048), F32), pltpu.VMEM((4, 128, 2048), jnp.bfloat16),
            dma((NBUF,)), dma((NBUF,)), dma((NBUF,))],
        compiler_params=pltpu.CompilerParams(vmem_limit_bytes=48 * 1024 * 1024),
        name='write_out',
    )(o)


def solution(mesh):
    n_dev = mesh.shape['dp']
    assert n_dev == DEV
    full, lead, cols = P(), P('dp'), P(None, 'dp')
    moment_specs = (lead, lead, cols, cols, cols, lead, lead, lead)
    in_specs = (full,) * 8 + (lead,) * 8 + moment_specs + (full,)
    out_specs = (full,) * 14 + moment_specs

    def body(w_in0, w_short, w_in, w_mid, w_out, w_fc, w_bn, w_bias,
             g_in0, g_short, g_in, g_mid, g_out, g_bn, pooled, dlogits,
             v_in0, v_short, v_in, v_mid, v_out, v_fc, v_bn, v_bias, learn_rate):
        rank = lax.axis_index('dp')
        fc_local = lax.dot_general(jnp.pad(dlogits, ((0, 0), (0, 24))), pooled, (((0,), (0,)), ((), ())),
                                   preferred_element_type=F32)
        bias_local = jnp.sum(dlogits, axis=0, dtype=F32)
        grads = (g_mid.reshape(MID), g_short.reshape(SHORT), g_out.reshape(OUT), g_in.reshape(INN),
                 g_in0.reshape(IN0), fc_local)
        weights = (w_mid.reshape(MID), w_short.reshape(SHORT), w_out.reshape(OUT), w_in.reshape(INN),
                   w_in0.reshape(IN0), w_fc.T)

        def own(x, shape):
            return x.reshape([1 if n == DEV else n for n in shape])
        moments = (own(v_mid, MID), own(v_short, SHORT), own(v_out, OUT), own(v_in, INN), own(v_in0, IN0),
                   jnp.pad(v_fc.reshape(LANES, 1000).T, ((0, 24), (0, 0))))

        def pad_bias(x):
            return jnp.pad(x, ((0, 0), (0, 65)))[:, None, :]
        small_g = jnp.concatenate([g_bn.reshape(DEV, 8, 128),
                                   jnp.pad(pad_bias(jnp.pad(bias_local, (0, 8)).reshape(DEV, 63)),
                                           ((0, 0), (0, 7), (0, 0)))], axis=1)

        def own_small(bn, bias):
            return jnp.concatenate([bn.reshape(8, 128), jnp.pad(bias.reshape(1, 63), ((0, 7), (0, 65)))], axis=0)
        small_w = own_small(lax.dynamic_slice_in_dim(w_bn, rank * 1024, 1024),
                            lax.dynamic_slice_in_dim(jnp.pad(w_bias, (0, 8)), rank * 63, 63))
        small_v = own_small(v_bn, v_bias)
        o, vn, so, sv = run_comm(learn_rate.reshape(1, 1), grads, weights, moments, small_g, small_w, small_v)
        f = run_write(o)
        mid, short, out, inn, in0, fc, mid_b, short_b, out_b, inn_b, in0_b, fc_b = f

        def wide(x, rows):
            return x.reshape(rows, 4, U, CW).transpose(0, 2, 1, 3)
        vn_fc = vn[40:48].reshape(8, U, 4, 128).transpose(0, 2, 1, 3).reshape(1024, 128)[:1000].T
        return (in0.reshape(w_in0.shape), short.reshape(w_short.shape), inn.reshape(w_in.shape),
                mid.reshape(w_mid.shape), out.reshape(w_out.shape), fc.T,
                so[:, :8].reshape(-1), so[:, 8, :63].reshape(-1)[:1000],
                in0_b.reshape(w_in0.shape), short_b.reshape(w_short.shape), inn_b.reshape(w_in.shape),
                mid_b.reshape(w_mid.shape), out_b.reshape(w_out.shape), fc_b.T,
                vn[38:40].reshape(v_in0.shape), wide(vn[18:26], 2).reshape(v_short.shape),
                vn[34:38].reshape(v_in.shape), vn[0:18].reshape(v_mid.shape),
                wide(vn[26:34], 2).reshape(v_out.shape), vn_fc.reshape(v_fc.shape),
                sv[:8].reshape(-1), sv[8, :63])

    return jax.shard_map(body, mesh=mesh, in_specs=in_specs, out_specs=out_specs, check_vma=False)
```

```python
import functools
import jax
import jax.numpy as jnp
from jax import lax
from jax.experimental import pallas as pl
from jax.experimental.pallas import tpu as pltpu
from jax.sharding import PartitionSpec as P

MOMENTUM = 0.9
TRUST_COEF = 0.001
DECAY = 0.0001

MESH = pl.DeviceIdType.MESH
F32, BF16 = jnp.float32, jnp.bfloat16
DEV = 16
LANES = 128
U, CW = 32, 512
NCH = 48
FC0 = 40
CLASSES, LASTROW = 1000, 992
SUB = 8
TABLE = ((0, 2, 9, 1), (18, 1, 8, 4), (26, 2, 4, 4), (34, 1, 4, 1), (38, 1, 2, 1))
STARTS = (9, 18, 26, 30, 34, 38, FC0)
SPLIT = 26
NSLOT = 15
LAGS = (2, 6, 10, 13)
AG0 = 43
FIRST = 1
AGLAGS = ((2, 5), (4, 10), (8, 16))
AGEND = 20
NSEND = 18
MM0 = 5
SMALL = 16


def tensor_of(c):
    return sum(jnp.where(c >= first, 1, 0) for first in STARTS)


def dshape(first, stack, per, blocks, lead):
    return (stack, lead, per // blocks * U, blocks * CW)


def unit_at(entry, c):
    first, _, per, blocks = entry
    k = (c - first) % per
    return (c - first) // per, k // blocks * U, k % blocks * CW


def aligned(x, size):
    return pl.ds(x if isinstance(x, int) else pl.multiple_of(x, size), size)


def chunk_views(c, refs, fn):
    for entry, ref in zip(TABLE, refs):
        first, stack, per, _ = entry

        @pl.when((c >= first) & (c < first + stack * per))
        def _():
            i, row, col = unit_at(entry, c)
            fn(lambda p: ref.at[i, p, aligned(row, U), aligned(col, CW)])


def comm_kernel(lr_ref, gm, gs, go, gi, g0, x_ref, d_ref, wm, ws, wo, wi, w0, wf, vm, vs, vo, vi, v0, vf,
                g_bn, w_bn, v_bn, w_bias, v_bias,
                o_ref, nm, ns, no, ni, n0, nf, so_ref, sv_ref,
                acc, rd, r1, r2, r3, grad, wbuf, vbuf, xbuf, dbuf, fcg,
                sums, nb, tr, sb, bias, snew, svnew,
                load_sem, ds_sem, dr_sem, s1_sem, p1_sem, s2_sem, p2_sem, s3_sem, p3_sem,
                w_sem, v_sem, x_sem, sm_send, sm_recv, so_send, so_recv, loc_sem, vn_sem, misc_sem,
                nb_send, nb_recv, a1_sem, a2_sem, a3_sem, ad_sem, as_sem,
                cd_sem, c1_sem, c2_sem, c3_sem):
    me = lax.axis_index('dp')
    core = me % 2
    chip = me // 2
    partner = me + 1 - 2 * core
    send_sems = (ds_sem, s1_sem, s2_sem, s3_sem)
    recv_sems = (dr_sem, p1_sem, p2_sem, p3_sem)
    ag_sems = (a1_sem, a2_sem, a3_sem)
    credits = (None, c1_sem, c2_sem, c3_sem)
    others = pl.ds(0, DEV - 1)

    def order(c):
        steps = []
        for i in range(3):
            d = (c + i) % 3
            weight = 1 + d + (d * (d - 1)) // 2
            steps.append(weight * (1 - 2 * ((chip // weight) % 2)))
        return steps

    def remote(src, dst, send, recv, dev):
        return pltpu.make_async_remote_copy(src_ref=src, dst_ref=dst, send_sem=send, recv_sem=recv,
                                            device_id=(dev,), device_id_type=MESH)

    def local(src, dst, sem):
        return pltpu.make_async_copy(src, dst, sem)

    def landed(ref, sem):
        local(ref, ref, sem).wait()

    def drain(n, sem):
        landed(o_ref.at[0, pl.ds(0, n)], sem)

    def signal(sem, dev):
        pl.semaphore_signal(sem, inc=1, device_id=(dev,), device_id_type=MESH)

    def loop(lo, hi, fn):
        def body(i, carry):
            fn(i)
            return carry
        lax.fori_loop(lo, hi, body, 0)

    def each_other(fn):
        loop(1, DEV, lambda d: fn((me + d) % DEV))

    def load_state(c):
        chunk_views(c, (wm, ws, wo, wi, w0), lambda view: local(view(me), wbuf.at[c], w_sem).start())

    def state():
        loop(0, FC0, load_state)
        loop(0, FC0, lambda c: strips(c, (vm, vs, vo, vi, v0), lambda src, dst: local(src, dst, v_sem).start()))
        lane = aligned(me * LANES, LANES)
        for b in range(CLASSES // U):
            dst = wbuf.at[FC0 + b // 4, :, pl.ds(b % 4 * LANES, LANES)]
            local(wf.at[pl.ds(b * U, U), lane], dst, w_sem).start()
        local(wf.at[pl.ds(LASTROW, SUB), lane], wbuf.at[NCH - 1, pl.ds(0, SUB), pl.ds(CW - LANES, LANES)], w_sem).start()
        wbuf[NCH - 1, SUB:, CW - LANES:] = jnp.zeros((U - SUB, LANES), F32)
        for b in range(U):
            dst = vbuf.at[FC0 + b // 4, :, pl.ds(b % 4 * LANES, LANES)]
            local(vf.at[pl.ds(b * U, U)], dst, v_sem).start()

    def strips(c, refs, fn):
        for entry, ref in zip(TABLE, refs):
            first, stack, per, _ = entry

            @pl.when((c >= first) & (c < first + stack * per))
            def _():
                i, row, col = unit_at(entry, c)
                for b in range(CW // LANES):
                    fn(ref.at[aligned(row, U), col // LANES + b, i, 0, :], vbuf.at[c, :, pl.ds(b * LANES, LANES)])

    def state_wait():
        landed(wbuf.at[pl.ds(0, NCH - 1)], w_sem)
        landed(wbuf.at[NCH - 1, :, pl.ds(0, CW - LANES)], w_sem)
        landed(wbuf.at[NCH - 1, pl.ds(0, SUB), pl.ds(CW - LANES, LANES)], w_sem)
        landed(vbuf, v_sem)
        loop(0, NCH, weight_sums)

    def fc_block(b):
        y = jnp.dot(dbuf[...], xbuf[:, aligned(b * 2 * LANES, 2 * LANES)], preferred_element_type=F32)
        for h in range(2):
            part = y[:, h * LANES:(h + 1) * LANES]
            for g in range(CLASSES // U):
                fcg[g // 4, 2 * b + h, :, g % 4 * LANES:(g % 4 + 1) * LANES] = part[g * U:(g + 1) * U]
            fcg[NCH - FC0 - 1, 2 * b + h, 0:SUB, CW - LANES:] = part[LASTROW:]
            fcg[NCH - FC0 - 1, 2 * b + h, SUB:, CW - LANES:] = jnp.zeros((U - SUB, LANES), F32)

    def bias_out():
        line = jnp.dot(dbuf[...], jnp.ones((dbuf.shape[1], LANES), BF16), preferred_element_type=F32)
        square = (LANES, LANES)
        diagonal = lax.broadcasted_iota(jnp.int32, square, 0) == lax.broadcasted_iota(jnp.int32, square, 1)
        for i in range(SUB):
            part = line[i * LANES:min(CLASSES, (i + 1) * LANES)]
            bias[i:i + 1, :] = jnp.sum(jnp.where(diagonal[:part.shape[0]], part, 0.0), axis=0, keepdims=True)
        bias[SUB:, :] = v_bias[...]
        sb[me, SUB:, :] = bias[...]
        each_other(lambda dev: remote(bias, sb.at[me, pl.ds(SUB, 2 * SUB)], sm_send, sm_recv, dev).start())

    def small_update():
        landed(sb.at[0, pl.ds(0, SUB)], misc_sem)
        landed(sb.at[others], sm_recv)
        landed(sb.at[others], sm_send)
        total = jnp.sum(sb[...], axis=0)
        rate = lr_ref[0, 0]
        v_new = MOMENTUM * v_bn[...] + rate * (total[0:SUB] * (1.0 / DEV))
        vb_new = MOMENTUM * total[2 * SUB:] + rate * (total[SUB:2 * SUB] * (1.0 / (DEV * dbuf.shape[1])))
        svnew[0:SUB, :] = v_new
        svnew[SUB:2 * SUB, :] = vb_new
        svnew[2 * SUB:, :] = w_bias[...] - vb_new
        snew[...] = w_bn[aligned(me * SUB, SUB), :] - v_new

    def sent(slot):
        for level in range(4):
            drain(8 >> level, send_sems[level].at[slot])

    def rs_start(c):
        slot = c % NSLOT

        @pl.when(c >= NSLOT)
        def _():
            sent(slot)
            pl.semaphore_wait(cd_sem, 1)
        x1, x2, x3 = order(c)
        pieces = [(q, 2 * (chip + (q // 4) * x1 + ((q // 2) % 2) * x2 + (q % 2) * x3))
                  for q in (4, 5, 6, 7, 0, 1, 2, 3)]

        def to_partner(src, q):
            remote(src, rd.at[slot, q], ds_sem.at[slot], dr_sem.at[slot], partner).start()

        def go_all(view):
            for q, p in pieces:
                to_partner(view(p + 1 - core), q)
                local(view(p + core), acc.at[slot, q], load_sem.at[slot]).start()
        chunk_views(c, (gm, gs, go, gi, g0), go_all)

        @pl.when(c >= FC0)
        def _():
            for q, p in pieces:
                to_partner(fcg.at[c - FC0, p + 1 - core], q)
            for q, p in pieces:
                acc[slot, q] = fcg[c - FC0, p + core]

    def rs_fold(c, level):
        slot, half = c % NSLOT, 4 >> level
        came, going = (rd, r1, r2, r3)[level:level + 2]
        dev = 2 * (chip + order(c)[level]) + core
        if level == 0:
            @pl.when(c < FC0)
            def _():
                drain(8, load_sem.at[slot])
        drain(2 * half, recv_sems[level].at[slot])
        acc[slot, half:2 * half] = acc[slot, half:2 * half] + came[slot, half:2 * half]

        @pl.when(c >= NSLOT)
        def _():
            pl.semaphore_wait(credits[level + 1].at[c % 3], 1)
        remote(acc.at[slot, pl.ds(half, half)], going.at[slot], send_sems[level + 1].at[slot],
               recv_sems[level + 1].at[slot], dev).start()
        acc[slot, 0:half] = acc[slot, 0:half] + came[slot, 0:half]
        give_credit(c, level)

    def give_credit(c, level):
        @pl.when(c + NSLOT < NCH)
        def _():
            if level == 0:
                signal(cd_sem, partner)
            else:
                signal(credits[level].at[c % 3], 2 * (chip + order(c)[level - 1]) + core)

    def fold(x):
        y = jnp.sum(x * x, axis=0, keepdims=True)
        return sum(y[:, i:i + LANES] for i in range(0, CW, LANES))

    def rs_end(c):
        slot = c % NSLOT
        drain(1, recv_sems[3].at[slot])
        scale = jnp.where(c >= FC0, 1.0 / (DEV * dbuf.shape[1]), 1.0 / DEV).astype(F32)
        g = (acc[slot, 0] + r3[slot, 0]) * scale
        grad[c] = g
        t = tensor_of(c)
        sums[pl.ds(t, 1), :] = sums[pl.ds(t, 1), :] + fold(g)
        give_credit(c, 3)

    def weight_sums(c):
        t = pl.ds(SUB + tensor_of(c), 1)
        sums[t, :] = sums[t, :] + fold(wbuf[c])

    def norms_out(n):
        nb[n, me] = sums[...]
        each_other(lambda dev: remote(nb.at[n, me], nb.at[n, me], nb_send.at[n], nb_recv.at[n], dev).start())

    def norms_in(n):
        landed(nb.at[n, others], nb_recv.at[n])
        landed(nb.at[n, others], nb_send.at[n])
        total = jnp.sum(nb[n], axis=0)
        norm = jnp.sqrt(jnp.broadcast_to(jnp.sum(total, axis=1, keepdims=True), (2 * SUB, LANES)))
        g_norm, w_norm = norm[0:SUB], norm[SUB:]
        ratio = jnp.where((w_norm > 0) & (g_norm > 0), TRUST_COEF * w_norm / (g_norm + DECAY * w_norm), 1.0)
        tr[...] = lr_ref[0, 0] * ratio

    def update(a):
        rate = tr[pl.ds(tensor_of(a), 1), :]
        for i in range(0, CW, LANES):
            s = slice(i, i + LANES)
            w = wbuf[a, :, s]
            v = MOMENTUM * vbuf[a, :, s] + rate * (grad[a, :, s] + DECAY * w)
            vbuf[a, :, s] = v
            wbuf[a, :, s] = w - v

    def ag_send(src, a, p, recv, dev):
        remote(src, o_ref.at[a, p], as_sem.at[a % NSEND], recv.at[a], dev).start()

    def ag_pass(a, n):
        x1, x2, x3 = order(a)
        e = [me + 2 * ((q % 2) * x1 + ((q // 2) % 2) * x2 + (q // 4) * x3) for q in range(8)]
        level = n.bit_length() - 1
        held = [wbuf.at[a]] + [o_ref.at[a, p] for p in e[1:n]]
        if n > 1:
            drain(n // 2, ag_sems[level - 1].at[a])
        if n < 8:
            for q in range(n):
                ag_send(held[q], a, e[q], ag_sems[level], e[n])
        for q in range(n // 2, n):
            ag_send(held[q], a, e[q], ad_sem, partner)

    def ag_first(a):
        @pl.when(a >= NSEND)
        def _():
            drain(DEV - 1, as_sem.at[a % NSEND])
        ag_pass(a, 1)
        local(wbuf.at[a], o_ref.at[a, me], loc_sem).start()
        strips(a, (nm, ns, no, ni, n0), lambda dst, src: local(src, dst, vn_sem).start())

    def ag_end(a):
        drain(8, ad_sem.at[a])

    def stage(s, lag, fn, count=NCH):
        c = s - lag

        @pl.when((c >= 0) & (c < count))
        def _():
            fn(c)

    def start_loads():
        local(d_ref, dbuf, misc_sem).start()
        local(x_ref, xbuf, x_sem).start()
        each_other(lambda dev: remote(g_bn.at[dev], sb.at[me, pl.ds(0, SUB)], sm_send, sm_recv, dev).start())
        sums[...] = jnp.zeros_like(sums)
        state()

    def first_products():
        landed(dbuf, misc_sem)
        landed(xbuf, x_sem)
        local(g_bn.at[me], sb.at[me, pl.ds(0, SUB)], misc_sem).start()
        bias_out()

    def small_tensors():
        state_wait()
        small_update()

    def small_back():
        each_other(lambda dev: remote(snew, so_ref.at[me], so_send, so_recv, dev).start())
        local(snew, so_ref.at[me], misc_sem).start()
        local(svnew, sv_ref, x_sem).start()

    def fc_moments():
        for b in range(U):
            local(vbuf.at[FC0 + b // 4, :, pl.ds(b % 4 * LANES, LANES)], nf.at[pl.ds(b * U, U)], vn_sem).start()

    def step(s):
        for at, fn in ((2, start_loads), (MM0, first_products), (SMALL, small_tensors), (SMALL + 1, small_back),
                       (AG0 + NCH + FIRST + 1, fc_moments)):
            pl.when(s == at)(fn)
        for n, at in enumerate((SPLIT, NCH)):
            pl.when(s == at + LAGS[3])(functools.partial(norms_out, n))
            pl.when(s == at + LAGS[3] + 4)(functools.partial(norms_in, n))
        stage(s, LAGS[3], rs_end)
        for level in (2, 1, 0):
            stage(s, LAGS[level], functools.partial(rs_fold, level=level))
        stage(s, 0, rs_start)
        stage(s, AG0 + AGEND, ag_end)
        for n, lag in AGLAGS[::-1]:
            stage(s, AG0 + lag, functools.partial(ag_pass, n=n))
        stage(s, AG0 + FIRST, ag_first)
        stage(s, AG0, update)
        stage(s, MM0, fc_block, DEV // 2)

    barrier = pltpu.get_barrier_semaphore()
    each_other(lambda dev: signal(barrier, dev))
    pl.semaphore_wait(barrier, DEV - 1)
    loop(0, AG0 + NCH + AGEND, step)

    loop(NCH - NSLOT, NCH, lambda c: sent(c % NSLOT))
    loop(NCH - NSEND, NCH, lambda a: drain(DEV - 1, as_sem.at[a % NSEND]))
    landed(snew, misc_sem)
    landed(svnew, x_sem)
    landed(so_ref.at[others], so_recv)
    landed(so_ref.at[others], so_send)
    landed(wbuf, loc_sem)
    landed(vbuf, vn_sem)


def run_comm(lr, grads, pooled, dlogits, weights, moments, small):
    unit = (U, CW)
    anyspec = pl.BlockSpec(memory_space=pl.ANY)
    vspec = pl.BlockSpec(memory_space=pltpu.VMEM)
    dma = pltpu.SemaphoreType.DMA
    reg = pltpu.SemaphoreType.REGULAR
    tile = (SUB, LANES)

    def vmem(*shape, dtype=F32):
        return pltpu.VMEM(shape, dtype)
    return pl.pallas_call(
        comm_kernel,
        out_shape=[jax.ShapeDtypeStruct(s, F32) for s in (
            [(NCH, DEV) + unit] + [v.shape for v in moments] + [(DEV,) + tile, (3 * SUB, LANES)])],
        in_specs=[pl.BlockSpec(memory_space=pltpu.SMEM)] + [anyspec] * 20 + [vspec] * 4,
        out_specs=[anyspec] * 9,
        scratch_shapes=[vmem(NSLOT, n, *unit) for n in (8, 8, 4, 2, 1)] + [vmem(NCH, *unit)] * 3
        + [vmem(*pooled.shape, dtype=BF16), vmem(*dlogits.shape, dtype=BF16),
           vmem(NCH - FC0, DEV, *unit),
           vmem(2 * SUB, LANES), vmem(2, DEV, 2 * SUB, LANES), vmem(*tile),
           vmem(DEV, 3 * SUB, LANES), vmem(2 * SUB, LANES), vmem(*tile), vmem(3 * SUB, LANES)]
        + [dma((NSLOT,))] * 9 + [dma] * 10 + [dma((2,))] * 2 + [dma((NCH,))] * 4 + [dma((NSEND,))]
        + [reg] + [reg((3,))] * 3,
        compiler_params=pltpu.CompilerParams(collective_id=0, has_side_effects=True,
                                             vmem_limit_bytes=60 * 1024 * 1024),
        name='lars_comm',
    )(lr, *grads, pooled, dlogits, *weights, *moments, *small)


NBUF = 6
AHEAD = 3
NFC = 4


def write_kernel(o_ref, nm, ns, no, ni, n0, nf, so_ref, sv_ref, om, os_, oo, oi, o0, of, bm, bs, bo, bi, b0, bf,
                 vm, vs, vo, vi, v0, vf, bn, vbn, vb, wb,
                 buf, bbuf, fbuf, fbbuf, in_sem, f_sem, b_sem, v_sem):
    def view(c, refs):
        entry, ref = [(e, r) for e, r in zip(TABLE, refs) if c >= e[0]][-1]
        i, row, col = unit_at(entry, c)
        return ref.at[i, :, pl.ds(row, U), pl.ds(col, CW)]

    def load(i):
        return [pltpu.make_async_copy(o_ref.at[i], buf.at[i % NBUF], in_sem.at[i % NBUF])]

    def stores(i):
        slot = i % NBUF
        if i < FC0:
            pairs = [(buf.at[slot], view(i, (om, os_, oo, oi, o0))), (bbuf.at[slot], view(i, (bm, bs, bo, bi, b0)))]
        else:
            size = min(LANES, CLASSES - LANES * (i - FC0))
            have, want = pl.ds(0, size), pl.ds(LANES * (i - FC0), size)
            pairs = [(fbuf.at[i % NFC, have], of.at[want]), (fbbuf.at[i % NFC, have], bf.at[want])]
        return [pltpu.make_async_copy(*pairs[0], f_sem.at[slot]), pltpu.make_async_copy(*pairs[1], b_sem.at[slot])]

    done = []

    def settle(upto):
        while len(done) <= upto:
            for d in stores(len(done)):
                d.wait()
            done.append(True)

    for i in range(AHEAD):
        for d in load(i):
            d.start()
    v_outs = [pltpu.make_async_copy(src, dst, v_sem) for src, dst in
              ((nm, vm), (ns, vs), (no, vo), (ni, vi), (n0, v0), (nf.at[pl.ds(0, CLASSES)], vf))]
    bn[...] = so_ref[...]
    vbn[...] = sv_ref[0:SUB]
    vb[...] = sv_ref[SUB:2 * SUB]
    wb[...] = sv_ref[2 * SUB:]
    for i in range(NCH):
        slot = i % NBUF
        for d in load(i):
            d.wait()
        if i < FC0:
            def cast(p, _):
                bbuf[slot, p] = buf[slot, p].astype(BF16)
                return 0
            lax.fori_loop(0, DEV, cast, 0)
        else:
            settle(i - NFC)
            for p in range(DEV):
                for r in range(CW // LANES):
                    x = buf[slot, p, :, LANES * r:LANES * (r + 1)]
                    at = (slice(U * r, U * (r + 1)), slice(LANES * p, LANES * (p + 1)))
                    fbuf[(i % NFC,) + at] = x
                    fbbuf[(i % NFC,) + at] = x.astype(BF16)
        for d in stores(i):
            d.start()
        if i == AHEAD:
            for d in v_outs:
                d.start()
        if i + AHEAD < NCH:
            settle(i + AHEAD - NBUF)
            for d in load(i + AHEAD):
                d.start()
    settle(NCH - 1)
    for d in v_outs:
        d.wait()


def run_write(o, moments_new, so, sv):
    anyspec = pl.BlockSpec(memory_space=pl.ANY)
    vspec = pl.BlockSpec(memory_space=pltpu.VMEM)
    shapes = [dshape(*e, DEV) for e in TABLE] + [(CLASSES, DEV * LANES)]
    moments = [(e[1] * e[2] * LANES, LANES) for e in TABLE] + [(CLASSES, LANES)]
    tile = (SUB, LANES)
    dma = pltpu.SemaphoreType.DMA
    outs = [(s, F32) for s in shapes] + [(s, BF16) for s in shapes] + [(s, F32) for s in moments]
    outs += [((DEV,) + tile, F32)] + [(tile, F32)] * 3
    return pl.pallas_call(
        write_kernel,
        out_shape=[jax.ShapeDtypeStruct(*s) for s in outs],
        in_specs=[anyspec] + [vspec] * 8,
        out_specs=[anyspec] * 18 + [vspec] * 4,
        scratch_shapes=[
            pltpu.VMEM((NBUF, DEV, U, CW), F32), pltpu.VMEM((NBUF, DEV, U, CW), BF16),
            pltpu.VMEM((NFC, LANES, DEV * LANES), F32), pltpu.VMEM((NFC, LANES, DEV * LANES), BF16),
            dma((NBUF,)), dma((NBUF,)), dma((NBUF,)), dma],
        compiler_params=pltpu.CompilerParams(vmem_limit_bytes=48 * 1024 * 1024),
        name='write_out',
    )(o, *moments_new, so, sv)


def solution(mesh):
    n_dev = mesh.shape['dp']
    assert n_dev == DEV
    full, lead, cols = P(), P('dp'), P(None, 'dp')
    moment_specs = (lead, lead, cols, cols, cols, lead, lead, lead)
    in_specs = (full,) * 8 + (lead,) * 8 + moment_specs + (full,)
    out_specs = (full,) * 14 + moment_specs

    def body(w_in0, w_short, w_in, w_mid, w_out, w_fc, w_bn, w_bias,
             g_in0, g_short, g_in, g_mid, g_out, g_bn, pooled, dlogits,
             v_in0, v_short, v_in, v_mid, v_out, v_fc, v_bn, v_bias, learn_rate):
        rank = lax.axis_index('dp')
        width = v_bias.shape[0]
        shapes = [dshape(*e, DEV) for e in TABLE]
        grads = [g.reshape(s) for g, s in zip((g_mid, g_short, g_out, g_in, g_in0), shapes)]
        weights = [w.reshape(s) for w, s in zip((w_mid, w_short, w_out, w_in, w_in0), shapes)] + [w_fc.T]

        def to_rows(v, entry):
            _, stack, _, blocks = entry
            return v.reshape(stack, -1, LANES).transpose(1, 0, 2).reshape(-1, blocks * CW // LANES, stack, 1, LANES)

        def from_rows(v, stack, like):
            return v.reshape(-1, stack, LANES).transpose(1, 0, 2).reshape(like.shape)
        olds = (v_mid, v_short, v_out, v_in, v_in0)
        moments = [to_rows(v, e) for v, e in zip(olds, TABLE)]
        moments.append(jnp.pad(v_fc.reshape(LANES, CLASSES).T, ((0, SUB * LANES - CLASSES), (0, 0))))
        tiles = (-1, SUB, LANES)
        pad = SUB * LANES
        placed = lax.dynamic_update_slice(jnp.zeros((pad,), F32), v_bias, (rank * width,))
        small = [g_bn.reshape(tiles), w_bn.reshape(-1, LANES), v_bn.reshape(SUB, LANES),
                 jnp.pad(w_bias, (0, pad - CLASSES)).reshape(SUB, LANES), placed.reshape(SUB, LANES)]
        o, *made, so, sv = run_comm(learn_rate.reshape(1, 1), grads, pooled, dlogits.T, weights, moments, small)
        mid, short, out, inn, in0, fc, mid_b, short_b, out_b, inn_b, in0_b, fc_b, *rest = run_write(o, [v.reshape(-1, LANES) for v in made], so, sv)
        vm, vs, vo, vi, v0, vf, bn, vbn, vb, wb = rest
        news = [from_rows(v, e[1], old) for v, e, old in zip((vm, vs, vo, vi, v0), TABLE, olds)]
        return (in0.reshape(w_in0.shape), short.reshape(w_short.shape), inn.reshape(w_in.shape),
                mid.reshape(w_mid.shape), out.reshape(w_out.shape), fc.T,
                bn.reshape(w_bn.shape), wb.reshape(-1)[:CLASSES],
                in0_b.reshape(w_in0.shape), short_b.reshape(w_short.shape), inn_b.reshape(w_in.shape),
                mid_b.reshape(w_mid.shape), out_b.reshape(w_out.shape), fc_b.T,
                news[4], news[1], news[3], news[0], news[2], vf.T.reshape(v_fc.shape),
                vbn.reshape(v_bn.shape), lax.dynamic_slice_in_dim(vb.reshape(-1), rank * width, width))

    return jax.shard_map(body, mesh=mesh, in_specs=in_specs, out_specs=out_specs, check_vma=False)
```

```python
import functools
import jax
import jax.numpy as jnp
from jax import lax
from jax.experimental import pallas as pl
from jax.experimental.pallas import tpu as pltpu
from jax.sharding import PartitionSpec as P

MOMENTUM = 0.9
TRUST_COEF = 0.001
DECAY = 0.0001

MESH = pl.DeviceIdType.MESH
F32, BF16 = jnp.float32, jnp.bfloat16
DEV = 16
LANES = 128
U, CW = 32, 512
NCH = 48
FC0 = 40
CLASSES, LASTROW = 1000, 992
SUB = 8
TABLE = ((0, 2, 9, 1), (18, 1, 8, 4), (26, 2, 4, 4), (34, 1, 4, 1), (38, 1, 2, 1))
STARTS = (9, 18, 26, 30, 34, 38, FC0)
SPLIT = 26
NSLOT = 15
LAGS = (2, 6, 10, 13)
AG0 = 43
FIRST = 1
AGLAGS = ((2, 5), (4, 10), (8, 16))
AGEND = 20
NSEND = 18
LOAD0 = 6
MM0 = 12
SMALL = 34


def tensor_of(c):
    return sum(jnp.where(c >= first, 1, 0) for first in STARTS)


def dshape(first, stack, per, blocks, lead):
    return (stack, lead, per // blocks * U, blocks * CW)


def unit_at(entry, c):
    first, _, per, blocks = entry
    k = (c - first) % per
    return (c - first) // per, k // blocks * U, k % blocks * CW


def aligned(x, size):
    return pl.ds(x if isinstance(x, int) else pl.multiple_of(x, size), size)


def chunk_views(c, refs, fn):
    for entry, ref in zip(TABLE, refs):
        first, stack, per, _ = entry

        @pl.when((c >= first) & (c < first + stack * per))
        def _():
            i, row, col = unit_at(entry, c)
            fn(lambda p: ref.at[i, p, aligned(row, U), aligned(col, CW)])


def comm_kernel(lr_ref, gm, gs, go, gi, g0, x_ref, d_ref, wm, ws, wo, wi, w0, wf, vm, vs, vo, vi, v0, vf,
                g_bn, w_bn, v_bn, w_bias, v_bias,
                o_ref, nm, ns, no, ni, n0, nf, so_ref, sv_ref,
                acc, rd, r1, r2, r3, grad, wbuf, vbuf, xbuf, dbuf, fcg,
                sums, nb, tr, sb, bias, snew, svnew,
                load_sem, ds_sem, dr_sem, s1_sem, p1_sem, s2_sem, p2_sem, s3_sem, p3_sem,
                w_sem, v_sem, x_sem, sm_send, sm_recv, so_send, so_recv, loc_sem, vn_sem, misc_sem,
                nb_send, nb_recv, a1_sem, a2_sem, a3_sem, ad_sem, as_sem,
                cd_sem, c1_sem, c2_sem, c3_sem):
    me = lax.axis_index('dp')
    core = me % 2
    chip = me // 2
    partner = me + 1 - 2 * core
    send_sems = (ds_sem, s1_sem, s2_sem, s3_sem)
    recv_sems = (dr_sem, p1_sem, p2_sem, p3_sem)
    ag_sems = (a1_sem, a2_sem, a3_sem)
    credits = (None, c1_sem, c2_sem, c3_sem)
    others = pl.ds(0, DEV - 1)

    def order(c):
        steps = []
        for i in range(3):
            d = (c + i) % 3
            weight = 1 + d + (d * (d - 1)) // 2
            steps.append(weight * (1 - 2 * ((chip // weight) % 2)))
        return steps

    def remote(src, dst, send, recv, dev):
        return pltpu.make_async_remote_copy(src_ref=src, dst_ref=dst, send_sem=send, recv_sem=recv,
                                            device_id=(dev,), device_id_type=MESH)

    def local(src, dst, sem):
        return pltpu.make_async_copy(src, dst, sem)

    def landed(ref, sem):
        local(ref, ref, sem).wait()

    def drain(n, sem):
        landed(o_ref.at[0, pl.ds(0, n)], sem)

    def signal(sem, dev):
        pl.semaphore_signal(sem, inc=1, device_id=(dev,), device_id_type=MESH)

    def loop(lo, hi, fn):
        def body(i, carry):
            fn(i)
            return carry
        lax.fori_loop(lo, hi, body, 0)

    def each_other(fn):
        loop(1, DEV, lambda d: fn((me + d) % DEV))

    def load_state(c):
        chunk_views(c, (wm, ws, wo, wi, w0), lambda view: local(view(me), wbuf.at[c], w_sem).start())
        strips(c, (vm, vs, vo, vi, v0), lambda src, dst: local(src, dst, v_sem).start())
        lane = aligned(me * LANES, LANES)

        def classifier(sizes):
            for i, size in enumerate(sizes):
                rows = pl.ds(pl.multiple_of((c - FC0) * LANES, LANES) + i * U, size)
                part = (c, pl.ds(0, size), pl.ds(i * LANES, LANES))
                local(wf.at[rows, lane], wbuf.at[part], w_sem).start()
                local(vf.at[rows], vbuf.at[part], v_sem).start()
        pl.when((c >= FC0) & (c < NCH - 1))(functools.partial(classifier, (U, U, U, U)))
        pl.when(c == NCH - 1)(functools.partial(classifier, (U, U, U, SUB)))

    def load_two(c):
        load_state(2 * c)
        load_state(2 * c + 1)

    def strips(c, refs, fn):
        for entry, ref in zip(TABLE, refs):
            first, stack, per, _ = entry

            @pl.when((c >= first) & (c < first + stack * per))
            def _():
                i, row, col = unit_at(entry, c)
                for b in range(CW // LANES):
                    fn(ref.at[aligned(row, U), col // LANES + b, i, 0, :], vbuf.at[c, :, pl.ds(b * LANES, LANES)])

    def state_wait():
        for buf, sem in ((wbuf, w_sem), (vbuf, v_sem)):
            landed(buf.at[pl.ds(0, NCH - 1)], sem)
            landed(buf.at[NCH - 1, :, pl.ds(0, CW - LANES)], sem)
            landed(buf.at[NCH - 1, pl.ds(0, SUB), pl.ds(CW - LANES, LANES)], sem)
            buf[NCH - 1, SUB:, CW - LANES:] = jnp.zeros((U - SUB, LANES), F32)
        loop(0, NCH, weight_sums)

    def fc_block(b):
        y = jnp.dot(dbuf[...], xbuf[:, aligned(b * 2 * LANES, 2 * LANES)], preferred_element_type=F32)
        for h in range(2):
            part = y[:, h * LANES:(h + 1) * LANES]
            for g in range(CLASSES // U):
                fcg[g // 4, 2 * b + h, :, g % 4 * LANES:(g % 4 + 1) * LANES] = part[g * U:(g + 1) * U]
            fcg[NCH - FC0 - 1, 2 * b + h, 0:SUB, CW - LANES:] = part[LASTROW:]
            fcg[NCH - FC0 - 1, 2 * b + h, SUB:, CW - LANES:] = jnp.zeros((U - SUB, LANES), F32)

    def bias_out():
        line = jnp.dot(dbuf[...], jnp.ones((dbuf.shape[1], LANES), BF16), preferred_element_type=F32)
        square = (LANES, LANES)
        diagonal = lax.broadcasted_iota(jnp.int32, square, 0) == lax.broadcasted_iota(jnp.int32, square, 1)
        for i in range(SUB):
            part = line[i * LANES:min(CLASSES, (i + 1) * LANES)]
            bias[i:i + 1, :] = jnp.sum(jnp.where(diagonal[:part.shape[0]], part, 0.0), axis=0, keepdims=True)
        bias[SUB:, :] = v_bias[...]
        sb[me, SUB:, :] = bias[...]
        each_other(lambda dev: remote(bias, sb.at[me, pl.ds(SUB, 2 * SUB)], sm_send, sm_recv, dev).start())

    def small_update():
        landed(sb.at[0, pl.ds(0, SUB)], misc_sem)
        landed(sb.at[others], sm_recv)
        landed(sb.at[others], sm_send)
        total = jnp.sum(sb[...], axis=0)
        rate = lr_ref[0, 0]
        v_new = MOMENTUM * v_bn[...] + rate * (total[0:SUB] * (1.0 / DEV))
        vb_new = MOMENTUM * total[2 * SUB:] + rate * (total[SUB:2 * SUB] * (1.0 / (DEV * dbuf.shape[1])))
        svnew[0:SUB, :] = v_new
        svnew[SUB:2 * SUB, :] = vb_new
        for i in range(SUB):
            part = w_bias[:, i * LANES:min(CLASSES, (i + 1) * LANES)]
            row = slice(2 * SUB + i, 2 * SUB + i + 1)
            svnew[row, :] = jnp.zeros((1, LANES), F32)
            svnew[row, :part.shape[1]] = part - vb_new[i:i + 1, :part.shape[1]]
        snew[...] = w_bn[aligned(me * SUB, SUB), :] - v_new

    def sent(slot):
        for level in range(4):
            drain(8 >> level, send_sems[level].at[slot])

    def rs_start(c):
        slot = c % NSLOT

        @pl.when(c >= NSLOT)
        def _():
            sent(slot)
            pl.semaphore_wait(cd_sem, 1)
        x1, x2, x3 = order(c)
        pieces = [(q, 2 * (chip + (q // 4) * x1 + ((q // 2) % 2) * x2 + (q % 2) * x3))
                  for q in (4, 5, 6, 7, 0, 1, 2, 3)]

        def to_partner(src, q):
            remote(src, rd.at[slot, q], ds_sem.at[slot], dr_sem.at[slot], partner).start()

        def go_all(view):
            for q, p in pieces:
                to_partner(view(p + 1 - core), q)
                local(view(p + core), acc.at[slot, q], load_sem.at[slot]).start()
        chunk_views(c, (gm, gs, go, gi, g0), go_all)

        @pl.when(c >= FC0)
        def _():
            for q, p in pieces:
                to_partner(fcg.at[c - FC0, p + 1 - core], q)
            for q, p in pieces:
                acc[slot, q] = fcg[c - FC0, p + core]

    def rs_fold(c, level):
        slot, half = c % NSLOT, 4 >> level
        came, going = (rd, r1, r2, r3)[level:level + 2]
        dev = 2 * (chip + order(c)[level]) + core
        if level == 0:
            @pl.when(c < FC0)
            def _():
                drain(8, load_sem.at[slot])
        drain(2 * half, recv_sems[level].at[slot])
        acc[slot, half:2 * half] = acc[slot, half:2 * half] + came[slot, half:2 * half]

        @pl.when(c >= NSLOT)
        def _():
            pl.semaphore_wait(credits[level + 1].at[c % 3], 1)
        remote(acc.at[slot, pl.ds(half, half)], going.at[slot], send_sems[level + 1].at[slot],
               recv_sems[level + 1].at[slot], dev).start()
        acc[slot, 0:half] = acc[slot, 0:half] + came[slot, 0:half]
        give_credit(c, level)

    def give_credit(c, level):
        @pl.when(c + NSLOT < NCH)
        def _():
            if level == 0:
                signal(cd_sem, partner)
            else:
                signal(credits[level].at[c % 3], 2 * (chip + order(c)[level - 1]) + core)

    def fold(x):
        y = jnp.sum(x * x, axis=0, keepdims=True)
        return sum(y[:, i:i + LANES] for i in range(0, CW, LANES))

    def rs_end(c):
        slot = c % NSLOT
        drain(1, recv_sems[3].at[slot])
        scale = jnp.where(c >= FC0, 1.0 / (DEV * dbuf.shape[1]), 1.0 / DEV).astype(F32)
        g = (acc[slot, 0] + r3[slot, 0]) * scale
        grad[c] = g
        t = tensor_of(c)
        sums[pl.ds(t, 1), :] = sums[pl.ds(t, 1), :] + fold(g)
        give_credit(c, 3)

    def weight_sums(c):
        t = pl.ds(SUB + tensor_of(c), 1)
        sums[t, :] = sums[t, :] + fold(wbuf[c])

    def norms_out(n):
        nb[n, me] = sums[...]
        each_other(lambda dev: remote(nb.at[n, me], nb.at[n, me], nb_send.at[n], nb_recv.at[n], dev).start())

    def norms_in(n):
        landed(nb.at[n, others], nb_recv.at[n])
        landed(nb.at[n, others], nb_send.at[n])
        total = jnp.sum(nb[n], axis=0)
        norm = jnp.sqrt(jnp.broadcast_to(jnp.sum(total, axis=1, keepdims=True), (2 * SUB, LANES)))
        g_norm, w_norm = norm[0:SUB], norm[SUB:]
        ratio = jnp.where((w_norm > 0) & (g_norm > 0), TRUST_COEF * w_norm / (g_norm + DECAY * w_norm), 1.0)
        tr[...] = lr_ref[0, 0] * ratio

    def update(a):
        rate = tr[pl.ds(tensor_of(a), 1), :]
        for i in range(0, CW, LANES):
            s = slice(i, i + LANES)
            w = wbuf[a, :, s]
            v = MOMENTUM * vbuf[a, :, s] + rate * (grad[a, :, s] + DECAY * w)
            vbuf[a, :, s] = v
            wbuf[a, :, s] = w - v

    def ag_send(src, a, p, recv, dev):
        remote(src, o_ref.at[a, p], as_sem.at[a % NSEND], recv.at[a], dev).start()

    def ag_pass(a, n):
        x1, x2, x3 = order(a)
        e = [me + 2 * ((q % 2) * x1 + ((q // 2) % 2) * x2 + (q // 4) * x3) for q in range(8)]
        level = n.bit_length() - 1
        held = [wbuf.at[a]] + [o_ref.at[a, p] for p in e[1:n]]
        if n > 1:
            drain(n // 2, ag_sems[level - 1].at[a])
        if n < 8:
            for q in range(n):
                ag_send(held[q], a, e[q], ag_sems[level], e[n])
        for q in range(n // 2, n):
            ag_send(held[q], a, e[q], ad_sem, partner)

    def ag_first(a):
        @pl.when(a >= NSEND)
        def _():
            drain(DEV - 1, as_sem.at[a % NSEND])
        ag_pass(a, 1)
        local(wbuf.at[a], o_ref.at[a, me], loc_sem).start()
        strips(a, (nm, ns, no, ni, n0), lambda dst, src: local(src, dst, vn_sem).start())

    def ag_end(a):
        drain(8, ad_sem.at[a])

    def stage(s, lag, fn, count=NCH):
        c = s - lag

        @pl.when((c >= 0) & (c < count))
        def _():
            fn(c)

    def start_small():
        each_other(lambda dev: remote(g_bn.at[dev], sb.at[me, pl.ds(0, SUB)], sm_send, sm_recv, dev).start())
        sums[...] = jnp.zeros_like(sums)

    def first_products():
        landed(dbuf, misc_sem)
        landed(xbuf, x_sem)
        local(g_bn.at[me], sb.at[me, pl.ds(0, SUB)], misc_sem).start()
        bias_out()

    def small_tensors():
        state_wait()
        small_update()

    def small_back():
        each_other(lambda dev: remote(snew, so_ref.at[me], so_send, so_recv, dev).start())
        local(snew, so_ref.at[me], misc_sem).start()
        local(svnew, sv_ref, x_sem).start()

    def fc_moments():
        for b in range(CLASSES // U):
            local(vbuf.at[FC0 + b // 4, :, pl.ds(b % 4 * LANES, LANES)], nf.at[pl.ds(b * U, U)], vn_sem).start()
        local(vbuf.at[NCH - 1, pl.ds(0, SUB), pl.ds(CW - LANES, LANES)], nf.at[pl.ds(LASTROW, SUB)], vn_sem).start()

    def step(s):
        for at, fn in ((LOAD0, start_small), (MM0, first_products), (SMALL, small_tensors), (SMALL + 1, small_back),
                       (AG0 + NCH + FIRST + 1, fc_moments)):
            pl.when(s == at)(fn)
        for n, at in enumerate((SPLIT, NCH)):
            pl.when(s == at + LAGS[3])(functools.partial(norms_out, n))
            pl.when(s == at + LAGS[3] + 4)(functools.partial(norms_in, n))
        stage(s, LAGS[3], rs_end)
        for level in (2, 1, 0):
            stage(s, LAGS[level], functools.partial(rs_fold, level=level))
        stage(s, 0, rs_start)
        stage(s, AG0 + AGEND, ag_end)
        for n, lag in AGLAGS[::-1]:
            stage(s, AG0 + lag, functools.partial(ag_pass, n=n))
        stage(s, AG0 + FIRST, ag_first)
        stage(s, AG0, update)
        stage(s, MM0, fc_block, DEV // 2)
        stage(s, LOAD0, load_two, NCH // 2)

    local(d_ref, dbuf, misc_sem).start()
    local(x_ref, xbuf, x_sem).start()
    barrier = pltpu.get_barrier_semaphore()
    each_other(lambda dev: signal(barrier, dev))
    pl.semaphore_wait(barrier, DEV - 1)
    loop(0, AG0 + NCH + AGEND, step)

    loop(NCH - NSLOT, NCH, lambda c: sent(c % NSLOT))
    loop(NCH - NSEND, NCH, lambda a: drain(DEV - 1, as_sem.at[a % NSEND]))
    landed(snew, misc_sem)
    landed(svnew, x_sem)
    landed(so_ref.at[others], so_recv)
    landed(so_ref.at[others], so_send)
    landed(wbuf, loc_sem)
    landed(vbuf.at[pl.ds(0, FC0)], vn_sem)
    landed(nf, vn_sem)


def run_comm(lr, grads, pooled, dlogits, weights, moments, small):
    unit = (U, CW)
    anyspec = pl.BlockSpec(memory_space=pl.ANY)
    vspec = pl.BlockSpec(memory_space=pltpu.VMEM)
    dma = pltpu.SemaphoreType.DMA
    reg = pltpu.SemaphoreType.REGULAR
    tile = (SUB, LANES)

    def vmem(*shape, dtype=F32):
        return pltpu.VMEM(shape, dtype)
    return pl.pallas_call(
        comm_kernel,
        out_shape=[jax.ShapeDtypeStruct(s, F32) for s in (
            [(NCH, DEV) + unit] + [v.shape for v in moments] + [(DEV,) + tile, (3 * SUB, LANES)])],
        in_specs=[pl.BlockSpec(memory_space=pltpu.SMEM)] + [anyspec] * 20 + [vspec] * 4,
        out_specs=[anyspec] * 9,
        scratch_shapes=[vmem(NSLOT, n, *unit) for n in (8, 8, 4, 2, 1)] + [vmem(NCH, *unit)] * 3
        + [vmem(*pooled.shape, dtype=BF16), vmem(*dlogits.shape, dtype=BF16),
           vmem(NCH - FC0, DEV, *unit),
           vmem(2 * SUB, LANES), vmem(2, DEV, 2 * SUB, LANES), vmem(*tile),
           vmem(DEV, 3 * SUB, LANES), vmem(2 * SUB, LANES), vmem(*tile), vmem(3 * SUB, LANES)]
        + [dma((NSLOT,))] * 9 + [dma] * 10 + [dma((2,))] * 2 + [dma((NCH,))] * 4 + [dma((NSEND,))]
        + [reg] + [reg((3,))] * 3,
        compiler_params=pltpu.CompilerParams(collective_id=0, has_side_effects=True,
                                             vmem_limit_bytes=60 * 1024 * 1024),
        name='lars_comm',
    )(lr, *grads, pooled, dlogits, *weights, *moments, *small)


NBUF = 12
AHEAD = 6
NFC = 4


def write_kernel(o_ref, nm, ns, no, ni, n0, nf, so_ref, sv_ref, om, os_, oo, oi, o0, of, bm, bs, bo, bi, b0, bf,
                 vm, vs, vo, vi, v0, vf, bn, vbn, vb, wb,
                 buf, bbuf, fbuf, fbbuf, vbuf, in_sem, f_sem, b_sem, v_sem):
    def view(c, refs):
        entry, ref = [(e, r) for e, r in zip(TABLE, refs) if c >= e[0]][-1]
        i, row, col = unit_at(entry, c)
        return ref.at[i, :, pl.ds(row, U), pl.ds(col, CW)]

    def load(i):
        return [pltpu.make_async_copy(o_ref.at[i], buf.at[i % NBUF], in_sem.at[i % NBUF])]

    def stores(i):
        slot = i % NBUF
        if i < FC0:
            pairs = [(buf.at[slot], view(i, (om, os_, oo, oi, o0))), (bbuf.at[slot], view(i, (bm, bs, bo, bi, b0)))]
        else:
            size = min(LANES, CLASSES - LANES * (i - FC0))
            have, want = pl.ds(0, size), pl.ds(LANES * (i - FC0), size)
            pairs = [(fbuf.at[i % NFC, have], of.at[want]), (fbbuf.at[i % NFC, have], bf.at[want])]
        return [pltpu.make_async_copy(*pairs[0], f_sem.at[slot]), pltpu.make_async_copy(*pairs[1], b_sem.at[slot])]

    done = []

    def settle(upto):
        while len(done) <= upto:
            for d in stores(len(done)):
                d.wait()
            done.append(True)

    for i in range(AHEAD):
        for d in load(i):
            d.start()
    firsts = [e[0] * LANES for e in TABLE] + [FC0 * LANES]

    def moments(refs, back):
        out = []
        for first, ref in zip(firsts, refs):
            pair = (ref, vbuf.at[pl.ds(first, ref.shape[0])])
            out.append(pltpu.make_async_copy(*(pair[::-1] if back else pair), v_sem))
        return out
    v_ins, v_outs = moments((nm, ns, no, ni, n0, nf), False), moments((vm, vs, vo, vi, v0, vf), True)
    for d in v_ins:
        d.start()
    bn[...] = so_ref[...]
    vbn[...] = sv_ref[0:SUB]
    vb[...] = sv_ref[SUB:2 * SUB]
    wb[...] = sv_ref[2 * SUB:]
    for i in range(NCH):
        slot = i % NBUF
        for d in load(i):
            d.wait()
        if i < FC0:
            def cast(p, _):
                bbuf[slot, p] = buf[slot, p].astype(BF16)
                return 0
            lax.fori_loop(0, DEV, cast, 0)
        else:
            settle(i - NFC)
            for p in range(DEV):
                for r in range(CW // LANES):
                    x = buf[slot, p, :, LANES * r:LANES * (r + 1)]
                    at = (slice(U * r, U * (r + 1)), slice(LANES * p, LANES * (p + 1)))
                    fbuf[(i % NFC,) + at] = x
                    fbbuf[(i % NFC,) + at] = x.astype(BF16)
        for d in stores(i):
            d.start()
        if i == AHEAD:
            for d in v_ins:
                d.wait()
            for d in v_outs:
                d.start()
        if i + AHEAD < NCH:
            settle(i + AHEAD - NBUF)
            for d in load(i + AHEAD):
                d.start()
    settle(NCH - 1)
    for d in v_outs:
        d.wait()


def run_write(o, moments_new, so, sv):
    anyspec = pl.BlockSpec(memory_space=pl.ANY)
    vspec = pl.BlockSpec(memory_space=pltpu.VMEM)
    shapes = [dshape(*e, DEV) for e in TABLE] + [(CLASSES, DEV * LANES)]
    moments = [(e[1] * e[2] * LANES, LANES) for e in TABLE] + [(CLASSES, LANES)]
    tile = (SUB, LANES)
    dma = pltpu.SemaphoreType.DMA
    outs = [(s, F32) for s in shapes] + [(s, BF16) for s in shapes] + [(s, F32) for s in moments]
    outs += [((DEV,) + tile, F32)] + [(tile, F32)] * 3
    return pl.pallas_call(
        write_kernel,
        out_shape=[jax.ShapeDtypeStruct(*s) for s in outs],
        in_specs=[anyspec] * 7 + [vspec] * 2,
        out_specs=[anyspec] * 18 + [vspec] * 4,
        scratch_shapes=[
            pltpu.VMEM((NBUF, DEV, U, CW), F32), pltpu.VMEM((NBUF, DEV, U, CW), BF16),
            pltpu.VMEM((NFC, LANES, DEV * LANES), F32), pltpu.VMEM((NFC, LANES, DEV * LANES), BF16),
            pltpu.VMEM((FC0 * LANES + CLASSES, LANES), F32),
            dma((NBUF,)), dma((NBUF,)), dma((NBUF,)), dma],
        compiler_params=pltpu.CompilerParams(vmem_limit_bytes=62 * 1024 * 1024),
        name='write_out',
    )(o, *moments_new, so, sv)


def solution(mesh):
    n_dev = mesh.shape['dp']
    assert n_dev == DEV
    full, lead, cols = P(), P('dp'), P(None, 'dp')
    moment_specs = (lead, lead, cols, cols, cols, lead, lead, lead)
    in_specs = (full,) * 8 + (lead,) * 8 + moment_specs + (full,)
    out_specs = (full,) * 14 + moment_specs

    def body(w_in0, w_short, w_in, w_mid, w_out, w_fc, w_bn, w_bias,
             g_in0, g_short, g_in, g_mid, g_out, g_bn, pooled, dlogits,
             v_in0, v_short, v_in, v_mid, v_out, v_fc, v_bn, v_bias, learn_rate):
        rank = lax.axis_index('dp')
        width = v_bias.shape[0]
        shapes = [dshape(*e, DEV) for e in TABLE]
        grads = [g.reshape(s) for g, s in zip((g_mid, g_short, g_out, g_in, g_in0), shapes)]
        weights = [w.reshape(s) for w, s in zip((w_mid, w_short, w_out, w_in, w_in0), shapes)] + [w_fc.T]

        def to_rows(v, entry):
            _, stack, _, blocks = entry
            return v.reshape(stack, -1, LANES).transpose(1, 0, 2).reshape(-1, blocks * CW // LANES, stack, 1, LANES)

        def from_rows(v, stack, like):
            return v.reshape(-1, stack, LANES).transpose(1, 0, 2).reshape(like.shape)
        olds = (v_mid, v_short, v_out, v_in, v_in0)
        moments = [to_rows(v, e) for v, e in zip(olds, TABLE)]
        moments.append(v_fc.reshape(LANES, CLASSES).T)
        tiles = (-1, SUB, LANES)
        pad = SUB * LANES
        placed = lax.dynamic_update_slice(jnp.zeros((pad,), F32), v_bias, (rank * width,))
        small = [g_bn.reshape(tiles), w_bn.reshape(-1, LANES), v_bn.reshape(SUB, LANES),
                 w_bias.reshape(1, CLASSES), placed.reshape(SUB, LANES)]
        o, *made, so, sv = run_comm(learn_rate.reshape(1, 1), grads, pooled, dlogits.T, weights, moments, small)
        mid, short, out, inn, in0, fc, mid_b, short_b, out_b, inn_b, in0_b, fc_b, *rest = run_write(o, [v.reshape(-1, LANES) for v in made], so, sv)
        vm, vs, vo, vi, v0, vf, bn, vbn, vb, wb = rest
        news = [from_rows(v, e[1], old) for v, e, old in zip((vm, vs, vo, vi, v0), TABLE, olds)]
        return (in0.reshape(w_in0.shape), short.reshape(w_short.shape), inn.reshape(w_in.shape),
                mid.reshape(w_mid.shape), out.reshape(w_out.shape), fc.T,
                bn.reshape(w_bn.shape), wb.reshape(-1)[:CLASSES],
                in0_b.reshape(w_in0.shape), short_b.reshape(w_short.shape), inn_b.reshape(w_in.shape),
                mid_b.reshape(w_mid.shape), out_b.reshape(w_out.shape), fc_b.T,
                news[4], news[1], news[3], news[0], news[2], vf.T.reshape(v_fc.shape),
                vbn.reshape(v_bn.shape), lax.dynamic_slice_in_dim(vb.reshape(-1), rank * width, width))

    return jax.shard_map(body, mesh=mesh, in_specs=in_specs, out_specs=out_specs, check_vma=False)
```

```python
import functools
import jax
import jax.numpy as jnp
from jax import lax
from jax.experimental import pallas as pl
from jax.experimental.pallas import tpu as pltpu
from jax.sharding import PartitionSpec as P

MOMENTUM = 0.9
TRUST_COEF = 0.001
DECAY = 0.0001

MESH = pl.DeviceIdType.MESH
F32, BF16 = jnp.float32, jnp.bfloat16
DEV = 16
LANES = 128
U, CW = 32, 512
NCH = 48
FC0, FCN = 22, 8
FCL = FC0 + FCN - 1
CLASSES, LASTROW = 1000, 992
SUB = 8
TABLE = ((0, 1, 8, 4), (8, 2, 4, 4), (16, 1, 4, 1), (20, 1, 2, 1), (30, 2, 9, 1))
STARTS = (8, 12, 16, 20, FC0, 30, 39)
TAIL0 = 33
TAILK = (NCH - TAIL0) // 3
SPLIT = 22
NSLOT = 15
LAGS = (2, 6, 10, 13)
AG0 = 44
FIRST = 1
AGLAGS = ((2, 5), (4, 10), (8, 16))
AGEND = 20
NSEND = 18
LOAD0 = 6
MM0 = 10
SMALL = 34


def tensor_of(c):
    return sum(jnp.where(c >= first, 1, 0) for first in STARTS)


def dshape(first, stack, per, blocks, lead):
    return (stack, lead, per // blocks * U, blocks * CW)


def unit_at(entry, c):
    first, _, per, blocks = entry
    k = (c - first) % per
    return (c - first) // per, k // blocks * U, k % blocks * CW


def is_fc(c):
    return (c >= FC0) & (c <= FCL)


def strides(chip, c):
    steps = []
    for i in range(3):
        d = (c + i) % 3
        weight = 1 + d + (d * (d - 1)) // 2
        steps.append(weight * (1 - 2 * ((chip // weight) % 2)))
    return steps


def devices(me, steps):
    x1, x2, x3 = steps
    return [me + 2 * ((q % 2) * x1 + ((q // 2) % 2) * x2 + (q // 4) * x3) for q in range(8)]


def aligned(x, size):
    return pl.ds(x if isinstance(x, int) else pl.multiple_of(x, size), size)


def chunk_views(c, refs, fn):
    for entry, ref in zip(TABLE, refs):
        first, stack, per, _ = entry

        @pl.when((c >= first) & (c < first + stack * per))
        def _():
            i, row, col = unit_at(entry, c)
            fn(lambda p: ref.at[i, p, aligned(row, U), aligned(col, CW)])


def comm_kernel(lr_ref, gs, go, gi, g0, gm, x_ref, d_ref, ws, wo, wi, w0, wm, wf, vs, vo, vi, v0, vm, vf,
                g_bn, w_bn, v_bn, w_bias, v_bias,
                o_ref, t0, t1, t2, u0, u1, u2, ns, no, ni, n0, nm, nf, so_ref, sv_ref,
                acc, rd, r1, r2, r3, grad, wbuf, vbuf, xbuf, dbuf, fcg,
                sums, nb, tr, sb, bias, snew, svnew,
                load_sem, ds_sem, dr_sem, s1_sem, p1_sem, s2_sem, p2_sem, s3_sem, p3_sem,
                w_sem, v_sem, x_sem, sm_send, sm_recv, so_send, so_recv, loc_sem, vn_sem, misc_sem,
                nb_send, nb_recv, a1_sem, a2_sem, a3_sem, ad_sem, as_sem,
                cd_sem, c1_sem, c2_sem, c3_sem):
    me = lax.axis_index('dp')
    core = me % 2
    chip = me // 2
    partner = me + 1 - 2 * core
    send_sems = (ds_sem, s1_sem, s2_sem, s3_sem)
    recv_sems = (dr_sem, p1_sem, p2_sem, p3_sem)
    ag_sems = (a1_sem, a2_sem, a3_sem)
    credits = (None, c1_sem, c2_sem, c3_sem)
    others = pl.ds(0, DEV - 1)

    def order(c):
        return strides(chip, c)

    def remote(src, dst, send, recv, dev):
        return pltpu.make_async_remote_copy(src_ref=src, dst_ref=dst, send_sem=send, recv_sem=recv,
                                            device_id=(dev,), device_id_type=MESH)

    def local(src, dst, sem):
        return pltpu.make_async_copy(src, dst, sem)

    def landed(ref, sem):
        local(ref, ref, sem).wait()

    def drain(n, sem):
        landed(o_ref.at[0, pl.ds(0, n)], sem)

    def signal(sem, dev):
        pl.semaphore_signal(sem, inc=1, device_id=(dev,), device_id_type=MESH)

    def loop(lo, hi, fn):
        def body(i, carry):
            fn(i)
            return carry
        lax.fori_loop(lo, hi, body, 0)

    def each_other(fn):
        loop(1, DEV, lambda d: fn((me + d) % DEV))

    def load_state(c):
        chunk_views(c, (ws, wo, wi, w0, wm), lambda view: local(view(me), wbuf.at[c], w_sem).start())
        strips(c, (vs, vo, vi, v0, vm), lambda src, dst: local(src, dst, v_sem).start())
        lane = aligned(me * LANES, LANES)

        def classifier(sizes):
            for i, size in enumerate(sizes):
                rows = pl.ds(pl.multiple_of((c - FC0) * LANES, LANES) + i * U, size)
                part = (c, pl.ds(0, size), pl.ds(i * LANES, LANES))
                local(wf.at[rows, lane], wbuf.at[part], w_sem).start()
                local(vf.at[rows], vbuf.at[part], v_sem).start()
        pl.when((c >= FC0) & (c < FCL))(functools.partial(classifier, (U, U, U, U)))
        pl.when(c == FCL)(functools.partial(classifier, (U, U, U, SUB)))

    def load_two(c):
        load_state(2 * c)
        load_state(2 * c + 1)

    def strips(c, refs, fn):
        for entry, ref in zip(TABLE, refs):
            first, stack, per, _ = entry

            @pl.when((c >= first) & (c < first + stack * per))
            def _():
                i, row, col = unit_at(entry, c)
                for b in range(CW // LANES):
                    fn(ref.at[aligned(row, U), col // LANES + b, i, 0, :], vbuf.at[c, :, pl.ds(b * LANES, LANES)])

    def state_wait():
        for buf, sem in ((wbuf, w_sem), (vbuf, v_sem)):
            landed(buf.at[pl.ds(0, NCH - 1)], sem)
            landed(buf.at[FCL, :, pl.ds(0, CW - LANES)], sem)
            landed(buf.at[FCL, pl.ds(0, SUB), pl.ds(CW - LANES, LANES)], sem)
            buf[FCL, SUB:, CW - LANES:] = jnp.zeros((U - SUB, LANES), F32)
        loop(0, NCH, weight_sums)

    def fc_block(b):
        y = jnp.dot(dbuf[...], xbuf[:, aligned(b * 2 * LANES, 2 * LANES)], preferred_element_type=F32)
        for h in range(2):
            part = y[:, h * LANES:(h + 1) * LANES]
            for g in range(CLASSES // U):
                fcg[g // 4, 2 * b + h, :, g % 4 * LANES:(g % 4 + 1) * LANES] = part[g * U:(g + 1) * U]
            fcg[FCN - 1, 2 * b + h, 0:SUB, CW - LANES:] = part[LASTROW:]
            fcg[FCN - 1, 2 * b + h, SUB:, CW - LANES:] = jnp.zeros((U - SUB, LANES), F32)

    def bias_out():
        line = jnp.dot(dbuf[...], jnp.ones((dbuf.shape[1], LANES), BF16), preferred_element_type=F32)
        square = (LANES, LANES)
        diagonal = lax.broadcasted_iota(jnp.int32, square, 0) == lax.broadcasted_iota(jnp.int32, square, 1)
        for i in range(SUB):
            part = line[i * LANES:min(CLASSES, (i + 1) * LANES)]
            bias[i:i + 1, :] = jnp.sum(jnp.where(diagonal[:part.shape[0]], part, 0.0), axis=0, keepdims=True)
        bias[SUB:, :] = v_bias[...]
        sb[me, SUB:, :] = bias[...]
        each_other(lambda dev: remote(bias, sb.at[me, pl.ds(SUB, 2 * SUB)], sm_send, sm_recv, dev).start())

    def small_update():
        landed(sb.at[0, pl.ds(0, SUB)], misc_sem)
        landed(sb.at[others], sm_recv)
        landed(sb.at[others], sm_send)
        total = jnp.sum(sb[...], axis=0)
        rate = lr_ref[0, 0]
        v_new = MOMENTUM * v_bn[...] + rate * (total[0:SUB] * (1.0 / DEV))
        vb_new = MOMENTUM * total[2 * SUB:] + rate * (total[SUB:2 * SUB] * (1.0 / (DEV * dbuf.shape[1])))
        svnew[0:SUB, :] = v_new
        svnew[SUB:2 * SUB, :] = vb_new
        for i in range(SUB):
            part = w_bias[:, i * LANES:min(CLASSES, (i + 1) * LANES)]
            row = slice(2 * SUB + i, 2 * SUB + i + 1)
            svnew[row, :] = jnp.zeros((1, LANES), F32)
            svnew[row, :part.shape[1]] = part - vb_new[i:i + 1, :part.shape[1]]
        snew[...] = w_bn[aligned(me * SUB, SUB), :] - v_new

    def sent(slot):
        for level in range(4):
            drain(8 >> level, send_sems[level].at[slot])

    def rs_start(c):
        slot = c % NSLOT

        @pl.when(c >= NSLOT)
        def _():
            sent(slot)
            pl.semaphore_wait(cd_sem, 1)
        x1, x2, x3 = order(c)
        pieces = [(q, 2 * (chip + (q // 4) * x1 + ((q // 2) % 2) * x2 + (q % 2) * x3))
                  for q in (4, 5, 6, 7, 0, 1, 2, 3)]

        def to_partner(src, q):
            remote(src, rd.at[slot, q], ds_sem.at[slot], dr_sem.at[slot], partner).start()

        def go_all(view):
            for q, p in pieces:
                to_partner(view(p + 1 - core), q)
                local(view(p + core), acc.at[slot, q], load_sem.at[slot]).start()
        chunk_views(c, (gs, go, gi, g0, gm), go_all)

        @pl.when(is_fc(c))
        def _():
            for q, p in pieces:
                to_partner(fcg.at[c - FC0, p + 1 - core], q)
            for q, p in pieces:
                acc[slot, q] = fcg[c - FC0, p + core]

    def rs_fold(c, level):
        slot, half = c % NSLOT, 4 >> level
        came, going = (rd, r1, r2, r3)[level:level + 2]
        dev = 2 * (chip + order(c)[level]) + core
        if level == 0:
            @pl.when((c < FC0) | (c > FCL))
            def _():
                drain(8, load_sem.at[slot])
        drain(2 * half, recv_sems[level].at[slot])
        acc[slot, half:2 * half] = acc[slot, half:2 * half] + came[slot, half:2 * half]

        @pl.when(c >= NSLOT)
        def _():
            pl.semaphore_wait(credits[level + 1].at[c % 3], 1)
        remote(acc.at[slot, pl.ds(half, half)], going.at[slot], send_sems[level + 1].at[slot],
               recv_sems[level + 1].at[slot], dev).start()
        acc[slot, 0:half] = acc[slot, 0:half] + came[slot, 0:half]
        give_credit(c, level)

    def give_credit(c, level):
        @pl.when(c + NSLOT < NCH)
        def _():
            if level == 0:
                signal(cd_sem, partner)
            else:
                signal(credits[level].at[c % 3], 2 * (chip + order(c)[level - 1]) + core)

    def fold(x):
        y = jnp.sum(x * x, axis=0, keepdims=True)
        return sum(y[:, i:i + LANES] for i in range(0, CW, LANES))

    def rs_end(c):
        slot = c % NSLOT
        drain(1, recv_sems[3].at[slot])
        scale = jnp.where(is_fc(c), 1.0 / (DEV * dbuf.shape[1]), 1.0 / DEV).astype(F32)
        g = (acc[slot, 0] + r3[slot, 0]) * scale
        grad[c] = g
        t = tensor_of(c)
        sums[pl.ds(t, 1), :] = sums[pl.ds(t, 1), :] + fold(g)
        give_credit(c, 3)

    def weight_sums(c):
        t = pl.ds(SUB + tensor_of(c), 1)
        sums[t, :] = sums[t, :] + fold(wbuf[c])

    def norms_out(n):
        nb[n, me] = sums[...]
        each_other(lambda dev: remote(nb.at[n, me], nb.at[n, me], nb_send.at[n], nb_recv.at[n], dev).start())

    def norms_in(n):
        landed(nb.at[n, others], nb_recv.at[n])
        landed(nb.at[n, others], nb_send.at[n])
        total = jnp.sum(nb[n], axis=0)
        norm = jnp.sqrt(jnp.broadcast_to(jnp.sum(total, axis=1, keepdims=True), (2 * SUB, LANES)))
        g_norm, w_norm = norm[0:SUB], norm[SUB:]
        ratio = jnp.where((w_norm > 0) & (g_norm > 0), TRUST_COEF * w_norm / (g_norm + DECAY * w_norm), 1.0)
        tr[...] = lr_ref[0, 0] * ratio

    def update(a):
        rate = tr[pl.ds(tensor_of(a), 1), :]
        for i in range(0, CW, LANES):
            s = slice(i, i + LANES)
            w = wbuf[a, :, s]
            v = MOMENTUM * vbuf[a, :, s] + rate * (grad[a, :, s] + DECAY * w)
            vbuf[a, :, s] = v
            wbuf[a, :, s] = w - v

    def ag_send(src, dst, a, recv, dev):
        remote(src, dst, as_sem.at[a % NSEND], recv.at[a], dev).start()

    def ag_pass(a, n, dst, mirror, last):
        e = devices(me, order(a))
        level = n.bit_length() - 1
        held = [wbuf.at[a]] + [dst(e[q], q) for q in range(1, n)]
        if n > 1:
            drain(n // 2, ag_sems[level - 1].at[a])
        if not last:
            for q in range(n):
                ag_send(held[q], dst(e[q], q + n), a, ag_sems[level], e[n])
        for q in range(n // 2, n):
            ag_send(held[q], mirror(e[q], q), a, ad_sem, partner)
        if n == 1:
            local(wbuf.at[a], dst(me, 0), loc_sem).start()

    def gather(a, n):
        if n == 1:
            @pl.when(a >= NSEND)
            def _():
                drain(DEV - 1, as_sem.at[a % NSEND])
            strips(a, (ns, no, ni, n0, nm), lambda dst, src: local(src, dst, vn_sem).start())

        @pl.when(a < TAIL0)
        def _():
            ag_pass(a, n, lambda p, q: o_ref.at[a, p], lambda p, q: o_ref.at[a, p], n == 8)
        if n < 8:
            for o, (t, u) in enumerate(((t0, u0), (t1, u1), (t2, u2))):
                @pl.when((a >= TAIL0) & (a % 3 == o))
                def _():
                    k = (a - TAIL0) // 3
                    ag_pass(a, n, lambda p, q: t.at[k, q], lambda p, q: u.at[k, q], n == 4)

    def ag_end(a):
        pl.when(a < TAIL0)(lambda: drain(8, ad_sem.at[a]))
        pl.when(a >= TAIL0)(lambda: drain(4, ad_sem.at[a]))

    def stage(s, lag, fn, count=NCH):
        c = s - lag

        @pl.when((c >= 0) & (c < count))
        def _():
            fn(c)

    def start_small():
        each_other(lambda dev: remote(g_bn.at[dev], sb.at[me, pl.ds(0, SUB)], sm_send, sm_recv, dev).start())
        sums[...] = jnp.zeros_like(sums)

    def first_products():
        landed(dbuf, misc_sem)
        landed(xbuf, x_sem)
        local(g_bn.at[me], sb.at[me, pl.ds(0, SUB)], misc_sem).start()
        bias_out()

    def small_tensors():
        state_wait()
        small_update()

    def small_back():
        each_other(lambda dev: remote(snew, so_ref.at[me], so_send, so_recv, dev).start())
        local(snew, so_ref.at[me], misc_sem).start()
        local(svnew, sv_ref, x_sem).start()

    def fc_moments():
        for b in range(CLASSES // U):
            local(vbuf.at[FC0 + b // 4, :, pl.ds(b % 4 * LANES, LANES)], nf.at[pl.ds(b * U, U)], vn_sem).start()
        local(vbuf.at[FCL, pl.ds(0, SUB), pl.ds(CW - LANES, LANES)], nf.at[pl.ds(LASTROW, SUB)], vn_sem).start()

    def step(s):
        for at, fn in ((LOAD0, start_small), (MM0, first_products), (SMALL, small_tensors), (SMALL + 1, small_back),
                       (AG0 + FCL + 2, fc_moments)):
            pl.when(s == at)(fn)
        for n, at in enumerate((SPLIT, NCH)):
            pl.when(s == at + LAGS[3])(functools.partial(norms_out, n))
            pl.when(s == at + LAGS[3] + 4)(functools.partial(norms_in, n))
        stage(s, LAGS[3], rs_end)
        for level in (2, 1, 0):
            stage(s, LAGS[level], functools.partial(rs_fold, level=level))
        stage(s, 0, rs_start)
        stage(s, AG0 + AGEND, ag_end)
        for n, lag in AGLAGS[::-1]:
            stage(s, AG0 + lag, functools.partial(gather, n=n))
        stage(s, AG0 + FIRST, functools.partial(gather, n=1))
        stage(s, AG0, update)
        stage(s, MM0, fc_block, DEV // 2)
        stage(s, LOAD0, load_two, NCH // 2)

    local(d_ref, dbuf, misc_sem).start()
    local(x_ref, xbuf, x_sem).start()
    barrier = pltpu.get_barrier_semaphore()
    each_other(lambda dev: signal(barrier, dev))
    pl.semaphore_wait(barrier, DEV - 1)
    loop(0, AG0 + NCH + AGEND, step)

    loop(NCH - NSLOT, NCH, lambda c: sent(c % NSLOT))
    loop(NCH - NSEND, TAIL0, lambda a: drain(DEV - 1, as_sem.at[a % NSEND]))
    loop(TAIL0, NCH, lambda a: drain(7, as_sem.at[a % NSEND]))
    landed(snew, misc_sem)
    landed(svnew, x_sem)
    landed(so_ref.at[others], so_recv)
    landed(so_ref.at[others], so_send)
    landed(wbuf, loc_sem)
    landed(vbuf.at[pl.ds(0, NCH - FCN)], vn_sem)
    landed(nf, vn_sem)


def run_comm(lr, grads, pooled, dlogits, weights, moments, small):
    unit = (U, CW)
    anyspec = pl.BlockSpec(memory_space=pl.ANY)
    vspec = pl.BlockSpec(memory_space=pltpu.VMEM)
    dma = pltpu.SemaphoreType.DMA
    reg = pltpu.SemaphoreType.REGULAR
    tile = (SUB, LANES)

    def vmem(*shape, dtype=F32):
        return pltpu.VMEM(shape, dtype)
    return pl.pallas_call(
        comm_kernel,
        out_shape=[jax.ShapeDtypeStruct(s, F32) for s in (
            [(TAIL0, DEV) + unit] + [(TAILK, 4) + unit] * 6 + [v.shape for v in moments] + [(DEV,) + tile, (3 * SUB, LANES)])],
        in_specs=[pl.BlockSpec(memory_space=pltpu.SMEM)] + [anyspec] * 20 + [vspec] * 4,
        out_specs=[anyspec] * 15,
        scratch_shapes=[vmem(NSLOT, n, *unit) for n in (8, 8, 4, 2, 1)] + [vmem(NCH, *unit)] * 3
        + [vmem(*pooled.shape, dtype=BF16), vmem(*dlogits.shape, dtype=BF16),
           vmem(FCN, DEV, *unit),
           vmem(2 * SUB, LANES), vmem(2, DEV, 2 * SUB, LANES), vmem(*tile),
           vmem(DEV, 3 * SUB, LANES), vmem(2 * SUB, LANES), vmem(*tile), vmem(3 * SUB, LANES)]
        + [dma((NSLOT,))] * 9 + [dma] * 10 + [dma((2,))] * 2 + [dma((NCH,))] * 4 + [dma((NSEND,))]
        + [reg] + [reg((3,))] * 3,
        compiler_params=pltpu.CompilerParams(collective_id=0, has_side_effects=True,
                                             vmem_limit_bytes=60 * 1024 * 1024),
        name='lars_comm',
    )(lr, *grads, pooled, dlogits, *weights, *moments, *small)


NBUF = 12
AHEAD = 6
NFC = 4
WRITE_FLOPS = 10 ** 8


def write_kernel(o_ref, ns, no, ni, n0, nm, so_ref, sv_ref, os_, oo, oi, o0, om, of, bs, bo, bi, b0, bm, bf,
                 vs, vo, vi, v0, vm, bn, vbn,
                 buf, bbuf, fbuf, fbbuf, vbuf, in_sem, f_sem, b_sem, v_sem):
    def view(c, refs):
        entry, ref = [(e, r) for e, r in zip(TABLE, refs) if c >= e[0]][-1]
        i, row, col = unit_at(entry, c)
        return ref.at[i, :, pl.ds(row, U), pl.ds(col, CW)]

    def load(i):
        return [pltpu.make_async_copy(o_ref.at[i], buf.at[i % NBUF], in_sem.at[i % NBUF])]

    def stores(i):
        slot = i % NBUF
        if not FC0 <= i <= FCL:
            pairs = [(buf.at[slot], view(i, (os_, oo, oi, o0, om))), (bbuf.at[slot], view(i, (bs, bo, bi, b0, bm)))]
        else:
            size = min(LANES, CLASSES - LANES * (i - FC0))
            have, want = pl.ds(0, size), pl.ds(LANES * (i - FC0), size)
            pairs = [(fbuf.at[i % NFC, have], of.at[want]), (fbbuf.at[i % NFC, have], bf.at[want])]
        return [pltpu.make_async_copy(*pairs[0], f_sem.at[slot]), pltpu.make_async_copy(*pairs[1], b_sem.at[slot])]

    done = []

    def settle(upto):
        while len(done) <= upto:
            for d in stores(len(done)):
                d.wait()
            done.append(True)

    for i in range(AHEAD):
        for d in load(i):
            d.start()
    sizes = [e[1] * e[2] * LANES for e in TABLE]
    firsts = [sum(sizes[:n]) for n in range(len(sizes))]

    def moments(refs, back):
        out = []
        for first, ref in zip(firsts, refs):
            pair = (ref, vbuf.at[pl.ds(first, ref.shape[0])])
            out.append(pltpu.make_async_copy(*(pair[::-1] if back else pair), v_sem))
        return out
    v_ins, v_outs = moments((ns, no, ni, n0, nm), False), moments((vs, vo, vi, v0, vm), True)
    for d in v_ins:
        d.start()
    bn[...] = so_ref[...]
    vbn[...] = sv_ref[0:SUB]
    for i in range(TAIL0):
        slot = i % NBUF
        for d in load(i):
            d.wait()
        if not FC0 <= i <= FCL:
            def cast(p, _):
                bbuf[slot, p] = buf[slot, p].astype(BF16)
                return 0
            lax.fori_loop(0, DEV, cast, 0)
        else:
            settle(i - NFC)
            for p in range(DEV):
                for r in range(CW // LANES):
                    x = buf[slot, p, :, LANES * r:LANES * (r + 1)]
                    at = (slice(U * r, U * (r + 1)), slice(LANES * p, LANES * (p + 1)))
                    fbuf[(i % NFC,) + at] = x
                    fbbuf[(i % NFC,) + at] = x.astype(BF16)
        for d in stores(i):
            d.start()
        if i == AHEAD:
            for d in v_ins:
                d.wait()
            for d in v_outs:
                d.start()
        if i + AHEAD < TAIL0:
            settle(i + AHEAD - NBUF)
            for d in load(i + AHEAD):
                d.start()
    settle(TAIL0 - 1)
    for d in v_outs:
        d.wait()


def run_write(o, moments_new, so, sv):
    anyspec = pl.BlockSpec(memory_space=pl.ANY)
    vspec = pl.BlockSpec(memory_space=pltpu.VMEM)
    shapes = [dshape(*e, DEV) for e in TABLE] + [(CLASSES, DEV * LANES)]
    moments = [(e[1] * e[2] * LANES, LANES) for e in TABLE]
    tile = (SUB, LANES)
    dma = pltpu.SemaphoreType.DMA
    outs = [(s, F32) for s in shapes] + [(s, BF16) for s in shapes] + [(s, F32) for s in moments]
    outs += [((DEV,) + tile, F32), (tile, F32)]
    return pl.pallas_call(
        write_kernel,
        out_shape=[jax.ShapeDtypeStruct(*s) for s in outs],
        in_specs=[anyspec] * 6 + [vspec] * 2,
        out_specs=[anyspec] * 17 + [vspec] * 2,
        scratch_shapes=[
            pltpu.VMEM((NBUF, DEV, U, CW), F32), pltpu.VMEM((NBUF, DEV, U, CW), BF16),
            pltpu.VMEM((NFC, LANES, DEV * LANES), F32), pltpu.VMEM((NFC, LANES, DEV * LANES), BF16),
            pltpu.VMEM(((NCH - FCN) * LANES, LANES), F32),
            dma((NBUF,)), dma((NBUF,)), dma((NBUF,)), dma],
        compiler_params=pltpu.CompilerParams(vmem_limit_bytes=62 * 1024 * 1024),
        cost_estimate=pl.CostEstimate(flops=WRITE_FLOPS, bytes_accessed=TAIL0 * 160 * U * CW, transcendentals=0),
        name='write_out',
    )(o, *moments_new, so, sv)


TBUF = 6


def tail_kernel(groups, *refs):
    count = 3 * len(groups)
    srcs, (_, _, om, bm, buf, bbuf, in_sem, f_sem, b_sem) = refs[:count], refs[count:]
    me = lax.axis_index('dp')
    mate = 1 - 2 * (me % 2)
    entry = TABLE[-1]
    size = 4 * len(groups)

    def load(n):
        k, o = n // 3, n % 3
        return [pltpu.make_async_copy(srcs[3 * j + o].at[k], buf.at[n % TBUF, pl.ds(4 * j, 4)], in_sem.at[n % TBUF])
                for j in range(len(groups))]

    def store(n):
        slot = n % TBUF
        e = devices(me, strides(me // 2, n % 3))
        i, row, _ = unit_at(entry, TAIL0 + n)
        for j, (base, other) in enumerate(groups):
            for q in range(4):
                p = e[base + q] + mate * other
                pltpu.make_async_copy(buf.at[slot, 4 * j + q], om.at[i, p, pl.ds(row, U)], f_sem.at[slot]).start()
                pltpu.make_async_copy(bbuf.at[slot, 4 * j + q], bm.at[i, p, pl.ds(row, U)], b_sem.at[slot]).start()

    def settled(n):
        for ref, sem in ((buf, f_sem), (bbuf, b_sem)):
            pltpu.make_async_copy(ref.at[n % TBUF], ref.at[n % TBUF], sem.at[n % TBUF]).wait()

    total, ahead = NCH - TAIL0, TBUF // 2
    for n in range(ahead):
        for d in load(n):
            d.start()
    for n in range(total):
        slot = n % TBUF
        for d in load(n):
            d.wait()

        def cast(p, _):
            bbuf[slot, p] = buf[slot, p].astype(BF16)
            return 0
        lax.fori_loop(0, size, cast, 0)
        store(n)
        nxt = n + ahead
        if nxt < total:
            if nxt >= TBUF:
                settled(nxt - TBUF)
            for d in load(nxt):
                d.start()
    for n in range(max(0, total - TBUF), total):
        settled(n)


def run_tail(groups, srcs, full, half, name):
    anyspec = pl.BlockSpec(memory_space=pl.ANY)
    dma = pltpu.SemaphoreType.DMA
    size = 4 * len(groups)
    count = len(srcs)
    return pl.pallas_call(
        functools.partial(tail_kernel, groups),
        out_shape=[jax.ShapeDtypeStruct(x.shape, x.dtype) for x in (full, half)],
        in_specs=[anyspec] * (count + 2),
        out_specs=[anyspec] * 2,
        input_output_aliases={count: 0, count + 1: 1},
        scratch_shapes=[pltpu.VMEM((TBUF, size, U, CW), F32), pltpu.VMEM((TBUF, size, U, CW), BF16),
                        dma((TBUF,)), dma((TBUF,)), dma((TBUF,))],
        compiler_params=pltpu.CompilerParams(vmem_limit_bytes=62 * 1024 * 1024),
        cost_estimate=pl.CostEstimate(flops=WRITE_FLOPS // 3, bytes_accessed=15 * size * 10 * U * CW, transcendentals=0),
        name=name,
    )(*srcs, full, half)


def solution(mesh):
    n_dev = mesh.shape['dp']
    assert n_dev == DEV
    full, lead, cols = P(), P('dp'), P(None, 'dp')
    moment_specs = (lead, lead, cols, cols, cols, lead, lead, lead)
    in_specs = (full,) * 8 + (lead,) * 8 + moment_specs + (full,)
    out_specs = (full,) * 14 + moment_specs

    def body(w_in0, w_short, w_in, w_mid, w_out, w_fc, w_bn, w_bias,
             g_in0, g_short, g_in, g_mid, g_out, g_bn, pooled, dlogits,
             v_in0, v_short, v_in, v_mid, v_out, v_fc, v_bn, v_bias, learn_rate):
        rank = lax.axis_index('dp')
        width = v_bias.shape[0]
        shapes = [dshape(*e, DEV) for e in TABLE]
        grads = [g.reshape(s) for g, s in zip((g_short, g_out, g_in, g_in0, g_mid), shapes)]
        weights = [w.reshape(s) for w, s in zip((w_short, w_out, w_in, w_in0, w_mid), shapes)] + [w_fc.T]

        def to_rows(v, entry):
            _, stack, _, blocks = entry
            return v.reshape(stack, -1, LANES).transpose(1, 0, 2).reshape(-1, blocks * CW // LANES, stack, 1, LANES)

        def from_rows(v, stack, like):
            return v.reshape(-1, stack, LANES).transpose(1, 0, 2).reshape(like.shape)
        olds = (v_short, v_out, v_in, v_in0, v_mid)
        moments = [to_rows(v, e) for v, e in zip(olds, TABLE)]
        moments.append(v_fc.reshape(LANES, CLASSES).T)
        tiles = (-1, SUB, LANES)
        pad = SUB * LANES
        placed = lax.dynamic_update_slice(jnp.zeros((pad,), F32), v_bias, (rank * width,))
        small = [g_bn.reshape(tiles), w_bn.reshape(-1, LANES), v_bn.reshape(SUB, LANES),
                 w_bias.reshape(1, CLASSES), placed.reshape(SUB, LANES)]
        o, t0, t1, t2, u0, u1, u2, *made, nf, so, sv = run_comm(
            learn_rate.reshape(1, 1), grads, pooled, dlogits.T, weights, moments, small)
        ts, us = (t0, t1, t2), (u0, u1, u2)

        def across(x, weight):
            return lax.ppermute(x, 'dp', [(i, i ^ weight) for i in range(DEV)])
        rs = [across(t, 2 << (n + 2) % 3) for n, t in enumerate(ts)]
        outs = run_write(o, [v.reshape(-1, LANES) for v in made], so, sv)
        short, out, inn, in0, mid, fc, short_b, out_b, inn_b, in0_b, mid_b, fc_b, vs, vo, vi, v0, vm, bn, vbn = outs
        *held, vbn = lax.optimization_barrier((*rs, vbn))
        mates = [across(r, 1) for r in held]
        mid, mid_b = run_tail(((0, False), (0, True), (4, False)), [*ts, *us, *rs], mid, mid_b, 'write_tail')
        mid, mid_b = run_tail(((4, True),), mates, mid, mid_b, 'write_last')
        news = [from_rows(v, e[1], old) for v, e, old in zip((vs, vo, vi, v0, vm), TABLE, olds)]
        vb, wb = sv[SUB:2 * SUB], sv[2 * SUB:]
        return (in0.reshape(w_in0.shape), short.reshape(w_short.shape), inn.reshape(w_in.shape),
                mid.reshape(w_mid.shape), out.reshape(w_out.shape), fc.T,
                bn.reshape(w_bn.shape), wb.reshape(-1)[:CLASSES],
                in0_b.reshape(w_in0.shape), short_b.reshape(w_short.shape), inn_b.reshape(w_in.shape),
                mid_b.reshape(w_mid.shape), out_b.reshape(w_out.shape), fc_b.T,
                news[3], news[0], news[2], news[4], news[1], nf.T.reshape(v_fc.shape),
                vbn.reshape(v_bn.shape), lax.dynamic_slice_in_dim(vb.reshape(-1), rank * width, width))

    return jax.shard_map(body, mesh=mesh, in_specs=in_specs, out_specs=out_specs, check_vma=False)
```

```python
import functools
import jax
import jax.numpy as jnp
from jax import lax
from jax.experimental import pallas as pl
from jax.experimental.pallas import tpu as pltpu
from jax.sharding import PartitionSpec as P

MOMENTUM = 0.9
TRUST_COEF = 0.001
DECAY = 0.0001


MESH = pl.DeviceIdType.MESH
F32, BF16 = jnp.float32, jnp.bfloat16
DEV = 16
LANES = 128
U, CW = 32, 512
NCH = 48
FC0, FCN = 16, 8
FCL = FC0 + FCN - 1
CLASSES, LASTROW = 1000, 992
SUB = 8
TABLE = ((0, 1, 8, 4), (8, 2, 4, 4), (24, 1, 4, 1), (28, 1, 2, 1), (30, 2, 9, 1))
STARTS = (8, 12, FC0, 24, 28, 30, 39)
TAIL0 = 24
GROUP = 12
TAILK = GROUP // 3
SPLIT = 24
NSLOT = 15
LAGS = (3, 6, 9, 12)
AG0 = 45
FIRST = 1
AGLAGS = ((2, 6), (4, 12), (8, 18))
AGEND = 21
NSEND = 18
LOAD0 = 6
MM0 = 6
SMALL = 34


def tensor_of(c):
    return sum(jnp.where(c >= first, 1, 0) for first in STARTS)


def dshape(first, stack, per, blocks, lead):
    return (stack, lead, per // blocks * U, blocks * CW)


def unit_at(entry, c):
    first, _, per, blocks = entry
    k = (c - first) % per
    return (c - first) // per, k // blocks * U, k % blocks * CW


def is_fc(c):
    return (c >= FC0) & (c <= FCL)


def strides(chip, c):
    steps = []
    for i in range(3):
        d = (c + i) % 3
        weight = 1 + d + (d * (d - 1)) // 2
        steps.append(weight * (1 - 2 * ((chip // weight) % 2)))
    return steps


def devices(me, steps):
    x1, x2, x3 = steps
    return [me + 2 * ((q % 2) * x1 + ((q // 2) % 2) * x2 + (q // 4) * x3) for q in range(8)]


def aligned(x, size):
    return pl.ds(x if isinstance(x, int) else pl.multiple_of(x, size), size)


def chunk_views(c, refs, fn):
    for entry, ref in zip(TABLE, refs):
        first, stack, per, _ = entry

        @pl.when((c >= first) & (c < first + stack * per))
        def _():
            i, row, col = unit_at(entry, c)
            fn(lambda p: ref.at[i, p, aligned(row, U), aligned(col, CW)])


def comm_kernel(lr_ref, gs, go, gi, g0, gm, x_ref, d_ref, ws, wo, wi, w0, wm, wf, vs, vo, vi, v0, vm, vf,
                g_bn, w_bn, v_bn, w_bias, v_bias,
                o_ref, t0, t1, t2, t3, t4, t5, u0, u1, u2, u3, u4, u5, ns, no, ni, n0, nm, nf, so_ref, sv_ref,
                acc, rd, r1, r2, r3, grad, wbuf, vbuf, xbuf, dbuf, fcg,
                sums, nb, tr, sb, bias, snew, svnew,
                load_sem, ds_sem, dr_sem, s1_sem, p1_sem, s2_sem, p2_sem, s3_sem, p3_sem,
                w_sem, v_sem, x_sem, sm_send, sm_recv, so_send, so_recv, loc_sem, vn_sem, misc_sem,
                nb_send, nb_recv, a1_sem, a2_sem, a3_sem, ad_sem, as_sem,
                cd_sem, c1_sem, c2_sem, c3_sem):
    me = lax.axis_index('dp')
    core = me % 2
    chip = me // 2
    partner = me + 1 - 2 * core
    send_sems = (ds_sem, s1_sem, s2_sem, s3_sem)
    recv_sems = (dr_sem, p1_sem, p2_sem, p3_sem)
    ag_sems = (a1_sem, a2_sem, a3_sem)
    credits = (None, c1_sem, c2_sem, c3_sem)
    others = pl.ds(0, DEV - 1)

    def order(c):
        return strides(chip, c)

    def remote(src, dst, send, recv, dev):
        return pltpu.make_async_remote_copy(src_ref=src, dst_ref=dst, send_sem=send, recv_sem=recv,
                                            device_id=(dev,), device_id_type=MESH)

    def local(src, dst, sem):
        return pltpu.make_async_copy(src, dst, sem)

    def landed(ref, sem):
        local(ref, ref, sem).wait()

    def drain(n, sem):
        landed(o_ref.at[0, pl.ds(0, n)], sem)

    def signal(sem, dev):
        pl.semaphore_signal(sem, inc=1, device_id=(dev,), device_id_type=MESH)

    def loop(lo, hi, fn):
        def body(i, carry):
            fn(i)
            return carry

        lax.fori_loop(lo, hi, body, 0)

    def each_other(fn):
        loop(1, DEV, lambda d: fn((me + d) % DEV))

    def load_state(c):
        chunk_views(c, (ws, wo, wi, w0, wm), lambda view: local(view(me), wbuf.at[c], w_sem).start())
        strips(c, (vs, vo, vi, v0, vm), lambda src, dst: local(src, dst, v_sem).start())
        lane = aligned(me * LANES, LANES)

        def classifier(sizes):
            for i, size in enumerate(sizes):
                rows = pl.ds(pl.multiple_of((c - FC0) * LANES, LANES) + i * U, size)
                part = (c, pl.ds(0, size), pl.ds(i * LANES, LANES))
                local(wf.at[rows, lane], wbuf.at[part], w_sem).start()
                local(vf.at[rows], vbuf.at[part], v_sem).start()

        pl.when((c >= FC0) & (c < FCL))(functools.partial(classifier, (U, U, U, U)))
        pl.when(c == FCL)(functools.partial(classifier, (U, U, U, SUB)))

    def load_two(c):
        load_state(2 * c)
        load_state(2 * c + 1)

    def strips(c, refs, fn):
        for entry, ref in zip(TABLE, refs):
            first, stack, per, _ = entry

            @pl.when((c >= first) & (c < first + stack * per))
            def _():
                i, row, col = unit_at(entry, c)
                for b in range(CW // LANES):
                    fn(ref.at[aligned(row, U), col // LANES + b, i, 0, :], vbuf.at[c, :, pl.ds(b * LANES, LANES)])

    def state_wait():
        for buf, sem in ((wbuf, w_sem), (vbuf, v_sem)):
            landed(buf.at[pl.ds(0, NCH - 1)], sem)
            landed(buf.at[FCL, :, pl.ds(0, CW - LANES)], sem)
            landed(buf.at[FCL, pl.ds(0, SUB), pl.ds(CW - LANES, LANES)], sem)
            buf[FCL, SUB:, CW - LANES:] = jnp.zeros((U - SUB, LANES), F32)
        loop(0, NCH, weight_sums)

    def fc_block(b):
        y = jnp.dot(dbuf[...], xbuf[:, aligned(b * 2 * LANES, 2 * LANES)], preferred_element_type=F32)
        for h in range(2):
            part = y[:, h * LANES:(h + 1) * LANES]
            for g in range(CLASSES // U):
                fcg[g // 4, 2 * b + h, :, g % 4 * LANES:(g % 4 + 1) * LANES] = part[g * U:(g + 1) * U]
            fcg[FCN - 1, 2 * b + h, 0:SUB, CW - LANES:] = part[LASTROW:]
            fcg[FCN - 1, 2 * b + h, SUB:, CW - LANES:] = jnp.zeros((U - SUB, LANES), F32)

    def bias_out():
        line = jnp.dot(dbuf[...], jnp.ones((dbuf.shape[1], LANES), BF16), preferred_element_type=F32)
        square = (LANES, LANES)
        diagonal = lax.broadcasted_iota(jnp.int32, square, 0) == lax.broadcasted_iota(jnp.int32, square, 1)
        for i in range(SUB):
            part = line[i * LANES:min(CLASSES, (i + 1) * LANES)]
            bias[i:i + 1, :] = jnp.sum(jnp.where(diagonal[:part.shape[0]], part, 0.0), axis=0, keepdims=True)
        bias[SUB:, :] = v_bias[...]
        sb[me, SUB:, :] = bias[...]
        each_other(lambda dev: remote(bias, sb.at[me, pl.ds(SUB, 2 * SUB)], sm_send, sm_recv, dev).start())

    def small_update():
        landed(sb.at[0, pl.ds(0, SUB)], misc_sem)
        landed(sb.at[others], sm_recv)
        landed(sb.at[others], sm_send)
        total = jnp.sum(sb[...], axis=0)
        rate = lr_ref[0, 0]
        v_new = MOMENTUM * v_bn[...] + rate * (total[0:SUB] * (1.0 / DEV))
        vb_new = MOMENTUM * total[2 * SUB:] + rate * (total[SUB:2 * SUB] * (1.0 / (DEV * dbuf.shape[1])))
        svnew[0:SUB, :] = v_new
        svnew[SUB:2 * SUB, :] = vb_new
        for i in range(SUB):
            part = w_bias[:, i * LANES:min(CLASSES, (i + 1) * LANES)]
            row = slice(2 * SUB + i, 2 * SUB + i + 1)
            svnew[row, :] = jnp.zeros((1, LANES), F32)
            svnew[row, :part.shape[1]] = part - vb_new[i:i + 1, :part.shape[1]]
        snew[...] = w_bn[aligned(me * SUB, SUB), :] - v_new

    def sent(slot):
        for level in range(4):
            drain(8 >> level, send_sems[level].at[slot])

    def rs_start(c):
        slot = c % NSLOT

        @pl.when(c >= NSLOT)
        def _():
            sent(slot)
            pl.semaphore_wait(cd_sem, 1)

        x1, x2, x3 = order(c)
        pieces = [(q, 2 * (chip + (q // 4) * x1 + ((q // 2) % 2) * x2 + (q % 2) * x3))
                  for q in (4, 5, 6, 7, 0, 1, 2, 3)]

        def to_partner(src, q):
            remote(src, rd.at[slot, q], ds_sem.at[slot], dr_sem.at[slot], partner).start()

        def go_all(view):
            for q, p in pieces:
                to_partner(view(p + 1 - core), q)
                local(view(p + core), acc.at[slot, q], load_sem.at[slot]).start()

        chunk_views(c, (gs, go, gi, g0, gm), go_all)

        @pl.when(is_fc(c))
        def _():
            for q, p in pieces:
                to_partner(fcg.at[c - FC0, p + 1 - core], q)
            for q, p in pieces:
                acc[slot, q] = fcg[c - FC0, p + core]

    def rs_fold(c, level):
        slot, half = c % NSLOT, 4 >> level
        came, going = (rd, r1, r2, r3)[level:level + 2]
        dev = 2 * (chip + order(c)[level]) + core
        if level == 0:
            @pl.when((c < FC0) | (c > FCL))
            def _():
                drain(8, load_sem.at[slot])
        drain(2 * half, recv_sems[level].at[slot])
        acc[slot, half:2 * half] = acc[slot, half:2 * half] + came[slot, half:2 * half]

        @pl.when(c >= NSLOT)
        def _():
            pl.semaphore_wait(credits[level + 1].at[c % 3], 1)

        remote(acc.at[slot, pl.ds(half, half)], going.at[slot], send_sems[level + 1].at[slot],
               recv_sems[level + 1].at[slot], dev).start()
        acc[slot, 0:half] = acc[slot, 0:half] + came[slot, 0:half]
        give_credit(c, level)

    def give_credit(c, level):
        @pl.when(c + NSLOT < NCH)
        def _():
            if level == 0:
                signal(cd_sem, partner)
            else:
                signal(credits[level].at[c % 3], 2 * (chip + order(c)[level - 1]) + core)

    def fold(x):
        y = jnp.sum(x * x, axis=0, keepdims=True)
        return sum(y[:, i:i + LANES] for i in range(0, CW, LANES))

    def rs_end(c):
        slot = c % NSLOT
        drain(1, recv_sems[3].at[slot])
        scale = jnp.where(is_fc(c), 1.0 / (DEV * dbuf.shape[1]), 1.0 / DEV).astype(F32)
        g = (acc[slot, 0] + r3[slot, 0]) * scale
        grad[c] = g
        t = tensor_of(c)
        sums[pl.ds(t, 1), :] = sums[pl.ds(t, 1), :] + fold(g)
        give_credit(c, 3)

    def weight_sums(c):
        t = pl.ds(SUB + tensor_of(c), 1)
        sums[t, :] = sums[t, :] + fold(wbuf[c])

    def norms_out(n):
        nb[n, me] = sums[...]
        each_other(lambda dev: remote(nb.at[n, me], nb.at[n, me], nb_send.at[n], nb_recv.at[n], dev).start())

    def norms_in(n):
        landed(nb.at[n, others], nb_recv.at[n])
        landed(nb.at[n, others], nb_send.at[n])
        total = jnp.sum(nb[n], axis=0)
        norm = jnp.sqrt(jnp.broadcast_to(jnp.sum(total, axis=1, keepdims=True), (2 * SUB, LANES)))
        g_norm, w_norm = norm[0:SUB], norm[SUB:]
        ratio = jnp.where((w_norm > 0) & (g_norm > 0), TRUST_COEF * w_norm / (g_norm + DECAY * w_norm), 1.0)
        tr[...] = lr_ref[0, 0] * ratio

    def update(a):
        rate = tr[pl.ds(tensor_of(a), 1), :]
        for i in range(0, CW, LANES):
            s = slice(i, i + LANES)
            w = wbuf[a, :, s]
            v = MOMENTUM * vbuf[a, :, s] + rate * (grad[a, :, s] + DECAY * w)
            vbuf[a, :, s] = v
            wbuf[a, :, s] = w - v

    def ag_send(src, dst, a, recv, dev):
        remote(src, dst, as_sem.at[a % NSEND], recv.at[a], dev).start()

    def ag_pass(a, n, dst, mirror, last):
        e = devices(me, order(a))
        level = n.bit_length() - 1
        held = [wbuf.at[a]] + [dst(e[q], q) for q in range(1, n)]
        if n > 1:
            drain(n // 2, ag_sems[level - 1].at[a])
        if not last:
            for q in range(n):
                ag_send(held[q], dst(e[q], q + n), a, ag_sems[level], e[n])
        for q in range(n // 2, n):
            ag_send(held[q], mirror(e[q], q), a, ad_sem, partner)
        if n == 1:
            local(wbuf.at[a], dst(me, 0), loc_sem).start()

    def gather(a, n):
        if n == 1:
            @pl.when(a >= NSEND)
            def _():
                pl.when(a - NSEND < TAIL0)(lambda: drain(DEV - 1, as_sem.at[a % NSEND]))
                pl.when(a - NSEND >= TAIL0)(lambda: drain(7, as_sem.at[a % NSEND]))

            strips(a, (ns, no, ni, n0, nm), lambda dst, src: local(src, dst, vn_sem).start())

        @pl.when(a < TAIL0)
        def _():
            ag_pass(a, n, lambda p, q: o_ref.at[a, p], lambda p, q: o_ref.at[a, p], n == 8)

        if n < 8:
            for j, (t, u) in enumerate(((t0, u0), (t1, u1), (t2, u2), (t3, u3), (t4, u4), (t5, u5))):
                first = TAIL0 + j // 3 * GROUP

                @pl.when((a >= first) & (a < first + GROUP) & (a % 3 == j % 3))
                def _():
                    k = (a - first) // 3
                    ag_pass(a, n, lambda p, q: t.at[k, q], lambda p, q: u.at[k, q], n == 4)

    def ag_end(a):
        pl.when(a < TAIL0)(lambda: drain(8, ad_sem.at[a]))
        pl.when(a >= TAIL0)(lambda: drain(4, ad_sem.at[a]))

    def stage(s, lag, fn, count=NCH):
        c = s - lag

        @pl.when((c >= 0) & (c < count))
        def _():
            fn(c)

    def start_small():
        each_other(lambda dev: remote(g_bn.at[dev], sb.at[me, pl.ds(0, SUB)], sm_send, sm_recv, dev).start())
        sums[...] = jnp.zeros_like(sums)

    def first_products():
        landed(dbuf, misc_sem)
        landed(xbuf, x_sem)
        local(g_bn.at[me], sb.at[me, pl.ds(0, SUB)], misc_sem).start()
        bias_out()

    def small_tensors():
        state_wait()
        small_update()

    def small_back():
        each_other(lambda dev: remote(snew, so_ref.at[me], so_send, so_recv, dev).start())
        local(snew, so_ref.at[me], misc_sem).start()
        local(svnew, sv_ref, x_sem).start()

    def fc_moments():
        for b in range(CLASSES // U):
            local(vbuf.at[FC0 + b // 4, :, pl.ds(b % 4 * LANES, LANES)], nf.at[pl.ds(b * U, U)], vn_sem).start()
        local(vbuf.at[FCL, pl.ds(0, SUB), pl.ds(CW - LANES, LANES)], nf.at[pl.ds(LASTROW, SUB)], vn_sem).start()

    def step(s):
        for at, fn in ((LOAD0, start_small), (MM0, first_products), (SMALL, small_tensors), (SMALL + 1, small_back),
                       (AG0 + FCL + 2, fc_moments)):
            pl.when(s == at)(fn)
        for n, at in enumerate((SPLIT, NCH)):
            pl.when(s == at + LAGS[3])(functools.partial(norms_out, n))
            pl.when(s == at + LAGS[3] + 4)(functools.partial(norms_in, n))
        stage(s, LAGS[3], rs_end)
        for level in (2, 1, 0):
            stage(s, LAGS[level], functools.partial(rs_fold, level=level))
        stage(s, 0, rs_start)
        stage(s, AG0 + AGEND, ag_end)
        for n, lag in AGLAGS[::-1]:
            stage(s, AG0 + lag, functools.partial(gather, n=n))
        stage(s, AG0 + FIRST, functools.partial(gather, n=1))
        stage(s, AG0, update)
        stage(s, MM0, fc_block, DEV // 2)
        stage(s, LOAD0, load_two, NCH // 2)

    local(d_ref, dbuf, misc_sem).start()
    local(x_ref, xbuf, x_sem).start()
    barrier = pltpu.get_barrier_semaphore()
    each_other(lambda dev: signal(barrier, dev))
    pl.semaphore_wait(barrier, DEV - 1)
    loop(0, AG0 + NCH + AGEND, step)

    loop(NCH - NSLOT, NCH, lambda c: sent(c % NSLOT))
    loop(NCH - NSEND, NCH, lambda a: drain(7, as_sem.at[a % NSEND]))
    landed(snew, misc_sem)
    landed(svnew, x_sem)
    landed(so_ref.at[others], so_recv)
    landed(so_ref.at[others], so_send)
    landed(wbuf, loc_sem)
    landed(vbuf.at[pl.ds(0, NCH - FCN)], vn_sem)
    landed(nf, vn_sem)


def run_comm(lr, grads, pooled, dlogits, weights, moments, small):
    unit = (U, CW)
    anyspec = pl.BlockSpec(memory_space=pl.ANY)
    vspec = pl.BlockSpec(memory_space=pltpu.VMEM)
    dma = pltpu.SemaphoreType.DMA
    reg = pltpu.SemaphoreType.REGULAR
    tile = (SUB, LANES)

    def vmem(*shape, dtype=F32):
        return pltpu.VMEM(shape, dtype)

    return pl.pallas_call(
        comm_kernel,
        out_shape=[jax.ShapeDtypeStruct(s, F32) for s in (
            [(TAIL0, DEV) + unit] + [(TAILK, 4) + unit] * 12 + [v.shape for v in moments] + [(DEV,) + tile, (3 * SUB, LANES)])],
        in_specs=[pl.BlockSpec(memory_space=pltpu.SMEM)] + [anyspec] * 20 + [vspec] * 4,
        out_specs=[anyspec] * 21,
        scratch_shapes=[vmem(NSLOT, n, *unit) for n in (8, 8, 4, 2, 1)] + [vmem(NCH, *unit)] * 3
        + [vmem(*pooled.shape, dtype=BF16), vmem(*dlogits.shape, dtype=BF16),
           vmem(FCN, DEV, *unit),
           vmem(2 * SUB, LANES), vmem(2, DEV, 2 * SUB, LANES), vmem(*tile),
           vmem(DEV, 3 * SUB, LANES), vmem(2 * SUB, LANES), vmem(*tile), vmem(3 * SUB, LANES)]
        + [dma((NSLOT,))] * 9 + [dma] * 10 + [dma((2,))] * 2 + [dma((NCH,))] * 4 + [dma((NSEND,))]
        + [reg] + [reg((3,))] * 3,
        compiler_params=pltpu.CompilerParams(collective_id=0, has_side_effects=True,
                                             vmem_limit_bytes=60 * 1024 * 1024),
        name='lars_comm',
    )(lr, *grads, pooled, dlogits, *weights, *moments, *small)


NBUF = 12
AHEAD = 6
NFC = 4
WRITE_FLOPS = 10 ** 8


def write_kernel(o_ref, ns, no, ni, n0, nm, so_ref, sv_ref, os_, oo, of, bs, bo, bf,
                 vs, vo, vi, v0, vm, bn, vbn,
                 buf, bbuf, fbuf, fbbuf, vbuf, in_sem, f_sem, b_sem, v_sem):
    def view(c, refs):
        entry, ref = [(e, r) for e, r in zip(TABLE, refs) if c >= e[0]][-1]
        i, row, col = unit_at(entry, c)
        return ref.at[i, :, pl.ds(row, U), pl.ds(col, CW)]

    def load(i):
        return [pltpu.make_async_copy(o_ref.at[i], buf.at[i % NBUF], in_sem.at[i % NBUF])]

    def stores(i):
        slot = i % NBUF
        if not FC0 <= i <= FCL:
            pairs = [(buf.at[slot], view(i, (os_, oo))), (bbuf.at[slot], view(i, (bs, bo)))]
        else:
            size = min(LANES, CLASSES - LANES * (i - FC0))
            have, want = pl.ds(0, size), pl.ds(LANES * (i - FC0), size)
            pairs = [(fbuf.at[i % NFC, have], of.at[want]), (fbbuf.at[i % NFC, have], bf.at[want])]
        return [pltpu.make_async_copy(*pairs[0], f_sem.at[slot]), pltpu.make_async_copy(*pairs[1], b_sem.at[slot])]

    done = []

    def settle(upto):
        while len(done) <= upto:
            for d in stores(len(done)):
                d.wait()
            done.append(True)

    for i in range(AHEAD):
        for d in load(i):
            d.start()
    sizes = [e[1] * e[2] * LANES for e in TABLE]
    firsts = [sum(sizes[:n]) for n in range(len(sizes))]

    def moments(refs, back):
        out = []
        for first, ref in zip(firsts, refs):
            pair = (ref, vbuf.at[pl.ds(first, ref.shape[0])])
            out.append(pltpu.make_async_copy(*(pair[::-1] if back else pair), v_sem))
        return out

    v_ins, v_outs = moments((ns, no, ni, n0, nm), False), moments((vs, vo, vi, v0, vm), True)
    for d in v_ins:
        d.start()
    bn[...] = so_ref[...]
    vbn[...] = sv_ref[0:SUB]
    for i in range(TAIL0):
        slot = i % NBUF
        for d in load(i):
            d.wait()
        if not FC0 <= i <= FCL:
            def cast(p, _):
                bbuf[slot, p] = buf[slot, p].astype(BF16)
                return 0

            lax.fori_loop(0, DEV, cast, 0)
        else:
            settle(i - NFC)
            for p in range(DEV):
                for r in range(CW // LANES):
                    x = buf[slot, p, :, LANES * r:LANES * (r + 1)]
                    at = (slice(U * r, U * (r + 1)), slice(LANES * p, LANES * (p + 1)))
                    fbuf[(i % NFC,) + at] = x
                    fbbuf[(i % NFC,) + at] = x.astype(BF16)
        for d in stores(i):
            d.start()
        if i == AHEAD:
            for d in v_ins:
                d.wait()
            for d in v_outs:
                d.start()
        if i + AHEAD < TAIL0:
            settle(i + AHEAD - NBUF)
            for d in load(i + AHEAD):
                d.start()
    settle(TAIL0 - 1)
    for d in v_outs:
        d.wait()


def run_write(o, moments_new, so, sv):
    anyspec = pl.BlockSpec(memory_space=pl.ANY)
    vspec = pl.BlockSpec(memory_space=pltpu.VMEM)
    shapes = [dshape(*e, DEV) for e in TABLE[:2]] + [(CLASSES, DEV * LANES)]
    moments = [(e[1] * e[2] * LANES, LANES) for e in TABLE]
    tile = (SUB, LANES)
    dma = pltpu.SemaphoreType.DMA
    outs = [(s, F32) for s in shapes] + [(s, BF16) for s in shapes] + [(s, F32) for s in moments]
    outs += [((DEV,) + tile, F32), (tile, F32)]
    return pl.pallas_call(
        write_kernel,
        out_shape=[jax.ShapeDtypeStruct(*s) for s in outs],
        in_specs=[anyspec] * 6 + [vspec] * 2,
        out_specs=[anyspec] * 11 + [vspec] * 2,
        scratch_shapes=[
            pltpu.VMEM((NBUF, DEV, U, CW), F32), pltpu.VMEM((NBUF, DEV, U, CW), BF16),
            pltpu.VMEM((NFC, LANES, DEV * LANES), F32), pltpu.VMEM((NFC, LANES, DEV * LANES), BF16),
            pltpu.VMEM(((NCH - FCN) * LANES, LANES), F32),
            dma((NBUF,)), dma((NBUF,)), dma((NBUF,)), dma],
        compiler_params=pltpu.CompilerParams(vmem_limit_bytes=62 * 1024 * 1024),
        cost_estimate=pl.CostEstimate(flops=WRITE_FLOPS, bytes_accessed=TAIL0 * 160 * U * CW, transcendentals=0),
        name='write_out',
    )(o, *moments_new, so, sv)


TBUF, TAHEAD = 16, 10


def tail_kernel(jobs, size, count, aliased, *refs):
    srcs, refs = refs[:count], refs[count + 7 * aliased:]
    fulls, halves, (token, buf, bbuf, in_sem, f_sem, b_sem) = refs[:3], refs[3:6], refs[6:]
    me = lax.axis_index('dp')
    mate = 1 - 2 * (me % 2)
    ring = buf.shape[0]
    token[...] = jnp.zeros_like(token)

    def load(n):
        return [pltpu.make_async_copy(srcs[src].at[k], buf.at[n % ring, pl.ds(4 * j, 4)], in_sem.at[n % ring])
                for j, (src, k, _, _) in enumerate(jobs[n][1])]

    def store(n):
        slot = n % ring
        c, parts = jobs[n]
        e = devices(me, strides(me // 2, c % 3))
        entry, full, half = [x for x in zip(TABLE[2:], fulls, halves) if c >= x[0][0]][-1]
        i, row, _ = unit_at(entry, c)
        for j, (_, _, base, other) in enumerate(parts):
            for q in range(4):
                p = e[base + q] + mate * other
                at = (i, p, pl.ds(row, U))
                pltpu.make_async_copy(buf.at[slot, 4 * j + q], full.at[at], f_sem.at[slot]).start()
                pltpu.make_async_copy(bbuf.at[slot, 4 * j + q], half.at[at], b_sem.at[slot]).start()

    def settled(n):
        for ref, sem in ((buf, f_sem), (bbuf, b_sem)):
            pltpu.make_async_copy(ref.at[n % ring], ref.at[n % ring], sem.at[n % ring]).wait()

    total = len(jobs)
    ahead = ring if ring == total else TAHEAD
    for n in range(ahead):
        for d in load(n):
            d.start()
    for n in range(total):
        slot = n % ring
        for d in load(n):
            d.wait()

        def cast(p, _):
            bbuf[slot, p] = buf[slot, p].astype(BF16)
            return 0

        lax.fori_loop(0, size, cast, 0)
        store(n)
        nxt = n + ahead
        if nxt < total:
            if nxt >= ring:
                settled(nxt - ring)
            for d in load(nxt):
                d.start()
    for n in range(max(0, total - ring), total):
        settled(n)


def run_tail(groups, sets, arrays):
    anyspec = pl.BlockSpec(memory_space=pl.ANY)
    dma = pltpu.SemaphoreType.DMA
    size = 4 * len(sets)
    srcs, jobs = [], []
    for g in groups:
        base = len(srcs)
        for arrs, _, _ in sets:
            srcs += arrs[3 * g:3 * g + 3]
        for n in range(GROUP):
            jobs.append((TAIL0 + g * GROUP + n, [(base + 3 * j + n % 3, n // 3, first, other)
                                                 for j, (_, first, other) in enumerate(sets)]))
    ring = min(len(jobs), TBUF)
    count = len(srcs)
    given = list(arrays or [])[:6]
    tokens = list(arrays or [])[6:]
    shapes = [dshape(*e, DEV) for e in TABLE[2:]]
    outs = [jax.ShapeDtypeStruct(s, t) for t in (F32, BF16) for s in shapes]
    return pl.pallas_call(
        functools.partial(tail_kernel, jobs, size, count, len(given) > 0),
        out_shape=outs + [jax.ShapeDtypeStruct((SUB, LANES), F32)],
        in_specs=[anyspec] * (count + len(given) + len(tokens)),
        out_specs=[anyspec] * 6 + [pl.BlockSpec(memory_space=pltpu.VMEM)],
        input_output_aliases={count + n: n for n in range(len(given))},
        scratch_shapes=[pltpu.VMEM((ring, size, U, CW), F32), pltpu.VMEM((ring, size, U, CW), BF16),
                        dma((ring,)), dma((ring,)), dma((ring,))],
        compiler_params=pltpu.CompilerParams(vmem_limit_bytes=62 * 1024 * 1024),
        cost_estimate=pl.CostEstimate(flops=WRITE_FLOPS // 3, bytes_accessed=len(jobs) * size * 10 * U * CW,
                                      transcendentals=0),
    )(*srcs, *given, *tokens)


def solution(mesh):
    n_dev = mesh.shape['dp']
    assert n_dev == DEV
    full, lead, cols = P(), P('dp'), P(None, 'dp')
    moment_specs = (lead, lead, cols, cols, cols, lead, lead, lead)
    in_specs = (full,) * 8 + (lead,) * 8 + moment_specs + (full,)
    out_specs = (full,) * 14 + moment_specs

    def body(w_in0, w_short, w_in, w_mid, w_out, w_fc, w_bn, w_bias,
             g_in0, g_short, g_in, g_mid, g_out, g_bn, pooled, dlogits,
             v_in0, v_short, v_in, v_mid, v_out, v_fc, v_bn, v_bias, learn_rate):
        rank = lax.axis_index('dp')
        width = v_bias.shape[0]
        shapes = [dshape(*e, DEV) for e in TABLE]
        grads = [g.reshape(s) for g, s in zip((g_short, g_out, g_in, g_in0, g_mid), shapes)]
        weights = [w.reshape(s) for w, s in zip((w_short, w_out, w_in, w_in0, w_mid), shapes)] + [w_fc.T]

        def to_rows(v, entry):
            _, stack, _, blocks = entry
            return v.reshape(stack, -1, LANES).transpose(1, 0, 2).reshape(-1, blocks * CW // LANES, stack, 1, LANES)

        def from_rows(v, stack, like):
            return v.reshape(-1, stack, LANES).transpose(1, 0, 2).reshape(like.shape)

        olds = (v_short, v_out, v_in, v_in0, v_mid)
        moments = [to_rows(v, e) for v, e in zip(olds, TABLE)]
        moments.append(v_fc.reshape(LANES, CLASSES).T)
        tiles = (-1, SUB, LANES)
        pad = SUB * LANES
        placed = lax.dynamic_update_slice(jnp.zeros((pad,), F32), v_bias, (rank * width,))
        small = [g_bn.reshape(tiles), w_bn.reshape(-1, LANES), v_bn.reshape(SUB, LANES),
                 w_bias.reshape(1, CLASSES), placed.reshape(SUB, LANES)]
        o, *made, nf, so, sv = run_comm(
            learn_rate.reshape(1, 1), grads, pooled, dlogits.T, weights, moments, small)
        ts, us, made = made[:6], made[6:12], made[12:]

        def across(x, weight):
            return lax.ppermute(x, 'dp', [(i, i ^ weight) for i in range(DEV)])

        def to_mates(arrs, token):
            *held, token = lax.optimization_barrier((*arrs, token))
            return [across(r, 1) for r in held], token

        rs = []
        for n, t in enumerate(ts):
            rs.append(across(t, 2 << (n + 2) % 3))
        outs = run_write(o, [v.reshape(-1, LANES) for v in made], so, sv)
        short, out, fc, short_b, out_b, fc_b, vs, vo, vi, v0, vm, bn, vbn = outs
        mates, vbn = to_mates(rs[:3], vbn)
        tail = run_tail((0, 1), [(ts, 0, False), (us, 0, True)], None)
        *tail, token = run_tail((0,), [(rs, 4, False), (mates, 4, True)], tail)
        last, token = to_mates(rs[3:], token)
        tail = run_tail((1,), [(rs, 4, False)], (*tail, token))
        *tail, _ = run_tail((1,), [(mates + last, 4, True)], tail)
        inn, in0, mid, inn_b, in0_b, mid_b = tail
        news = [from_rows(v, e[1], old) for v, e, old in zip((vs, vo, vi, v0, vm), TABLE, olds)]
        vb, wb = sv[SUB:2 * SUB], sv[2 * SUB:]
        return (in0.reshape(w_in0.shape), short.reshape(w_short.shape), inn.reshape(w_in.shape),
                mid.reshape(w_mid.shape), out.reshape(w_out.shape), fc.T,
                bn.reshape(w_bn.shape), wb.reshape(-1)[:CLASSES],
                in0_b.reshape(w_in0.shape), short_b.reshape(w_short.shape), inn_b.reshape(w_in.shape),
                mid_b.reshape(w_mid.shape), out_b.reshape(w_out.shape), fc_b.T,
                news[3], news[0], news[2], news[4], news[1], nf.T.reshape(v_fc.shape),
                vbn.reshape(v_bn.shape), lax.dynamic_slice_in_dim(vb.reshape(-1), rank * width, width))

    return jax.shard_map(body, mesh=mesh, in_specs=in_specs, out_specs=out_specs, check_vma=False)
```

```python
import functools
import jax
import jax.numpy as jnp
from jax import lax
from jax.experimental import pallas as pl
from jax.experimental.pallas import tpu as pltpu
from jax.sharding import PartitionSpec as P

MOMENTUM = 0.9
TRUST_COEF = 0.001
DECAY = 0.0001


MESH = pl.DeviceIdType.MESH
F32, BF16 = jnp.float32, jnp.bfloat16
DEV = 16
LANES = 128
U, CW = 32, 512
NCH = 48
FC0, FCN = 16, 8
FCL = FC0 + FCN - 1
CLASSES, LASTROW = 1000, 992
SUB = 8
TABLE = ((0, 1, 8, 4), (8, 2, 4, 4), (24, 1, 4, 1), (28, 1, 2, 1), (30, 2, 9, 1))
STARTS = (8, 12, FC0, 24, 28, 30, 39)
TAIL0 = 24
GROUP = 12
TAILK = GROUP // 3
SPLIT = 24
NSLOT = 15
LAGS = (2, 5, 8, 11)
AG0 = 41
FIRST = 1
AGLAGS = ((2, 6), (4, 12), (8, 18))
AGEND = 21
NSEND = 18
LOAD0 = 6
MM0 = 6
SMALL = 34


def tensor_of(c):
    return sum(jnp.where(c >= first, 1, 0) for first in STARTS)


def dshape(first, stack, per, blocks, lead):
    return (stack, lead, per // blocks * U, blocks * CW)


def unit_at(entry, c):
    first, _, per, blocks = entry
    k = (c - first) % per
    return (c - first) // per, k // blocks * U, k % blocks * CW


def is_fc(c):
    return (c >= FC0) & (c <= FCL)


def strides(chip, c):
    steps = []
    for i in range(3):
        d = (c + i) % 3
        weight = 1 + d + (d * (d - 1)) // 2
        steps.append(weight * (1 - 2 * ((chip // weight) % 2)))
    return steps


def devices(me, steps):
    x1, x2, x3 = steps
    return [me + 2 * ((q % 2) * x1 + ((q // 2) % 2) * x2 + (q // 4) * x3) for q in range(8)]


def aligned(x, size):
    return pl.ds(x if isinstance(x, int) else pl.multiple_of(x, size), size)


def chunk_views(c, refs, fn):
    for entry, ref in zip(TABLE, refs):
        first, stack, per, _ = entry

        @pl.when((c >= first) & (c < first + stack * per))
        def _():
            i, row, col = unit_at(entry, c)
            fn(lambda p: ref.at[i, p, aligned(row, U), aligned(col, CW)])


def comm_kernel(lr_ref, gs, go, gi, g0, gm, x_ref, d_ref, ws, wo, wi, w0, wm, wf, vs, vo, vi, v0, vm, vf,
                g_bn, w_bn, v_bn, w_bias, v_bias,
                o_ref, t0, t1, t2, t3, t4, t5, u0, u1, u2, u3, u4, u5, ns, no, ni, n0, nm, nf, so_ref, sv_ref,
                acc, rd, r1, r2, r3, grad, wbuf, vbuf, xbuf, dbuf, fcg,
                sums, nb, tr, sb, bias, snew, svnew,
                load_sem, ds_sem, dr_sem, s1_sem, p1_sem, s2_sem, p2_sem, s3_sem, p3_sem,
                w_sem, v_sem, x_sem, sm_send, sm_recv, so_send, so_recv, loc_sem, vn_sem, misc_sem,
                nb_send, nb_recv, a1_sem, a2_sem, a3_sem, ad_sem, as_sem,
                cd_sem, c1_sem, c2_sem, c3_sem):
    me = lax.axis_index('dp')
    core = me % 2
    chip = me // 2
    partner = me + 1 - 2 * core
    send_sems = (ds_sem, s1_sem, s2_sem, s3_sem)
    recv_sems = (dr_sem, p1_sem, p2_sem, p3_sem)
    ag_sems = (a1_sem, a2_sem, a3_sem)
    credits = (None, c1_sem, c2_sem, c3_sem)
    others = pl.ds(0, DEV - 1)

    def order(c):
        return strides(chip, c)

    def remote(src, dst, send, recv, dev):
        return pltpu.make_async_remote_copy(src_ref=src, dst_ref=dst, send_sem=send, recv_sem=recv,
                                            device_id=(dev,), device_id_type=MESH)

    def local(src, dst, sem):
        return pltpu.make_async_copy(src, dst, sem)

    def landed(ref, sem):
        local(ref, ref, sem).wait()

    def drain(n, sem):
        landed(o_ref.at[0, pl.ds(0, n)], sem)

    def signal(sem, dev):
        pl.semaphore_signal(sem, inc=1, device_id=(dev,), device_id_type=MESH)

    def loop(lo, hi, fn):
        def body(i, carry):
            fn(i)
            return carry

        lax.fori_loop(lo, hi, body, 0)

    def each_other(fn):
        loop(1, DEV, lambda d: fn((me + d) % DEV))

    def load_state(c):
        chunk_views(c, (ws, wo, wi, w0, wm), lambda view: local(view(me), wbuf.at[c], w_sem).start())
        strips(c, (vs, vo, vi, v0, vm), lambda src, dst: local(src, dst, v_sem).start())
        lane = aligned(me * LANES, LANES)

        def classifier(sizes):
            for i, size in enumerate(sizes):
                rows = pl.ds(pl.multiple_of((c - FC0) * LANES, LANES) + i * U, size)
                part = (c, pl.ds(0, size), pl.ds(i * LANES, LANES))
                local(wf.at[rows, lane], wbuf.at[part], w_sem).start()
                local(vf.at[rows], vbuf.at[part], v_sem).start()

        pl.when((c >= FC0) & (c < FCL))(functools.partial(classifier, (U, U, U, U)))
        pl.when(c == FCL)(functools.partial(classifier, (U, U, U, SUB)))

    def load_two(c):
        load_state(2 * c)
        load_state(2 * c + 1)

    def strips(c, refs, fn):
        for entry, ref in zip(TABLE, refs):
            first, stack, per, _ = entry

            @pl.when((c >= first) & (c < first + stack * per))
            def _():
                i, row, col = unit_at(entry, c)
                for b in range(CW // LANES):
                    fn(ref.at[aligned(row, U), col // LANES + b, i, 0, :], vbuf.at[c, :, pl.ds(b * LANES, LANES)])

    def state_wait():
        for buf, sem in ((wbuf, w_sem), (vbuf, v_sem)):
            landed(buf.at[pl.ds(0, NCH - 1)], sem)
            landed(buf.at[FCL, :, pl.ds(0, CW - LANES)], sem)
            landed(buf.at[FCL, pl.ds(0, SUB), pl.ds(CW - LANES, LANES)], sem)
            buf[FCL, SUB:, CW - LANES:] = jnp.zeros((U - SUB, LANES), F32)
        loop(0, NCH, weight_sums)

    def fc_block(b):
        y = jnp.dot(dbuf[...], xbuf[:, aligned(b * 2 * LANES, 2 * LANES)], preferred_element_type=F32)
        for h in range(2):
            part = y[:, h * LANES:(h + 1) * LANES]
            for g in range(CLASSES // U):
                fcg[g // 4, 2 * b + h, :, g % 4 * LANES:(g % 4 + 1) * LANES] = part[g * U:(g + 1) * U]
            fcg[FCN - 1, 2 * b + h, 0:SUB, CW - LANES:] = part[LASTROW:]
            fcg[FCN - 1, 2 * b + h, SUB:, CW - LANES:] = jnp.zeros((U - SUB, LANES), F32)

    def bias_out():
        line = jnp.dot(dbuf[...], jnp.ones((dbuf.shape[1], LANES), BF16), preferred_element_type=F32)
        square = (LANES, LANES)
        diagonal = lax.broadcasted_iota(jnp.int32, square, 0) == lax.broadcasted_iota(jnp.int32, square, 1)
        for i in range(SUB):
            part = line[i * LANES:min(CLASSES, (i + 1) * LANES)]
            bias[i:i + 1, :] = jnp.sum(jnp.where(diagonal[:part.shape[0]], part, 0.0), axis=0, keepdims=True)
        bias[SUB:, :] = v_bias[...]
        sb[me, SUB:, :] = bias[...]
        each_other(lambda dev: remote(bias, sb.at[me, pl.ds(SUB, 2 * SUB)], sm_send, sm_recv, dev).start())

    def small_update():
        landed(sb.at[0, pl.ds(0, SUB)], misc_sem)
        landed(sb.at[others], sm_recv)
        landed(sb.at[others], sm_send)
        total = jnp.sum(sb[...], axis=0)
        rate = lr_ref[0, 0]
        v_new = MOMENTUM * v_bn[...] + rate * (total[0:SUB] * (1.0 / DEV))
        vb_new = MOMENTUM * total[2 * SUB:] + rate * (total[SUB:2 * SUB] * (1.0 / (DEV * dbuf.shape[1])))
        svnew[0:SUB, :] = v_new
        svnew[SUB:2 * SUB, :] = vb_new
        for i in range(SUB):
            part = w_bias[:, i * LANES:min(CLASSES, (i + 1) * LANES)]
            row = slice(2 * SUB + i, 2 * SUB + i + 1)
            svnew[row, :] = jnp.zeros((1, LANES), F32)
            svnew[row, :part.shape[1]] = part - vb_new[i:i + 1, :part.shape[1]]
        snew[...] = w_bn[aligned(me * SUB, SUB), :] - v_new

    def sent(slot):
        for level in range(4):
            drain(8 >> level, send_sems[level].at[slot])

    def rs_start(c):
        slot = c % NSLOT

        @pl.when(c >= NSLOT)
        def _():
            sent(slot)
            pl.semaphore_wait(cd_sem, 1)

        x1, x2, x3 = order(c)
        pieces = [(q, 2 * (chip + (q // 4) * x1 + ((q // 2) % 2) * x2 + (q % 2) * x3))
                  for q in (4, 5, 6, 7, 0, 1, 2, 3)]

        def to_partner(src, q):
            remote(src, rd.at[slot, q], ds_sem.at[slot], dr_sem.at[slot], partner).start()

        def go_all(view):
            for q, p in pieces:
                to_partner(view(p + 1 - core), q)
                local(view(p + core), acc.at[slot, q], load_sem.at[slot]).start()

        chunk_views(c, (gs, go, gi, g0, gm), go_all)

        @pl.when(is_fc(c))
        def _():
            for q, p in pieces:
                to_partner(fcg.at[c - FC0, p + 1 - core], q)
            for q, p in pieces:
                acc[slot, q] = fcg[c - FC0, p + core]

    def rs_fold(c, level):
        slot, half = c % NSLOT, 4 >> level
        came, going = (rd, r1, r2, r3)[level:level + 2]
        dev = 2 * (chip + order(c)[level]) + core
        if level == 0:
            @pl.when((c < FC0) | (c > FCL))
            def _():
                drain(8, load_sem.at[slot])
        drain(2 * half, recv_sems[level].at[slot])
        acc[slot, half:2 * half] = acc[slot, half:2 * half] + came[slot, half:2 * half]

        @pl.when(c >= NSLOT)
        def _():
            pl.semaphore_wait(credits[level + 1].at[c % 3], 1)

        remote(acc.at[slot, pl.ds(half, half)], going.at[slot], send_sems[level + 1].at[slot],
               recv_sems[level + 1].at[slot], dev).start()
        acc[slot, 0:half] = acc[slot, 0:half] + came[slot, 0:half]
        give_credit(c, level)

    def give_credit(c, level):
        @pl.when(c + NSLOT < NCH)
        def _():
            if level == 0:
                signal(cd_sem, partner)
            else:
                signal(credits[level].at[c % 3], 2 * (chip + order(c)[level - 1]) + core)

    def fold(x):
        y = jnp.sum(x * x, axis=0, keepdims=True)
        return sum(y[:, i:i + LANES] for i in range(0, CW, LANES))

    def rs_end(c):
        slot = c % NSLOT
        drain(1, recv_sems[3].at[slot])
        scale = jnp.where(is_fc(c), 1.0 / (DEV * dbuf.shape[1]), 1.0 / DEV).astype(F32)
        g = (acc[slot, 0] + r3[slot, 0]) * scale
        grad[c] = g
        t = tensor_of(c)
        sums[pl.ds(t, 1), :] = sums[pl.ds(t, 1), :] + fold(g)
        give_credit(c, 3)

    def weight_sums(c):
        t = pl.ds(SUB + tensor_of(c), 1)
        sums[t, :] = sums[t, :] + fold(wbuf[c])

    def norms_out(n):
        nb[n, me] = sums[...]
        each_other(lambda dev: remote(nb.at[n, me], nb.at[n, me], nb_send.at[n], nb_recv.at[n], dev).start())

    def norms_in(n):
        landed(nb.at[n, others], nb_recv.at[n])
        landed(nb.at[n, others], nb_send.at[n])
        total = jnp.sum(nb[n], axis=0)
        norm = jnp.sqrt(jnp.broadcast_to(jnp.sum(total, axis=1, keepdims=True), (2 * SUB, LANES)))
        g_norm, w_norm = norm[0:SUB], norm[SUB:]
        ratio = jnp.where((w_norm > 0) & (g_norm > 0), TRUST_COEF * w_norm / (g_norm + DECAY * w_norm), 1.0)
        tr[...] = lr_ref[0, 0] * ratio

    def update(a):
        rate = tr[pl.ds(tensor_of(a), 1), :]
        for i in range(0, CW, LANES):
            s = slice(i, i + LANES)
            w = wbuf[a, :, s]
            v = MOMENTUM * vbuf[a, :, s] + rate * (grad[a, :, s] + DECAY * w)
            vbuf[a, :, s] = v
            wbuf[a, :, s] = w - v

    def ag_send(src, dst, a, recv, dev):
        remote(src, dst, as_sem.at[a % NSEND], recv.at[a], dev).start()

    def ag_pass(a, n, dst, mirror, last):
        e = devices(me, order(a))
        level = n.bit_length() - 1
        held = [wbuf.at[a]] + [dst(e[q], q) for q in range(1, n)]
        if n > 1:
            drain(n // 2, ag_sems[level - 1].at[a])
        if not last:
            for q in range(n):
                ag_send(held[q], dst(e[q], q + n), a, ag_sems[level], e[n])
        for q in range(n // 2, n):
            ag_send(held[q], mirror(e[q], q), a, ad_sem, partner)
        if n == 1:
            local(wbuf.at[a], dst(me, 0), loc_sem).start()

    def gather(a, n):
        if n == 1:
            @pl.when(a >= NSEND)
            def _():
                pl.when(a - NSEND < TAIL0)(lambda: drain(DEV - 1, as_sem.at[a % NSEND]))
                pl.when(a - NSEND >= TAIL0)(lambda: drain(7, as_sem.at[a % NSEND]))

            strips(a, (ns, no, ni, n0, nm), lambda dst, src: local(src, dst, vn_sem).start())

        @pl.when(a < TAIL0)
        def _():
            ag_pass(a, n, lambda p, q: o_ref.at[a, p], lambda p, q: o_ref.at[a, p], n == 8)

        if n < 8:
            for j, (t, u) in enumerate(((t0, u0), (t1, u1), (t2, u2), (t3, u3), (t4, u4), (t5, u5))):
                first = TAIL0 + j // 3 * GROUP

                @pl.when((a >= first) & (a < first + GROUP) & (a % 3 == j % 3))
                def _():
                    k = (a - first) // 3
                    ag_pass(a, n, lambda p, q: t.at[k, q], lambda p, q: u.at[k, q], n == 4)

    def ag_end(a):
        pl.when(a < TAIL0)(lambda: drain(8, ad_sem.at[a]))
        pl.when(a >= TAIL0)(lambda: drain(4, ad_sem.at[a]))

    def stage(s, lag, fn, count=NCH):
        c = s - lag

        @pl.when((c >= 0) & (c < count))
        def _():
            fn(c)

    def start_small():
        each_other(lambda dev: remote(g_bn.at[dev], sb.at[me, pl.ds(0, SUB)], sm_send, sm_recv, dev).start())
        sums[...] = jnp.zeros_like(sums)

    def first_products():
        landed(dbuf, misc_sem)
        landed(xbuf, x_sem)
        local(g_bn.at[me], sb.at[me, pl.ds(0, SUB)], misc_sem).start()
        bias_out()

    def small_tensors():
        state_wait()
        small_update()

    def small_back():
        each_other(lambda dev: remote(snew, so_ref.at[me], so_send, so_recv, dev).start())
        local(snew, so_ref.at[me], misc_sem).start()
        local(svnew, sv_ref, x_sem).start()

    def fc_moments():
        for b in range(CLASSES // U):
            local(vbuf.at[FC0 + b // 4, :, pl.ds(b % 4 * LANES, LANES)], nf.at[pl.ds(b * U, U)], vn_sem).start()
        local(vbuf.at[FCL, pl.ds(0, SUB), pl.ds(CW - LANES, LANES)], nf.at[pl.ds(LASTROW, SUB)], vn_sem).start()

    def step(s):
        for at, fn in ((LOAD0, start_small), (MM0, first_products), (SMALL, small_tensors), (SMALL + 1, small_back),
                       (AG0 + FCL + 2, fc_moments)):
            pl.when(s == at)(fn)
        for n, at in enumerate((SPLIT, NCH)):
            pl.when(s == at + LAGS[3])(functools.partial(norms_out, n))
            pl.when(s == at + LAGS[3] + 4)(functools.partial(norms_in, n))
        stage(s, 0, rs_start)
        for level in range(3):
            stage(s, LAGS[level], functools.partial(rs_fold, level=level))
        stage(s, LAGS[3], rs_end)
        stage(s, AG0 + AGEND, ag_end)
        for n, lag in AGLAGS[::-1]:
            stage(s, AG0 + lag, functools.partial(gather, n=n))
        stage(s, AG0 + FIRST, functools.partial(gather, n=1))
        stage(s, AG0, update)
        stage(s, MM0, fc_block, DEV // 2)
        stage(s, LOAD0, load_two, NCH // 2)

    local(d_ref, dbuf, misc_sem).start()
    local(x_ref, xbuf, x_sem).start()
    barrier = pltpu.get_barrier_semaphore()
    each_other(lambda dev: signal(barrier, dev))
    pl.semaphore_wait(barrier, DEV - 1)
    loop(0, AG0 + NCH + AGEND, step)

    loop(NCH - NSLOT, NCH, lambda c: sent(c % NSLOT))
    loop(NCH - NSEND, NCH, lambda a: drain(7, as_sem.at[a % NSEND]))
    landed(snew, misc_sem)
    landed(svnew, x_sem)
    landed(so_ref.at[others], so_recv)
    landed(so_ref.at[others], so_send)
    landed(wbuf, loc_sem)
    landed(vbuf.at[pl.ds(0, NCH - FCN)], vn_sem)
    landed(nf, vn_sem)


def run_comm(lr, grads, pooled, dlogits, weights, moments, small):
    unit = (U, CW)
    anyspec = pl.BlockSpec(memory_space=pl.ANY)
    vspec = pl.BlockSpec(memory_space=pltpu.VMEM)
    dma = pltpu.SemaphoreType.DMA
    reg = pltpu.SemaphoreType.REGULAR
    tile = (SUB, LANES)

    def vmem(*shape, dtype=F32):
        return pltpu.VMEM(shape, dtype)

    return pl.pallas_call(
        comm_kernel,
        out_shape=[jax.ShapeDtypeStruct(s, F32) for s in (
            [(TAIL0, DEV) + unit] + [(TAILK, 4) + unit] * 12 + [v.shape for v in moments] + [(DEV,) + tile, (3 * SUB, LANES)])],
        in_specs=[pl.BlockSpec(memory_space=pltpu.SMEM)] + [anyspec] * 20 + [vspec] * 4,
        out_specs=[anyspec] * 21,
        scratch_shapes=[vmem(NSLOT, n, *unit) for n in (8, 8, 4, 2, 1)] + [vmem(NCH, *unit)] * 3
        + [vmem(*pooled.shape, dtype=BF16), vmem(*dlogits.shape, dtype=BF16),
           vmem(FCN, DEV, *unit),
           vmem(2 * SUB, LANES), vmem(2, DEV, 2 * SUB, LANES), vmem(*tile),
           vmem(DEV, 3 * SUB, LANES), vmem(2 * SUB, LANES), vmem(*tile), vmem(3 * SUB, LANES)]
        + [dma((NSLOT,))] * 9 + [dma] * 10 + [dma((2,))] * 2 + [dma((NCH,))] * 4 + [dma((NSEND,))]
        + [reg] + [reg((3,))] * 3,
        compiler_params=pltpu.CompilerParams(collective_id=0, has_side_effects=True,
                                             vmem_limit_bytes=60 * 1024 * 1024),
        name='lars_comm',
    )(lr, *grads, pooled, dlogits, *weights, *moments, *small)


NBUF = 12
AHEAD = 6
NFC = 4
WRITE_FLOPS = 10 ** 8
VMEM = 67043328


def write_kernel(o_ref, ns, no, ni, n0, nm, so_ref, sv_ref, os_, oo, of, bs, bo, bf,
                 vs, vo, vi, v0, vm, bn, vbn,
                 buf, bbuf, fbuf, fbbuf, vbuf, in_sem, f_sem, b_sem, v_sem):
    def view(c, refs):
        entry, ref = [(e, r) for e, r in zip(TABLE, refs) if c >= e[0]][-1]
        i, row, col = unit_at(entry, c)
        return ref.at[i, :, pl.ds(row, U), pl.ds(col, CW)]

    def load(i):
        return [pltpu.make_async_copy(o_ref.at[i], buf.at[i % NBUF], in_sem.at[i % NBUF])]

    def stores(i):
        slot = i % NBUF
        if not FC0 <= i <= FCL:
            pairs = [(buf.at[slot], view(i, (os_, oo))), (bbuf.at[slot], view(i, (bs, bo)))]
        else:
            size = min(LANES, CLASSES - LANES * (i - FC0))
            have, want = pl.ds(0, size), pl.ds(LANES * (i - FC0), size)
            pairs = [(fbuf.at[i % NFC, have], of.at[want]), (fbbuf.at[i % NFC, have], bf.at[want])]
        return [pltpu.make_async_copy(*pairs[0], f_sem.at[slot]), pltpu.make_async_copy(*pairs[1], b_sem.at[slot])]

    done = []

    def settle(upto):
        while len(done) <= upto:
            for d in stores(len(done)):
                d.wait()
            done.append(True)

    for i in range(AHEAD):
        for d in load(i):
            d.start()
    sizes = [e[1] * e[2] * LANES for e in TABLE]
    firsts = [sum(sizes[:n]) for n in range(len(sizes))]

    def moments(refs, back):
        out = []
        for first, ref in zip(firsts, refs):
            pair = (ref, vbuf.at[pl.ds(first, ref.shape[0])])
            out.append(pltpu.make_async_copy(*(pair[::-1] if back else pair), v_sem))
        return out

    v_ins, v_outs = moments((ns, no, ni, n0, nm), False), moments((vs, vo, vi, v0, vm), True)
    for d in v_ins:
        d.start()
    bn[...] = so_ref[...]
    vbn[...] = sv_ref[0:SUB]
    for i in range(TAIL0):
        slot = i % NBUF
        for d in load(i):
            d.wait()
        if not FC0 <= i <= FCL:
            def cast(p, _):
                bbuf[slot, p] = buf[slot, p].astype(BF16)
                return 0

            lax.fori_loop(0, DEV, cast, 0)
        else:
            settle(i - NFC)
            for p in range(DEV):
                for r in range(CW // LANES):
                    x = buf[slot, p, :, LANES * r:LANES * (r + 1)]
                    at = (slice(U * r, U * (r + 1)), slice(LANES * p, LANES * (p + 1)))
                    fbuf[(i % NFC,) + at] = x
                    fbbuf[(i % NFC,) + at] = x.astype(BF16)
        for d in stores(i):
            d.start()
        if i == AHEAD:
            for d in v_ins:
                d.wait()
            for d in v_outs:
                d.start()
        if i + AHEAD < TAIL0:
            settle(i + AHEAD - NBUF)
            for d in load(i + AHEAD):
                d.start()
    settle(TAIL0 - 1)
    for d in v_outs:
        d.wait()


def run_write(o, moments_new, so, sv):
    anyspec = pl.BlockSpec(memory_space=pl.ANY)
    vspec = pl.BlockSpec(memory_space=pltpu.VMEM)
    shapes = [dshape(*e, DEV) for e in TABLE[:2]] + [(CLASSES, DEV * LANES)]
    moments = [(e[1] * e[2] * LANES, LANES) for e in TABLE]
    tile = (SUB, LANES)
    dma = pltpu.SemaphoreType.DMA
    outs = [(s, F32) for s in shapes] + [(s, BF16) for s in shapes] + [(s, F32) for s in moments]
    outs += [((DEV,) + tile, F32), (tile, F32)]
    return pl.pallas_call(
        write_kernel,
        out_shape=[jax.ShapeDtypeStruct(*s) for s in outs],
        in_specs=[anyspec] * 6 + [vspec] * 2,
        out_specs=[anyspec] * 11 + [vspec] * 2,
        scratch_shapes=[
            pltpu.VMEM((NBUF, DEV, U, CW), F32), pltpu.VMEM((NBUF, DEV, U, CW), BF16),
            pltpu.VMEM((NFC, LANES, DEV * LANES), F32), pltpu.VMEM((NFC, LANES, DEV * LANES), BF16),
            pltpu.VMEM(((NCH - FCN) * LANES, LANES), F32),
            dma((NBUF,)), dma((NBUF,)), dma((NBUF,)), dma],
        compiler_params=pltpu.CompilerParams(vmem_limit_bytes=VMEM),
        cost_estimate=pl.CostEstimate(flops=WRITE_FLOPS, bytes_accessed=TAIL0 * 160 * U * CW, transcendentals=0),
        name='write_out',
    )(o, *moments_new, so, sv)


TBUF, TAHEAD = 16, 10


def tail_kernel(jobs, size, count, aliased, *refs):
    srcs, refs = refs[:count], refs[count + 7 * aliased:]
    fulls, halves, (token, buf, bbuf, in_sem, f_sem, b_sem) = refs[:3], refs[3:6], refs[6:]
    me = lax.axis_index('dp')
    mate = 1 - 2 * (me % 2)
    ring = buf.shape[0]
    token[...] = jnp.zeros_like(token)

    def load(n):
        return [pltpu.make_async_copy(srcs[src].at[k], buf.at[n % ring, pl.ds(4 * j, 4)], in_sem.at[n % ring])
                for j, (src, k, _, _) in enumerate(jobs[n][1])]

    def store(n):
        slot = n % ring
        c, parts = jobs[n]
        e = devices(me, strides(me // 2, c % 3))
        entry, full, half = [x for x in zip(TABLE[2:], fulls, halves) if c >= x[0][0]][-1]
        i, row, _ = unit_at(entry, c)
        for j, (_, _, base, other) in enumerate(parts):
            for q in range(4):
                p = e[base + q] + mate * other
                at = (i, p, pl.ds(row, U))
                pltpu.make_async_copy(buf.at[slot, 4 * j + q], full.at[at], f_sem.at[slot]).start()
                pltpu.make_async_copy(bbuf.at[slot, 4 * j + q], half.at[at], b_sem.at[slot]).start()

    def settled(n):
        for ref, sem in ((buf, f_sem), (bbuf, b_sem)):
            pltpu.make_async_copy(ref.at[n % ring], ref.at[n % ring], sem.at[n % ring]).wait()

    total = len(jobs)
    ahead = ring if ring == total else TAHEAD
    for n in range(ahead):
        for d in load(n):
            d.start()
    for n in range(total):
        slot = n % ring
        for d in load(n):
            d.wait()

        def cast(p, _):
            bbuf[slot, p] = buf[slot, p].astype(BF16)
            return 0

        lax.fori_loop(0, size, cast, 0)
        store(n)
        nxt = n + ahead
        if nxt < total:
            if nxt >= ring:
                settled(nxt - ring)
            for d in load(nxt):
                d.start()
    for n in range(max(0, total - ring), total):
        settled(n)


def run_tail(groups, sets, arrays):
    anyspec = pl.BlockSpec(memory_space=pl.ANY)
    dma = pltpu.SemaphoreType.DMA
    size = 4 * len(sets)
    srcs, jobs = [], []
    for g in groups:
        base = len(srcs)
        for arrs, _, _ in sets:
            srcs += arrs[3 * g:3 * g + 3]
        for n in range(GROUP):
            jobs.append((TAIL0 + g * GROUP + n, [(base + 3 * j + n % 3, n // 3, first, other)
                                                 for j, (_, first, other) in enumerate(sets)]))
    ring = min(len(jobs), TBUF)
    count = len(srcs)
    given = list(arrays or [])[:6]
    tokens = list(arrays or [])[6:]
    shapes = [dshape(*e, DEV) for e in TABLE[2:]]
    outs = [jax.ShapeDtypeStruct(s, t) for t in (F32, BF16) for s in shapes]
    return pl.pallas_call(
        functools.partial(tail_kernel, jobs, size, count, len(given) > 0),
        out_shape=outs + [jax.ShapeDtypeStruct((SUB, LANES), F32)],
        in_specs=[anyspec] * (count + len(given) + len(tokens)),
        out_specs=[anyspec] * 6 + [pl.BlockSpec(memory_space=pltpu.VMEM)],
        input_output_aliases={count + n: n for n in range(len(given))},
        scratch_shapes=[pltpu.VMEM((ring, size, U, CW), F32), pltpu.VMEM((ring, size, U, CW), BF16),
                        dma((ring,)), dma((ring,)), dma((ring,))],
        compiler_params=pltpu.CompilerParams(vmem_limit_bytes=VMEM),
        cost_estimate=pl.CostEstimate(flops=WRITE_FLOPS // 3, bytes_accessed=len(jobs) * size * 10 * U * CW,
                                      transcendentals=0),
    )(*srcs, *given, *tokens)


def solution(mesh):
    n_dev = mesh.shape['dp']
    assert n_dev == DEV
    full, lead, cols = P(), P('dp'), P(None, 'dp')
    moment_specs = (lead, lead, cols, cols, cols, lead, lead, lead)
    in_specs = (full,) * 8 + (lead,) * 8 + moment_specs + (full,)
    out_specs = (full,) * 14 + moment_specs

    def body(w_in0, w_short, w_in, w_mid, w_out, w_fc, w_bn, w_bias,
             g_in0, g_short, g_in, g_mid, g_out, g_bn, pooled, dlogits,
             v_in0, v_short, v_in, v_mid, v_out, v_fc, v_bn, v_bias, learn_rate):
        rank = lax.axis_index('dp')
        width = v_bias.shape[0]
        shapes = [dshape(*e, DEV) for e in TABLE]
        grads = [g.reshape(s) for g, s in zip((g_short, g_out, g_in, g_in0, g_mid), shapes)]
        weights = [w.reshape(s) for w, s in zip((w_short, w_out, w_in, w_in0, w_mid), shapes)] + [w_fc.T]

        def to_rows(v, entry):
            _, stack, _, blocks = entry
            return v.reshape(stack, -1, LANES).transpose(1, 0, 2).reshape(-1, blocks * CW // LANES, stack, 1, LANES)

        def from_rows(v, stack, like):
            return v.reshape(-1, stack, LANES).transpose(1, 0, 2).reshape(like.shape)

        olds = (v_short, v_out, v_in, v_in0, v_mid)
        moments = [to_rows(v, e) for v, e in zip(olds, TABLE)]
        moments.append(v_fc.reshape(LANES, CLASSES).T)
        tiles = (-1, SUB, LANES)
        pad = SUB * LANES
        placed = lax.dynamic_update_slice(jnp.zeros((pad,), F32), v_bias, (rank * width,))
        small = [g_bn.reshape(tiles), w_bn.reshape(-1, LANES), v_bn.reshape(SUB, LANES),
                 w_bias.reshape(1, CLASSES), placed.reshape(SUB, LANES)]
        o, *made, nf, so, sv = run_comm(
            learn_rate.reshape(1, 1), grads, pooled, dlogits.T, weights, moments, small)
        ts, us, made = made[:6], made[6:12], made[12:]

        def across(x, weight):
            return lax.ppermute(x, 'dp', [(i, i ^ weight) for i in range(DEV)])

        def to_mates(arrs, token):
            *held, token = lax.optimization_barrier((*arrs, token))
            return [across(r, 1) for r in held], token

        rs = []
        for n, t in enumerate(ts):
            rs.append(across(t, 2 << (n + 2) % 3))
        outs = run_write(o, [v.reshape(-1, LANES) for v in made], so, sv)
        short, out, fc, short_b, out_b, fc_b, vs, vo, vi, v0, vm, bn, vbn = outs
        mates, vbn = to_mates(rs[:3], vbn)
        tail = run_tail((0, 1), [(ts, 0, False), (us, 0, True)], None)
        *tail, token = run_tail((0,), [(rs, 4, False), (mates, 4, True)], tail)
        last, token = to_mates(rs[3:], token)
        tail = run_tail((1,), [(rs, 4, False)], (*tail, token))
        *tail, _ = run_tail((1,), [(mates + last, 4, True)], tail)
        inn, in0, mid, inn_b, in0_b, mid_b = tail
        news = [from_rows(v, e[1], old) for v, e, old in zip((vs, vo, vi, v0, vm), TABLE, olds)]
        vb, wb = sv[SUB:2 * SUB], sv[2 * SUB:]
        return (in0.reshape(w_in0.shape), short.reshape(w_short.shape), inn.reshape(w_in.shape),
                mid.reshape(w_mid.shape), out.reshape(w_out.shape), fc.T,
                bn.reshape(w_bn.shape), wb.reshape(-1)[:CLASSES],
                in0_b.reshape(w_in0.shape), short_b.reshape(w_short.shape), inn_b.reshape(w_in.shape),
                mid_b.reshape(w_mid.shape), out_b.reshape(w_out.shape), fc_b.T,
                news[3], news[0], news[2], news[4], news[1], nf.T.reshape(v_fc.shape),
                vbn.reshape(v_bn.shape), lax.dynamic_slice_in_dim(vb.reshape(-1), rank * width, width))

    return jax.shard_map(body, mesh=mesh, in_specs=in_specs, out_specs=out_specs, check_vma=False)
```

```python
import functools
import jax
import jax.numpy as jnp
from jax import lax
from jax.experimental import pallas as pl
from jax.experimental.pallas import tpu as pltpu
from jax.sharding import PartitionSpec as P

MOMENTUM = 0.9
TRUST_COEF = 0.001
DECAY = 0.0001


MESH = pl.DeviceIdType.MESH
F32, BF16 = jnp.float32, jnp.bfloat16
DEV = 16
LANES = 128
U, CW = 32, 512
NCH = 48
FC0, FCN = 16, 8
FCL = FC0 + FCN - 1
CLASSES, LASTROW = 1000, 992
SUB = 8
TABLE = ((0, 1, 8, 4), (8, 2, 4, 4), (24, 1, 4, 1), (28, 1, 2, 1), (30, 2, 9, 1))
STARTS = (8, 12, FC0, 24, 28, 30, 39)
TAIL0 = 24
GROUP = 12
TAILK = GROUP // 3
SPLIT = 24
NSLOT = 15
LAGS = (3, 9, 12, 14)
AG0 = 45
FIRST = 1
AGLAGS = ((2, 6), (4, 12), (8, 18))
AGEND = 21
NSEND = 18
LOAD0 = 6
MM0 = 6
SMALL = 34


def tensor_of(c):
    return sum(jnp.where(c >= first, 1, 0) for first in STARTS)


def dshape(first, stack, per, blocks, lead):
    return (stack, lead, per // blocks * U, blocks * CW)


def unit_at(entry, c):
    first, _, per, blocks = entry
    k = (c - first) % per
    return (c - first) // per, k // blocks * U, k % blocks * CW


def is_fc(c):
    return (c >= FC0) & (c <= FCL)


def strides(chip, c):
    steps = []
    for i in range(3):
        d = (c + i) % 3
        weight = 1 + d + (d * (d - 1)) // 2
        steps.append(weight * (1 - 2 * ((chip // weight) % 2)))
    return steps


def devices(me, steps):
    x1, x2, x3 = steps
    return [me + 2 * ((q % 2) * x1 + ((q // 2) % 2) * x2 + (q // 4) * x3) for q in range(8)]


def aligned(x, size):
    return pl.ds(x if isinstance(x, int) else pl.multiple_of(x, size), size)


def chunk_views(c, refs, fn):
    for entry, ref in zip(TABLE, refs):
        first, stack, per, _ = entry

        @pl.when((c >= first) & (c < first + stack * per))
        def _():
            i, row, col = unit_at(entry, c)
            fn(lambda p: ref.at[i, p, aligned(row, U), aligned(col, CW)])


def comm_kernel(lr_ref, gs, go, gi, g0, gm, x_ref, d_ref, ws, wo, wi, w0, wm, wf, vs, vo, vi, v0, vm, vf,
                g_bn, w_bn, v_bn, w_bias, v_bias,
                o_ref, t0, t1, t2, t3, t4, t5, u0, u1, u2, u3, u4, u5, ns, no, ni, n0, nm, nf, so_ref, sv_ref,
                acc, rd, r1, r2, r3, grad, wbuf, vbuf, xbuf, dbuf, fcg,
                sums, nb, tr, sb, bias, snew, svnew,
                load_sem, ds_sem, dr_sem, s1_sem, p1_sem, s2_sem, p2_sem, s3_sem, p3_sem,
                w_sem, v_sem, x_sem, sm_send, sm_recv, so_send, so_recv, loc_sem, vn_sem, misc_sem,
                nb_send, nb_recv, a1_sem, a2_sem, a3_sem, ad_sem, as_sem,
                cd_sem, c1_sem, c2_sem, c3_sem):
    me = lax.axis_index('dp')
    core = me % 2
    chip = me // 2
    partner = me + 1 - 2 * core
    send_sems = (ds_sem, s1_sem, s2_sem, s3_sem)
    recv_sems = (dr_sem, p1_sem, p2_sem, p3_sem)
    ag_sems = (a1_sem, a2_sem, a3_sem)
    credits = (None, c1_sem, c2_sem, c3_sem)
    others = pl.ds(0, DEV - 1)

    def order(c):
        return strides(chip, c)

    def remote(src, dst, send, recv, dev):
        return pltpu.make_async_remote_copy(src_ref=src, dst_ref=dst, send_sem=send, recv_sem=recv,
                                            device_id=(dev,), device_id_type=MESH)

    def local(src, dst, sem):
        return pltpu.make_async_copy(src, dst, sem)

    def landed(ref, sem):
        local(ref, ref, sem).wait()

    def drain(n, sem):
        landed(o_ref.at[0, pl.ds(0, n)], sem)

    def signal(sem, dev):
        pl.semaphore_signal(sem, inc=1, device_id=(dev,), device_id_type=MESH)

    def loop(lo, hi, fn):
        def body(i, carry):
            fn(i)
            return carry

        lax.fori_loop(lo, hi, body, 0)

    def each_other(fn):
        loop(1, DEV, lambda d: fn((me + d) % DEV))

    def load_state(c):
        chunk_views(c, (ws, wo, wi, w0, wm), lambda view: local(view(me), wbuf.at[c], w_sem).start())
        strips(c, (vs, vo, vi, v0, vm), lambda src, dst: local(src, dst, v_sem).start())
        lane = aligned(me * LANES, LANES)

        def classifier(sizes):
            for i, size in enumerate(sizes):
                rows = pl.ds(pl.multiple_of((c - FC0) * LANES, LANES) + i * U, size)
                part = (c, pl.ds(0, size), pl.ds(i * LANES, LANES))
                local(wf.at[rows, lane], wbuf.at[part], w_sem).start()
                local(vf.at[rows], vbuf.at[part], v_sem).start()

        pl.when((c >= FC0) & (c < FCL))(functools.partial(classifier, (U, U, U, U)))
        pl.when(c == FCL)(functools.partial(classifier, (U, U, U, SUB)))

    def load_two(c):
        load_state(2 * c)
        load_state(2 * c + 1)

    def strips(c, refs, fn):
        for entry, ref in zip(TABLE, refs):
            first, stack, per, _ = entry

            @pl.when((c >= first) & (c < first + stack * per))
            def _():
                i, row, col = unit_at(entry, c)
                for b in range(CW // LANES):
                    fn(ref.at[aligned(row, U), col // LANES + b, i, 0, :], vbuf.at[c, :, pl.ds(b * LANES, LANES)])

    def state_wait():
        for buf, sem in ((wbuf, w_sem), (vbuf, v_sem)):
            landed(buf.at[pl.ds(0, NCH - 1)], sem)
            landed(buf.at[FCL, :, pl.ds(0, CW - LANES)], sem)
            landed(buf.at[FCL, pl.ds(0, SUB), pl.ds(CW - LANES, LANES)], sem)
            buf[FCL, SUB:, CW - LANES:] = jnp.zeros((U - SUB, LANES), F32)
        loop(0, NCH, weight_sums)

    def fc_block(b):
        y = jnp.dot(dbuf[...], xbuf[:, aligned(b * 2 * LANES, 2 * LANES)], preferred_element_type=F32)
        for h in range(2):
            part = y[:, h * LANES:(h + 1) * LANES]
            for g in range(CLASSES // U):
                fcg[g // 4, 2 * b + h, :, g % 4 * LANES:(g % 4 + 1) * LANES] = part[g * U:(g + 1) * U]
            fcg[FCN - 1, 2 * b + h, 0:SUB, CW - LANES:] = part[LASTROW:]
            fcg[FCN - 1, 2 * b + h, SUB:, CW - LANES:] = jnp.zeros((U - SUB, LANES), F32)

    def bias_out():
        line = jnp.dot(dbuf[...], jnp.ones((dbuf.shape[1], LANES), BF16), preferred_element_type=F32)
        square = (LANES, LANES)
        diagonal = lax.broadcasted_iota(jnp.int32, square, 0) == lax.broadcasted_iota(jnp.int32, square, 1)
        for i in range(SUB):
            part = line[i * LANES:min(CLASSES, (i + 1) * LANES)]
            bias[i:i + 1, :] = jnp.sum(jnp.where(diagonal[:part.shape[0]], part, 0.0), axis=0, keepdims=True)
        width = v_bias.shape[1]
        spread = (width, SUB * LANES)
        chosen = (lax.broadcasted_iota(jnp.int32, spread, 0) + me * width == lax.broadcasted_iota(jnp.int32, spread, 1))
        placed = jnp.dot(jnp.broadcast_to(v_bias[...], (SUB, width)), jnp.where(chosen, 1.0, 0.0),
                         precision=lax.Precision.HIGHEST, preferred_element_type=F32)
        for i in range(SUB):
            bias[SUB + i:SUB + i + 1, :] = placed[0:1, i * LANES:(i + 1) * LANES]
        sb[me, SUB:, :] = bias[...]
        each_other(lambda dev: remote(bias, sb.at[me, pl.ds(SUB, 2 * SUB)], sm_send, sm_recv, dev).start())

    def small_update():
        landed(sb.at[0, pl.ds(0, SUB)], misc_sem)
        landed(sb.at[others], sm_recv)
        landed(sb.at[others], sm_send)
        total = jnp.sum(sb[...], axis=0)
        rate = lr_ref[0, 0]
        v_new = MOMENTUM * v_bn[...] + rate * (total[0:SUB] * (1.0 / DEV))
        vb_new = MOMENTUM * total[2 * SUB:] + rate * (total[SUB:2 * SUB] * (1.0 / (DEV * dbuf.shape[1])))
        svnew[0:SUB, :] = v_new
        svnew[SUB:2 * SUB, :] = vb_new
        for i in range(SUB):
            part = w_bias[:, i * LANES:min(CLASSES, (i + 1) * LANES)]
            row = slice(2 * SUB + i, 2 * SUB + i + 1)
            svnew[row, :] = jnp.zeros((1, LANES), F32)
            svnew[row, :part.shape[1]] = part - vb_new[i:i + 1, :part.shape[1]]
        snew[...] = w_bn[aligned(me * SUB, SUB), :] - v_new

    def sent(slot):
        for level in range(4):
            drain(8 >> level, send_sems[level].at[slot])

    def rs_start(c):
        slot = c % NSLOT

        @pl.when(c >= NSLOT)
        def _():
            sent(slot)
            pl.semaphore_wait(cd_sem, 1)

        x1, x2, x3 = order(c)
        pieces = [(q, 2 * (chip + (q // 4) * x1 + ((q // 2) % 2) * x2 + (q % 2) * x3))
                  for q in (4, 5, 6, 7, 0, 1, 2, 3)]

        def to_partner(src, q):
            remote(src, rd.at[slot, q], ds_sem.at[slot], dr_sem.at[slot], partner).start()

        def go_all(view):
            for q, p in pieces:
                to_partner(view(p + 1 - core), q)
                local(view(p + core), acc.at[slot, q], load_sem.at[slot]).start()

        chunk_views(c, (gs, go, gi, g0, gm), go_all)

        @pl.when(is_fc(c))
        def _():
            for q, p in pieces:
                to_partner(fcg.at[c - FC0, p + 1 - core], q)
            for q, p in pieces:
                acc[slot, q] = fcg[c - FC0, p + core]

    def rs_fold(c, level):
        slot, half = c % NSLOT, 4 >> level
        came, going = (rd, r1, r2, r3)[level:level + 2]
        dev = 2 * (chip + order(c)[level]) + core
        if level == 0:
            @pl.when((c < FC0) | (c > FCL))
            def _():
                drain(8, load_sem.at[slot])
        drain(2 * half, recv_sems[level].at[slot])
        acc[slot, half:2 * half] = acc[slot, half:2 * half] + came[slot, half:2 * half]

        @pl.when(c >= NSLOT)
        def _():
            pl.semaphore_wait(credits[level + 1].at[c % 3], 1)

        remote(acc.at[slot, pl.ds(half, half)], going.at[slot], send_sems[level + 1].at[slot],
               recv_sems[level + 1].at[slot], dev).start()
        acc[slot, 0:half] = acc[slot, 0:half] + came[slot, 0:half]
        give_credit(c, level)

    def give_credit(c, level):
        @pl.when(c + NSLOT < NCH)
        def _():
            if level == 0:
                signal(cd_sem, partner)
            else:
                signal(credits[level].at[c % 3], 2 * (chip + order(c)[level - 1]) + core)

    def fold(x):
        y = jnp.sum(x * x, axis=0, keepdims=True)
        return sum(y[:, i:i + LANES] for i in range(0, CW, LANES))

    def rs_end(c):
        slot = c % NSLOT
        drain(1, recv_sems[3].at[slot])
        scale = jnp.where(is_fc(c), 1.0 / (DEV * dbuf.shape[1]), 1.0 / DEV).astype(F32)
        g = (acc[slot, 0] + r3[slot, 0]) * scale
        grad[c] = g
        t = tensor_of(c)
        sums[pl.ds(t, 1), :] = sums[pl.ds(t, 1), :] + fold(g)
        give_credit(c, 3)

    def weight_sums(c):
        t = pl.ds(SUB + tensor_of(c), 1)
        sums[t, :] = sums[t, :] + fold(wbuf[c])

    def norms_out(n):
        nb[n, me] = sums[...]
        each_other(lambda dev: remote(nb.at[n, me], nb.at[n, me], nb_send.at[n], nb_recv.at[n], dev).start())

    def norms_in(n):
        landed(nb.at[n, others], nb_recv.at[n])
        landed(nb.at[n, others], nb_send.at[n])
        total = jnp.sum(nb[n], axis=0)
        norm = jnp.sqrt(jnp.broadcast_to(jnp.sum(total, axis=1, keepdims=True), (2 * SUB, LANES)))
        g_norm, w_norm = norm[0:SUB], norm[SUB:]
        ratio = jnp.where((w_norm > 0) & (g_norm > 0), TRUST_COEF * w_norm / (g_norm + DECAY * w_norm), 1.0)
        tr[...] = lr_ref[0, 0] * ratio

    def update(a):
        rate = tr[pl.ds(tensor_of(a), 1), :]
        for i in range(0, CW, LANES):
            s = slice(i, i + LANES)
            w = wbuf[a, :, s]
            v = MOMENTUM * vbuf[a, :, s] + rate * (grad[a, :, s] + DECAY * w)
            vbuf[a, :, s] = v
            wbuf[a, :, s] = w - v

    def ag_send(src, dst, a, recv, dev):
        remote(src, dst, as_sem.at[a % NSEND], recv.at[a], dev).start()

    def ag_pass(a, n, dst, mirror, last):
        e = devices(me, order(a))
        level = n.bit_length() - 1
        held = [wbuf.at[a]] + [dst(e[q], q) for q in range(1, n)]
        if n > 1:
            drain(n // 2, ag_sems[level - 1].at[a])
        if not last:
            for q in range(n):
                ag_send(held[q], dst(e[q], q + n), a, ag_sems[level], e[n])
        for q in range(n // 2, n):
            ag_send(held[q], mirror(e[q], q), a, ad_sem, partner)
        if n == 1:
            local(wbuf.at[a], dst(me, 0), loc_sem).start()

    def gather(a, n):
        if n == 1:
            @pl.when(a >= NSEND)
            def _():
                pl.when(a - NSEND < TAIL0)(lambda: drain(DEV - 1, as_sem.at[a % NSEND]))
                pl.when(a - NSEND >= TAIL0)(lambda: drain(7, as_sem.at[a % NSEND]))

            strips(a, (ns, no, ni, n0, nm), lambda dst, src: local(src, dst, vn_sem).start())

        @pl.when(a < TAIL0)
        def _():
            ag_pass(a, n, lambda p, q: o_ref.at[a, p], lambda p, q: o_ref.at[a, p], n == 8)

        if n < 8:
            for j, (t, u) in enumerate(((t0, u0), (t1, u1), (t2, u2), (t3, u3), (t4, u4), (t5, u5))):
                first = TAIL0 + j // 3 * GROUP

                @pl.when((a >= first) & (a < first + GROUP) & (a % 3 == j % 3))
                def _():
                    k = (a - first) // 3
                    ag_pass(a, n, lambda p, q: t.at[k, q], lambda p, q: u.at[k, q], n == 4)

    def ag_end(a):
        pl.when(a < TAIL0)(lambda: drain(8, ad_sem.at[a]))
        pl.when(a >= TAIL0)(lambda: drain(4, ad_sem.at[a]))

    def stage(s, lag, fn, count=NCH):
        c = s - lag

        @pl.when((c >= 0) & (c < count))
        def _():
            fn(c)

    def start_small():
        each_other(lambda dev: remote(g_bn.at[dev], sb.at[me, pl.ds(0, SUB)], sm_send, sm_recv, dev).start())
        sums[...] = jnp.zeros_like(sums)

    def first_products():
        landed(dbuf, misc_sem)
        landed(xbuf, x_sem)
        local(g_bn.at[me], sb.at[me, pl.ds(0, SUB)], misc_sem).start()
        bias_out()

    def small_tensors():
        state_wait()
        small_update()

    def small_back():
        each_other(lambda dev: remote(snew, so_ref.at[me], so_send, so_recv, dev).start())
        local(snew, so_ref.at[me], misc_sem).start()
        local(svnew, sv_ref, x_sem).start()

    def fc_moments():
        for b in range(CLASSES // U):
            local(vbuf.at[FC0 + b // 4, :, pl.ds(b % 4 * LANES, LANES)], nf.at[pl.ds(b * U, U)], vn_sem).start()
        local(vbuf.at[FCL, pl.ds(0, SUB), pl.ds(CW - LANES, LANES)], nf.at[pl.ds(LASTROW, SUB)], vn_sem).start()

    def step(s):
        for at, fn in ((LOAD0, start_small), (MM0, first_products), (SMALL, small_tensors), (SMALL + 1, small_back),
                       (AG0 + FCL + 2, fc_moments)):
            pl.when(s == at)(fn)
        for n, at in enumerate((SPLIT, NCH)):
            pl.when(s == at + LAGS[3])(functools.partial(norms_out, n))
            pl.when(s == at + LAGS[3] + 4)(functools.partial(norms_in, n))
        stage(s, LAGS[3], rs_end)
        for level in (2, 1, 0):
            stage(s, LAGS[level], functools.partial(rs_fold, level=level))
        stage(s, 0, rs_start)
        stage(s, AG0 + AGEND, ag_end)
        for n, lag in AGLAGS[::-1]:
            stage(s, AG0 + lag, functools.partial(gather, n=n))
        stage(s, AG0 + FIRST, functools.partial(gather, n=1))
        stage(s, AG0, update)
        stage(s, MM0, fc_block, DEV // 2)
        stage(s, LOAD0, load_two, NCH // 2)

    local(d_ref, dbuf, misc_sem).start()
    local(x_ref, xbuf, x_sem).start()
    barrier = pltpu.get_barrier_semaphore()
    each_other(lambda dev: signal(barrier, dev))
    pl.semaphore_wait(barrier, DEV - 1)
    loop(0, AG0 + NCH + AGEND, step)

    loop(NCH - NSLOT, NCH, lambda c: sent(c % NSLOT))
    loop(NCH - NSEND, NCH, lambda a: drain(7, as_sem.at[a % NSEND]))
    landed(snew, misc_sem)
    landed(svnew, x_sem)
    landed(so_ref.at[others], so_recv)
    landed(so_ref.at[others], so_send)
    landed(wbuf, loc_sem)
    landed(vbuf.at[pl.ds(0, NCH - FCN)], vn_sem)
    landed(nf, vn_sem)


def run_comm(lr, grads, pooled, dlogits, weights, moments, small):
    unit = (U, CW)
    anyspec = pl.BlockSpec(memory_space=pl.ANY)
    vspec = pl.BlockSpec(memory_space=pltpu.VMEM)
    dma = pltpu.SemaphoreType.DMA
    reg = pltpu.SemaphoreType.REGULAR
    tile = (SUB, LANES)

    def vmem(*shape, dtype=F32):
        return pltpu.VMEM(shape, dtype)

    return pl.pallas_call(
        comm_kernel,
        out_shape=[jax.ShapeDtypeStruct(s, F32) for s in (
            [(TAIL0, DEV) + unit] + [(TAILK, 4) + unit] * 12 + [v.shape for v in moments] + [(DEV,) + tile, (3 * SUB, LANES)])],
        in_specs=[pl.BlockSpec(memory_space=pltpu.SMEM)] + [anyspec] * 20 + [vspec] * 4,
        out_specs=[anyspec] * 21,
        scratch_shapes=[vmem(NSLOT, n, *unit) for n in (8, 8, 4, 2, 1)] + [vmem(NCH, *unit)] * 3
        + [vmem(*pooled.shape, dtype=BF16), vmem(*dlogits.shape, dtype=BF16),
           vmem(FCN, DEV, *unit),
           vmem(2 * SUB, LANES), vmem(2, DEV, 2 * SUB, LANES), vmem(*tile),
           vmem(DEV, 3 * SUB, LANES), vmem(2 * SUB, LANES), vmem(*tile), vmem(3 * SUB, LANES)]
        + [dma((NSLOT,))] * 9 + [dma] * 10 + [dma((2,))] * 2 + [dma((NCH,))] * 4 + [dma((NSEND,))]
        + [reg] + [reg((3,))] * 3,
        compiler_params=pltpu.CompilerParams(collective_id=0, has_side_effects=True,
                                             vmem_limit_bytes=60 * 1024 * 1024),
        name='lars_comm',
    )(lr, *grads, pooled, dlogits, *weights, *moments, *small)


NBUF = 12
AHEAD = 6
NFC = 4
WRITE_FLOPS = 10 ** 8
VMEM = 67043328


def write_kernel(o_ref, ns, no, ni, n0, nm, so_ref, sv_ref, os_, oo, of, bs, bo, bf,
                 vs, vo, vi, v0, vm, bn, vbn, wb,
                 buf, bbuf, fbuf, fbbuf, vbuf, in_sem, f_sem, b_sem, v_sem):
    def view(c, refs):
        entry, ref = [(e, r) for e, r in zip(TABLE, refs) if c >= e[0]][-1]
        i, row, col = unit_at(entry, c)
        return ref.at[i, :, pl.ds(row, U), pl.ds(col, CW)]

    def load(i):
        return [pltpu.make_async_copy(o_ref.at[i], buf.at[i % NBUF], in_sem.at[i % NBUF])]

    def stores(i):
        slot = i % NBUF
        if not FC0 <= i <= FCL:
            pairs = [(buf.at[slot], view(i, (os_, oo))), (bbuf.at[slot], view(i, (bs, bo)))]
        else:
            size = min(LANES, CLASSES - LANES * (i - FC0))
            have, want = pl.ds(0, size), pl.ds(LANES * (i - FC0), size)
            pairs = [(fbuf.at[i % NFC, have], of.at[want]), (fbbuf.at[i % NFC, have], bf.at[want])]
        return [pltpu.make_async_copy(*pairs[0], f_sem.at[slot]), pltpu.make_async_copy(*pairs[1], b_sem.at[slot])]

    done = []

    def settle(upto):
        while len(done) <= upto:
            for d in stores(len(done)):
                d.wait()
            done.append(True)

    for i in range(AHEAD):
        for d in load(i):
            d.start()
    sizes = [e[1] * e[2] * LANES for e in TABLE]
    firsts = [sum(sizes[:n]) for n in range(len(sizes))]

    def moments(refs, back):
        out = []
        for first, ref in zip(firsts, refs):
            pair = (ref, vbuf.at[pl.ds(first, ref.shape[0])])
            out.append(pltpu.make_async_copy(*(pair[::-1] if back else pair), v_sem))
        return out

    v_ins, v_outs = moments((ns, no, ni, n0, nm), False), moments((vs, vo, vi, v0, vm), True)
    for d in v_ins:
        d.start()
    bn[...] = so_ref[...]
    vbn[...] = sv_ref[0:SUB]
    for i in range(SUB):
        lanes = slice(i * LANES, min(CLASSES, (i + 1) * LANES))
        wb[:, lanes] = sv_ref[2 * SUB + i:2 * SUB + i + 1, :lanes.stop - lanes.start]
    for i in range(TAIL0):
        slot = i % NBUF
        for d in load(i):
            d.wait()
        if not FC0 <= i <= FCL:
            def cast(p, _):
                bbuf[slot, p] = buf[slot, p].astype(BF16)
                return 0

            lax.fori_loop(0, DEV, cast, 0)
        else:
            settle(i - NFC)
            for p in range(DEV):
                for r in range(CW // LANES):
                    x = buf[slot, p, :, LANES * r:LANES * (r + 1)]
                    at = (slice(U * r, U * (r + 1)), slice(LANES * p, LANES * (p + 1)))
                    fbuf[(i % NFC,) + at] = x
                    fbbuf[(i % NFC,) + at] = x.astype(BF16)
        for d in stores(i):
            d.start()
        if i == AHEAD:
            for d in v_ins:
                d.wait()
            for d in v_outs:
                d.start()
        if i + AHEAD < TAIL0:
            settle(i + AHEAD - NBUF)
            for d in load(i + AHEAD):
                d.start()
    settle(TAIL0 - 1)
    for d in v_outs:
        d.wait()


def run_write(o, moments_new, so, sv):
    anyspec = pl.BlockSpec(memory_space=pl.ANY)
    vspec = pl.BlockSpec(memory_space=pltpu.VMEM)
    shapes = [dshape(*e, DEV) for e in TABLE[:2]] + [(CLASSES, DEV * LANES)]
    moments = [(e[1] * e[2] * LANES, LANES) for e in TABLE]
    tile = (SUB, LANES)
    dma = pltpu.SemaphoreType.DMA
    outs = [(s, F32) for s in shapes] + [(s, BF16) for s in shapes] + [(s, F32) for s in moments]
    outs += [((DEV,) + tile, F32), (tile, F32), ((1, CLASSES), F32)]
    return pl.pallas_call(
        write_kernel,
        out_shape=[jax.ShapeDtypeStruct(*s) for s in outs],
        in_specs=[anyspec] * 6 + [vspec] * 2,
        out_specs=[anyspec] * 11 + [vspec] * 3,
        scratch_shapes=[
            pltpu.VMEM((NBUF, DEV, U, CW), F32), pltpu.VMEM((NBUF, DEV, U, CW), BF16),
            pltpu.VMEM((NFC, LANES, DEV * LANES), F32), pltpu.VMEM((NFC, LANES, DEV * LANES), BF16),
            pltpu.VMEM(((NCH - FCN) * LANES, LANES), F32),
            dma((NBUF,)), dma((NBUF,)), dma((NBUF,)), dma],
        compiler_params=pltpu.CompilerParams(vmem_limit_bytes=VMEM),
        cost_estimate=pl.CostEstimate(flops=WRITE_FLOPS, bytes_accessed=TAIL0 * 160 * U * CW, transcendentals=0),
        name='write_out',
    )(o, *moments_new, so, sv)


TBUF, TAHEAD = 16, 10


def tail_kernel(jobs, size, count, aliased, *refs):
    srcs, refs = refs[:count], refs[count + 7 * aliased:]
    fulls, halves, (token, buf, bbuf, in_sem, f_sem, b_sem) = refs[:3], refs[3:6], refs[6:]
    me = lax.axis_index('dp')
    mate = 1 - 2 * (me % 2)
    ring = buf.shape[0]
    token[...] = jnp.zeros_like(token)

    def load(n):
        return [pltpu.make_async_copy(srcs[src].at[k], buf.at[n % ring, pl.ds(4 * j, 4)], in_sem.at[n % ring])
                for j, (src, k, _, _) in enumerate(jobs[n][1])]

    def store(n):
        slot = n % ring
        c, parts = jobs[n]
        e = devices(me, strides(me // 2, c % 3))
        entry, full, half = [x for x in zip(TABLE[2:], fulls, halves) if c >= x[0][0]][-1]
        i, row, _ = unit_at(entry, c)
        for j, (_, _, base, other) in enumerate(parts):
            for q in range(4):
                p = e[base + q] + mate * other
                at = (i, p, pl.ds(row, U))
                pltpu.make_async_copy(buf.at[slot, 4 * j + q], full.at[at], f_sem.at[slot]).start()
                pltpu.make_async_copy(bbuf.at[slot, 4 * j + q], half.at[at], b_sem.at[slot]).start()

    def settled(n):
        for ref, sem in ((buf, f_sem), (bbuf, b_sem)):
            pltpu.make_async_copy(ref.at[n % ring], ref.at[n % ring], sem.at[n % ring]).wait()

    total = len(jobs)
    ahead = ring if ring == total else TAHEAD
    for n in range(ahead):
        for d in load(n):
            d.start()
    for n in range(total):
        slot = n % ring
        for d in load(n):
            d.wait()

        def cast(p, _):
            bbuf[slot, p] = buf[slot, p].astype(BF16)
            return 0

        lax.fori_loop(0, size, cast, 0)
        store(n)
        nxt = n + ahead
        if nxt < total:
            if nxt >= ring:
                settled(nxt - ring)
            for d in load(nxt):
                d.start()
    for n in range(max(0, total - ring), total):
        settled(n)


def run_tail(groups, sets, arrays):
    anyspec = pl.BlockSpec(memory_space=pl.ANY)
    dma = pltpu.SemaphoreType.DMA
    size = 4 * len(sets)
    srcs, jobs = [], []
    for g in groups:
        base = len(srcs)
        for arrs, _, _ in sets:
            srcs += arrs[3 * g:3 * g + 3]
        for n in range(GROUP):
            jobs.append((TAIL0 + g * GROUP + n, [(base + 3 * j + n % 3, n // 3, first, other)
                                                 for j, (_, first, other) in enumerate(sets)]))
    ring = min(len(jobs), TBUF)
    count = len(srcs)
    given = list(arrays or [])[:6]
    tokens = list(arrays or [])[6:]
    shapes = [dshape(*e, DEV) for e in TABLE[2:]]
    outs = [jax.ShapeDtypeStruct(s, t) for t in (F32, BF16) for s in shapes]
    return pl.pallas_call(
        functools.partial(tail_kernel, jobs, size, count, len(given) > 0),
        out_shape=outs + [jax.ShapeDtypeStruct((SUB, LANES), F32)],
        in_specs=[anyspec] * (count + len(given) + len(tokens)),
        out_specs=[anyspec] * 6 + [pl.BlockSpec(memory_space=pltpu.VMEM)],
        input_output_aliases={count + n: n for n in range(len(given))},
        scratch_shapes=[pltpu.VMEM((ring, size, U, CW), F32), pltpu.VMEM((ring, size, U, CW), BF16),
                        dma((ring,)), dma((ring,)), dma((ring,))],
        compiler_params=pltpu.CompilerParams(vmem_limit_bytes=VMEM),
        cost_estimate=pl.CostEstimate(flops=WRITE_FLOPS // 3, bytes_accessed=len(jobs) * size * 10 * U * CW,
                                      transcendentals=0),
    )(*srcs, *given, *tokens)


def solution(mesh):
    n_dev = mesh.shape['dp']
    assert n_dev == DEV
    full, lead, cols = P(), P('dp'), P(None, 'dp')
    moment_specs = (lead, lead, cols, cols, cols, lead, lead, lead)
    in_specs = (full,) * 8 + (lead,) * 8 + moment_specs + (full,)
    out_specs = (full,) * 14 + moment_specs

    def body(w_in0, w_short, w_in, w_mid, w_out, w_fc, w_bn, w_bias,
             g_in0, g_short, g_in, g_mid, g_out, g_bn, pooled, dlogits,
             v_in0, v_short, v_in, v_mid, v_out, v_fc, v_bn, v_bias, learn_rate):
        rank = lax.axis_index('dp')
        width = v_bias.shape[0]
        shapes = [dshape(*e, DEV) for e in TABLE]
        grads = [g.reshape(s) for g, s in zip((g_short, g_out, g_in, g_in0, g_mid), shapes)]
        weights = [w.reshape(s) for w, s in zip((w_short, w_out, w_in, w_in0, w_mid), shapes)] + [w_fc.T]

        def to_rows(v, entry):
            _, stack, _, blocks = entry
            return v.reshape(stack, -1, LANES).transpose(1, 0, 2).reshape(-1, blocks * CW // LANES, stack, 1, LANES)

        def from_rows(v, stack, like):
            return v.reshape(-1, stack, LANES).transpose(1, 0, 2).reshape(like.shape)

        olds = (v_short, v_out, v_in, v_in0, v_mid)
        moments = [to_rows(v, e) for v, e in zip(olds, TABLE)]
        moments.append(v_fc.reshape(LANES, CLASSES).T)
        tiles = (-1, SUB, LANES)
        small = [g_bn.reshape(tiles), w_bn.reshape(-1, LANES), v_bn.reshape(SUB, LANES),
                 w_bias.reshape(1, CLASSES), v_bias.reshape(1, width)]
        o, *made, nf, so, sv = run_comm(
            learn_rate.reshape(1, 1), grads, pooled, dlogits.T, weights, moments, small)
        ts, us, made = made[:6], made[6:12], made[12:]

        def across(x, weight):
            return lax.ppermute(x, 'dp', [(i, i ^ weight) for i in range(DEV)])

        def to_mates(arrs, token):
            *held, token = lax.optimization_barrier((*arrs, token))
            return [across(r, 1) for r in held], token

        rs = []
        for n, t in enumerate(ts):
            rs.append(across(t, 2 << (n + 2) % 3))
        outs = run_write(o, [v.reshape(-1, LANES) for v in made], so, sv)
        short, out, fc, short_b, out_b, fc_b, vs, vo, vi, v0, vm, bn, vbn, wb = outs
        mates, vbn = to_mates(rs[:3], vbn)
        tail = run_tail((0, 1), [(ts, 0, False), (us, 0, True)], None)
        *tail, token = run_tail((0,), [(rs, 4, False), (mates, 4, True)], tail)
        last, token = to_mates(rs[3:], token)
        tail = run_tail((1,), [(rs, 4, False)], (*tail, token))
        *tail, _ = run_tail((1,), [(mates + last, 4, True)], tail)
        inn, in0, mid, inn_b, in0_b, mid_b = tail
        news = [from_rows(v, e[1], old) for v, e, old in zip((vs, vo, vi, v0, vm), TABLE, olds)]
        vb = sv[SUB:2 * SUB]
        return (in0.reshape(w_in0.shape), short.reshape(w_short.shape), inn.reshape(w_in.shape),
                mid.reshape(w_mid.shape), out.reshape(w_out.shape), fc.T,
                bn.reshape(w_bn.shape), wb.reshape(w_bias.shape),
                in0_b.reshape(w_in0.shape), short_b.reshape(w_short.shape), inn_b.reshape(w_in.shape),
                mid_b.reshape(w_mid.shape), out_b.reshape(w_out.shape), fc_b.T,
                news[3], news[0], news[2], news[4], news[1], nf.T.reshape(v_fc.shape),
                vbn.reshape(v_bn.shape), lax.dynamic_slice_in_dim(vb.reshape(-1), rank * width, width))

    return jax.shard_map(body, mesh=mesh, in_specs=in_specs, out_specs=out_specs, check_vma=False)
```

```python
import functools
import jax
import jax.numpy as jnp
from jax import lax
from jax.experimental import pallas as pl
from jax.experimental.pallas import tpu as pltpu
from jax.sharding import PartitionSpec as P

MOMENTUM = 0.9
TRUST_COEF = 0.001
DECAY = 0.0001


MESH = pl.DeviceIdType.MESH
F32, BF16 = jnp.float32, jnp.bfloat16
DEV = 16
LANES = 128
U, CW = 32, 512
NCH = 48
FC0, FCN = 16, 8
FCL = FC0 + FCN - 1
CLASSES, LASTROW = 1000, 992
SUB = 8
TABLE = ((0, 1, 8, 4), (8, 2, 4, 4), (24, 1, 4, 1), (28, 1, 2, 1), (30, 2, 9, 1))
STARTS = (8, 12, FC0, 24, 28, 30, 39)
TAIL0 = 24
GROUP = 12
TAILK = GROUP // 3
SPLIT = 24
NSLOT = 15
LAGS = (3, 9, 12, 14)
AG0 = 45
FIRST = 1
AGLAGS = ((2, 6), (4, 12), (8, 18))
AGEND = 21
NSEND = 18
LOAD0 = 6
MM0 = 6
SMALL = 34


def tensor_of(c):
    return sum(jnp.where(c >= first, 1, 0) for first in STARTS)


def dshape(first, stack, per, blocks, lead):
    return (stack, lead, per // blocks * U, blocks * CW)


def unit_at(entry, c):
    first, _, per, blocks = entry
    k = (c - first) % per
    return (c - first) // per, k // blocks * U, k % blocks * CW


def is_fc(c):
    return (c >= FC0) & (c <= FCL)


def strides(chip, c):
    steps = []
    for i in range(3):
        d = (c + i) % 3
        weight = 1 + d + (d * (d - 1)) // 2
        steps.append(weight * (1 - 2 * ((chip // weight) % 2)))
    return steps


def devices(me, steps):
    x1, x2, x3 = steps
    return [me + 2 * ((q % 2) * x1 + ((q // 2) % 2) * x2 + (q // 4) * x3) for q in range(8)]


def aligned(x, size):
    return pl.ds(x if isinstance(x, int) else pl.multiple_of(x, size), size)


def chunk_views(c, refs, fn):
    for entry, ref in zip(TABLE, refs):
        first, stack, per, _ = entry

        @pl.when((c >= first) & (c < first + stack * per))
        def _():
            i, row, col = unit_at(entry, c)
            fn(lambda p: ref.at[i, p, aligned(row, U), aligned(col, CW)])


def comm_kernel(lr_ref, gs, go, gi, g0, gm, x_ref, d_ref, ws, wo, wi, w0, wm, wf, vs, vo, vi, v0, vm, vf,
                g_bn, w_bn, v_bn, w_bias, v_bias,
                o_ref, t0, t1, t2, t3, t4, t5, u0, u1, u2, u3, u4, u5, ns, no, ni, n0, nm, nf, so_ref, sv_ref,
                acc, rd, r1, r2, r3, grad, wbuf, vbuf, xbuf, dbuf, fcg,
                sums, nb, tr, sb, bias, snew, svnew,
                load_sem, ds_sem, dr_sem, s1_sem, p1_sem, s2_sem, p2_sem, s3_sem, p3_sem,
                w_sem, v_sem, x_sem, sm_send, sm_recv, so_send, so_recv, loc_sem, vn_sem, misc_sem,
                nb_send, nb_recv, a1_sem, a2_sem, a3_sem, ad_sem, as_sem,
                cd_sem, c1_sem, c2_sem, c3_sem):
    me = lax.axis_index('dp')
    core = me % 2
    chip = me // 2
    partner = me + 1 - 2 * core
    send_sems = (ds_sem, s1_sem, s2_sem, s3_sem)
    recv_sems = (dr_sem, p1_sem, p2_sem, p3_sem)
    ag_sems = (a1_sem, a2_sem, a3_sem)
    credits = (None, c1_sem, c2_sem, c3_sem)
    others = pl.ds(0, DEV - 1)

    def order(c):
        return strides(chip, c)

    def remote(src, dst, send, recv, dev):
        return pltpu.make_async_remote_copy(src_ref=src, dst_ref=dst, send_sem=send, recv_sem=recv,
                                            device_id=(dev,), device_id_type=MESH)

    def local(src, dst, sem):
        return pltpu.make_async_copy(src, dst, sem)

    def landed(ref, sem):
        local(ref, ref, sem).wait()

    def drain(n, sem):
        landed(o_ref.at[0, pl.ds(0, n)], sem)

    def signal(sem, dev):
        pl.semaphore_signal(sem, inc=1, device_id=(dev,), device_id_type=MESH)

    def loop(lo, hi, fn):
        def body(i, carry):
            fn(i)
            return carry

        lax.fori_loop(lo, hi, body, 0)

    def each_other(fn):
        loop(1, DEV, lambda d: fn((me + d) % DEV))

    def load_state(c):
        chunk_views(c, (ws, wo, wi, w0, wm), lambda view: local(view(me), wbuf.at[c], w_sem).start())
        strips(c, (vs, vo, vi, v0, vm), lambda src, dst: local(src, dst, v_sem).start())
        lane = aligned(me * LANES, LANES)

        def classifier(sizes):
            for i, size in enumerate(sizes):
                rows = pl.ds(pl.multiple_of((c - FC0) * LANES, LANES) + i * U, size)
                part = (c, pl.ds(0, size), pl.ds(i * LANES, LANES))
                local(wf.at[rows, lane], wbuf.at[part], w_sem).start()
                local(vf.at[rows], vbuf.at[part], v_sem).start()

        pl.when((c >= FC0) & (c < FCL))(functools.partial(classifier, (U, U, U, U)))
        pl.when(c == FCL)(functools.partial(classifier, (U, U, U, SUB)))

    def load_two(c):
        load_state(2 * c)
        load_state(2 * c + 1)

    def strips(c, refs, fn):
        for entry, ref in zip(TABLE, refs):
            first, stack, per, _ = entry

            @pl.when((c >= first) & (c < first + stack * per))
            def _():
                i, row, col = unit_at(entry, c)
                for b in range(CW // LANES):
                    fn(ref.at[aligned(row, U), col // LANES + b, i, 0, :], vbuf.at[c, :, pl.ds(b * LANES, LANES)])

    def state_wait():
        for buf, sem in ((wbuf, w_sem), (vbuf, v_sem)):
            landed(buf.at[pl.ds(0, NCH - 1)], sem)
            landed(buf.at[FCL, :, pl.ds(0, CW - LANES)], sem)
            landed(buf.at[FCL, pl.ds(0, SUB), pl.ds(CW - LANES, LANES)], sem)
            buf[FCL, SUB:, CW - LANES:] = jnp.zeros((U - SUB, LANES), F32)
        loop(0, NCH, weight_sums)

    def fc_block(b):
        y = jnp.dot(dbuf[...], xbuf[:, aligned(b * 2 * LANES, 2 * LANES)], preferred_element_type=F32)
        for h in range(2):
            part = y[:, h * LANES:(h + 1) * LANES]
            for g in range(CLASSES // U):
                fcg[g // 4, 2 * b + h, :, g % 4 * LANES:(g % 4 + 1) * LANES] = part[g * U:(g + 1) * U]
            fcg[FCN - 1, 2 * b + h, 0:SUB, CW - LANES:] = part[LASTROW:]
            fcg[FCN - 1, 2 * b + h, SUB:, CW - LANES:] = jnp.zeros((U - SUB, LANES), F32)

    def bias_out():
        line = jnp.dot(dbuf[...], jnp.ones((dbuf.shape[1], LANES), BF16), preferred_element_type=F32)
        square = (LANES, LANES)
        diagonal = lax.broadcasted_iota(jnp.int32, square, 0) == lax.broadcasted_iota(jnp.int32, square, 1)
        for i in range(SUB):
            part = line[i * LANES:min(CLASSES, (i + 1) * LANES)]
            bias[i:i + 1, :] = jnp.sum(jnp.where(diagonal[:part.shape[0]], part, 0.0), axis=0, keepdims=True)
        width = v_bias.shape[1]
        spread = (width, SUB * LANES)
        chosen = (lax.broadcasted_iota(jnp.int32, spread, 0) + me * width == lax.broadcasted_iota(jnp.int32, spread, 1))
        placed = jnp.dot(jnp.broadcast_to(v_bias[...], (SUB, width)), jnp.where(chosen, 1.0, 0.0),
                         precision=lax.Precision.HIGHEST, preferred_element_type=F32)
        for i in range(SUB):
            bias[SUB + i:SUB + i + 1, :] = placed[0:1, i * LANES:(i + 1) * LANES]
        sb[me, SUB:, :] = bias[...]
        each_other(lambda dev: remote(bias, sb.at[me, pl.ds(SUB, 2 * SUB)], sm_send, sm_recv, dev).start())

    def small_update():
        landed(sb.at[0, pl.ds(0, SUB)], misc_sem)
        landed(sb.at[others], sm_recv)
        landed(sb.at[others], sm_send)
        total = jnp.sum(sb[...], axis=0)
        rate = lr_ref[0, 0]
        v_new = MOMENTUM * v_bn[...] + rate * (total[0:SUB] * (1.0 / DEV))
        vb_new = MOMENTUM * total[2 * SUB:] + rate * (total[SUB:2 * SUB] * (1.0 / (DEV * dbuf.shape[1])))
        svnew[0:SUB, :] = v_new
        svnew[SUB:2 * SUB, :] = vb_new
        for i in range(SUB):
            part = w_bias[:, i * LANES:min(CLASSES, (i + 1) * LANES)]
            row = slice(2 * SUB + i, 2 * SUB + i + 1)
            svnew[row, :] = jnp.zeros((1, LANES), F32)
            svnew[row, :part.shape[1]] = part - vb_new[i:i + 1, :part.shape[1]]
        snew[...] = w_bn[aligned(me * SUB, SUB), :] - v_new

    def sent(slot):
        for level in range(4):
            drain(8 >> level, send_sems[level].at[slot])

    def rs_start(c):
        slot = c % NSLOT

        @pl.when(c >= NSLOT)
        def _():
            sent(slot)
            pl.semaphore_wait(cd_sem, 1)

        x1, x2, x3 = order(c)
        pieces = [(q, 2 * (chip + (q // 4) * x1 + ((q // 2) % 2) * x2 + (q % 2) * x3))
                  for q in (4, 5, 6, 7, 0, 1, 2, 3)]

        def to_partner(src, q):
            remote(src, rd.at[slot, q], ds_sem.at[slot], dr_sem.at[slot], partner).start()

        def go_all(view):
            for q, p in pieces:
                to_partner(view(p + 1 - core), q)
                local(view(p + core), acc.at[slot, q], load_sem.at[slot]).start()

        chunk_views(c, (gs, go, gi, g0, gm), go_all)

        @pl.when(is_fc(c))
        def _():
            for q, p in pieces:
                to_partner(fcg.at[c - FC0, p + 1 - core], q)
            for q, p in pieces:
                acc[slot, q] = fcg[c - FC0, p + core]

    def rs_fold(c, level):
        slot, half = c % NSLOT, 4 >> level
        came, going = (rd, r1, r2, r3)[level:level + 2]
        dev = 2 * (chip + order(c)[level]) + core
        if level == 0:
            @pl.when((c < FC0) | (c > FCL))
            def _():
                drain(8, load_sem.at[slot])
        drain(2 * half, recv_sems[level].at[slot])
        acc[slot, half:2 * half] = acc[slot, half:2 * half] + came[slot, half:2 * half]

        @pl.when(c >= NSLOT)
        def _():
            pl.semaphore_wait(credits[level + 1].at[c % 3], 1)

        remote(acc.at[slot, pl.ds(half, half)], going.at[slot], send_sems[level + 1].at[slot],
               recv_sems[level + 1].at[slot], dev).start()
        acc[slot, 0:half] = acc[slot, 0:half] + came[slot, 0:half]
        give_credit(c, level)

    def give_credit(c, level):
        @pl.when(c + NSLOT < NCH)
        def _():
            if level == 0:
                signal(cd_sem, partner)
            else:
                signal(credits[level].at[c % 3], 2 * (chip + order(c)[level - 1]) + core)

    def fold(x):
        y = jnp.sum(x * x, axis=0, keepdims=True)
        return sum(y[:, i:i + LANES] for i in range(0, CW, LANES))

    def rs_end(c):
        slot = c % NSLOT
        drain(1, recv_sems[3].at[slot])
        scale = jnp.where(is_fc(c), 1.0 / (DEV * dbuf.shape[1]), 1.0 / DEV).astype(F32)
        g = (acc[slot, 0] + r3[slot, 0]) * scale
        grad[c] = g
        t = tensor_of(c)
        sums[pl.ds(t, 1), :] = sums[pl.ds(t, 1), :] + fold(g)
        give_credit(c, 3)

    def weight_sums(c):
        t = pl.ds(SUB + tensor_of(c), 1)
        sums[t, :] = sums[t, :] + fold(wbuf[c])

    def norms_out(n):
        nb[n, me] = sums[...]
        each_other(lambda dev: remote(nb.at[n, me], nb.at[n, me], nb_send.at[n], nb_recv.at[n], dev).start())

    def norms_in(n):
        landed(nb.at[n, others], nb_recv.at[n])
        landed(nb.at[n, others], nb_send.at[n])
        total = jnp.sum(nb[n], axis=0)
        norm = jnp.sqrt(jnp.broadcast_to(jnp.sum(total, axis=1, keepdims=True), (2 * SUB, LANES)))
        g_norm, w_norm = norm[0:SUB], norm[SUB:]
        ratio = jnp.where((w_norm > 0) & (g_norm > 0), TRUST_COEF * w_norm / (g_norm + DECAY * w_norm), 1.0)
        tr[...] = lr_ref[0, 0] * ratio

    def update(a):
        rate = tr[pl.ds(tensor_of(a), 1), :]
        for i in range(0, CW, LANES):
            s = slice(i, i + LANES)
            w = wbuf[a, :, s]
            v = MOMENTUM * vbuf[a, :, s] + rate * (grad[a, :, s] + DECAY * w)
            vbuf[a, :, s] = v
            wbuf[a, :, s] = w - v

    def ag_send(src, dst, a, recv, dev):
        remote(src, dst, as_sem.at[a % NSEND], recv.at[a], dev).start()

    def ag_pass(a, n, dst, mirror, last):
        e = devices(me, order(a))
        level = n.bit_length() - 1
        held = [wbuf.at[a]] + [dst(e[q], q) for q in range(1, n)]
        if n > 1:
            drain(n // 2, ag_sems[level - 1].at[a])
        if not last:
            for q in range(n):
                ag_send(held[q], dst(e[q], q + n), a, ag_sems[level], e[n])
        for q in range(n // 2, n):
            ag_send(held[q], mirror(e[q], q), a, ad_sem, partner)
        if n == 1:
            local(wbuf.at[a], dst(me, 0), loc_sem).start()

    def gather(a, n):
        if n == 1:
            @pl.when(a >= NSEND)
            def _():
                pl.when(a - NSEND < TAIL0)(lambda: drain(DEV - 1, as_sem.at[a % NSEND]))
                pl.when(a - NSEND >= TAIL0)(lambda: drain(7, as_sem.at[a % NSEND]))

            strips(a, (ns, no, ni, n0, nm), lambda dst, src: local(src, dst, vn_sem).start())

        @pl.when(a < TAIL0)
        def _():
            ag_pass(a, n, lambda p, q: o_ref.at[a, p], lambda p, q: o_ref.at[a, p], n == 8)

        if n < 8:
            for j, (t, u) in enumerate(((t0, u0), (t1, u1), (t2, u2), (t3, u3), (t4, u4), (t5, u5))):
                first = TAIL0 + j // 3 * GROUP

                @pl.when((a >= first) & (a < first + GROUP) & (a % 3 == j % 3))
                def _():
                    k = (a - first) // 3
                    ag_pass(a, n, lambda p, q: t.at[k, q], lambda p, q: u.at[k, q], n == 4)

    def ag_end(a):
        pl.when(a < TAIL0)(lambda: drain(8, ad_sem.at[a]))
        pl.when(a >= TAIL0)(lambda: drain(4, ad_sem.at[a]))

    def stage(s, lag, fn, count=NCH):
        c = s - lag

        @pl.when((c >= 0) & (c < count))
        def _():
            fn(c)

    def start_small():
        each_other(lambda dev: remote(g_bn.at[dev], sb.at[me, pl.ds(0, SUB)], sm_send, sm_recv, dev).start())
        sums[...] = jnp.zeros_like(sums)

    def first_products():
        landed(dbuf, misc_sem)
        landed(xbuf, x_sem)
        local(g_bn.at[me], sb.at[me, pl.ds(0, SUB)], misc_sem).start()
        bias_out()

    def small_tensors():
        state_wait()
        small_update()

    def small_back():
        each_other(lambda dev: remote(snew, so_ref.at[me], so_send, so_recv, dev).start())
        local(snew, so_ref.at[me], misc_sem).start()
        local(svnew, sv_ref, x_sem).start()

    def fc_moments():
        for b in range(CLASSES // U):
            local(vbuf.at[FC0 + b // 4, :, pl.ds(b % 4 * LANES, LANES)], nf.at[pl.ds(b * U, U)], vn_sem).start()
        local(vbuf.at[FCL, pl.ds(0, SUB), pl.ds(CW - LANES, LANES)], nf.at[pl.ds(LASTROW, SUB)], vn_sem).start()

    def step(s):
        for at, fn in ((LOAD0, start_small), (MM0, first_products), (SMALL, small_tensors), (SMALL + 1, small_back),
                       (AG0 + FCL + 2, fc_moments)):
            pl.when(s == at)(fn)
        for n, at in enumerate((SPLIT, NCH)):
            pl.when(s == at + LAGS[3])(functools.partial(norms_out, n))
            pl.when(s == at + LAGS[3] + 4)(functools.partial(norms_in, n))
        stage(s, LAGS[3], rs_end)
        for level in (2, 1, 0):
            stage(s, LAGS[level], functools.partial(rs_fold, level=level))
        stage(s, 0, rs_start)
        stage(s, AG0 + AGEND, ag_end)
        for n, lag in AGLAGS[::-1]:
            stage(s, AG0 + lag, functools.partial(gather, n=n))
        stage(s, AG0 + FIRST, functools.partial(gather, n=1))
        stage(s, AG0, update)
        stage(s, MM0, fc_block, DEV // 2)
        stage(s, LOAD0, load_two, NCH // 2)

    local(d_ref, dbuf, misc_sem).start()
    local(x_ref, xbuf, x_sem).start()
    barrier = pltpu.get_barrier_semaphore()
    each_other(lambda dev: signal(barrier, dev))
    pl.semaphore_wait(barrier, DEV - 1)
    loop(0, AG0 + NCH + AGEND, step)

    loop(NCH - NSLOT, NCH, lambda c: sent(c % NSLOT))
    loop(NCH - NSEND, NCH, lambda a: drain(7, as_sem.at[a % NSEND]))
    landed(snew, misc_sem)
    landed(svnew, x_sem)
    landed(so_ref.at[others], so_recv)
    landed(so_ref.at[others], so_send)
    landed(wbuf, loc_sem)
    landed(vbuf.at[pl.ds(0, NCH - FCN)], vn_sem)
    landed(nf, vn_sem)


def run_comm(lr, grads, pooled, dlogits, weights, moments, small):
    unit = (U, CW)
    anyspec = pl.BlockSpec(memory_space=pl.ANY)
    vspec = pl.BlockSpec(memory_space=pltpu.VMEM)
    dma = pltpu.SemaphoreType.DMA
    reg = pltpu.SemaphoreType.REGULAR
    tile = (SUB, LANES)

    def vmem(*shape, dtype=F32):
        return pltpu.VMEM(shape, dtype)

    return pl.pallas_call(
        comm_kernel,
        out_shape=[jax.ShapeDtypeStruct(s, F32) for s in (
            [(TAIL0, DEV) + unit] + [(TAILK, 4) + unit] * 12 + [v.shape for v in moments] + [(DEV,) + tile, (3 * SUB, LANES)])],
        in_specs=[pl.BlockSpec(memory_space=pltpu.SMEM)] + [anyspec] * 20 + [vspec] * 4,
        out_specs=[anyspec] * 21,
        scratch_shapes=[vmem(NSLOT, n, *unit) for n in (8, 8, 4, 2, 1)] + [vmem(NCH, *unit)] * 3
        + [vmem(*pooled.shape, dtype=BF16), vmem(*dlogits.shape, dtype=BF16),
           vmem(FCN, DEV, *unit),
           vmem(2 * SUB, LANES), vmem(2, DEV, 2 * SUB, LANES), vmem(*tile),
           vmem(DEV, 3 * SUB, LANES), vmem(2 * SUB, LANES), vmem(*tile), vmem(3 * SUB, LANES)]
        + [dma((NSLOT,))] * 9 + [dma] * 10 + [dma((2,))] * 2 + [dma((NCH,))] * 4 + [dma((NSEND,))]
        + [reg] + [reg((3,))] * 3,
        compiler_params=pltpu.CompilerParams(collective_id=0, has_side_effects=True,
                                             vmem_limit_bytes=60 * 1024 * 1024),
        name='lars_comm',
    )(lr, *grads, pooled, dlogits, *weights, *moments, *small)


NBUF = 12
AHEAD = 6
NFC = 4
WRITE_FLOPS = 10 ** 8
VMEM = 67043328


def write_kernel(o_ref, ns, no, ni, n0, nm, nf, so_ref, sv_ref, os_, oo, of, bs, bo, bf,
                 vs, vo, vi, v0, vm, vf, bn, vbn, wb, vb,
                 buf, bbuf, fbuf, fbbuf, vbuf, nbuf, across, line, flat, in_sem, f_sem, b_sem, v_sem, n_sem):
    def view(c, refs):
        entry, ref = [(e, r) for e, r in zip(TABLE, refs) if c >= e[0]][-1]
        i, row, col = unit_at(entry, c)
        return ref.at[i, :, pl.ds(row, U), pl.ds(col, CW)]

    def load(i):
        return [pltpu.make_async_copy(o_ref.at[i], buf.at[i % NBUF], in_sem.at[i % NBUF])]

    def stores(i):
        slot = i % NBUF
        if not FC0 <= i <= FCL:
            pairs = [(buf.at[slot], view(i, (os_, oo))), (bbuf.at[slot], view(i, (bs, bo)))]
        else:
            size = min(LANES, CLASSES - LANES * (i - FC0))
            have, want = pl.ds(0, size), pl.ds(LANES * (i - FC0), size)
            pairs = [(fbuf.at[i % NFC, have], of.at[want]), (fbbuf.at[i % NFC, have], bf.at[want])]
        return [pltpu.make_async_copy(*pairs[0], f_sem.at[slot]), pltpu.make_async_copy(*pairs[1], b_sem.at[slot])]

    done = []

    def settle(upto):
        while len(done) <= upto:
            for d in stores(len(done)):
                d.wait()
            done.append(True)

    for i in range(AHEAD):
        for d in load(i):
            d.start()
    sizes = [e[1] * e[2] * LANES for e in TABLE]
    firsts = [sum(sizes[:n]) for n in range(len(sizes))]

    def moments(refs, back):
        out = []
        for first, ref in zip(firsts, refs):
            pair = (ref, vbuf.at[pl.ds(first, ref.shape[0])])
            out.append(pltpu.make_async_copy(*(pair[::-1] if back else pair), v_sem))
        return out

    v_ins, v_outs = moments((ns, no, ni, n0, nm), False), moments((vs, vo, vi, v0, vm), True)
    for d in v_ins:
        d.start()
    nf_in = pltpu.make_async_copy(nf, nbuf.at[pl.ds(0, CLASSES)], n_sem)
    nf_in.start()
    nf_out = pltpu.make_async_copy(flat, vf, n_sem)

    def flatten_fc():
        period = 2 * SUB
        rows_per = CLASSES * period // LANES
        nbuf[CLASSES:, :] = jnp.zeros((SUB * LANES - CLASSES, LANES), F32)
        across[SUB] = jnp.zeros((LANES, LANES), F32)
        for b in range(SUB):
            across[b] = nbuf[b * LANES:(b + 1) * LANES, :].T
        live = {}
        for r in range(period):
            first, shift = divmod(CLASSES * r, LANES)
            x = [across[b, pl.ds(r, SUB, stride=period), :] for b in range(SUB + 1)]
            y = pltpu.roll(jnp.concatenate(x, axis=1), shift, 1)
            for b in range(SUB + 1):
                part = y[:, b * LANES:(b + 1) * LANES]
                if first + b < rows_per:
                    live[first + b] = live[first + b] + part if first + b in live else part
            after = CLASSES * (r + 1) // LANES
            for row in [k for k in live if k < after]:
                flat[pl.ds(row, SUB, stride=rows_per), :] = live.pop(row)

    width = vb.shape[1]
    for i in range(SUB):
        line[:, i * LANES:(i + 1) * LANES] = jnp.broadcast_to(sv_ref[SUB + i:SUB + i + 1, :], (SUB, LANES))
    spread = (SUB * LANES, width)
    chosen = (lax.broadcasted_iota(jnp.int32, spread, 1) + lax.axis_index('dp') * width
              == lax.broadcasted_iota(jnp.int32, spread, 0))
    own = jnp.dot(line[...], jnp.where(chosen, 1.0, 0.0), precision=lax.Precision.HIGHEST, preferred_element_type=F32)
    vb[...] = own[0:1]
    bn[...] = so_ref[...]
    vbn[...] = sv_ref[0:SUB]
    for i in range(SUB):
        lanes = slice(i * LANES, min(CLASSES, (i + 1) * LANES))
        wb[:, lanes] = sv_ref[2 * SUB + i:2 * SUB + i + 1, :lanes.stop - lanes.start]
    for i in range(TAIL0):
        slot = i % NBUF
        for d in load(i):
            d.wait()
        if not FC0 <= i <= FCL:
            def cast(p, _):
                bbuf[slot, p] = buf[slot, p].astype(BF16)
                return 0

            lax.fori_loop(0, DEV, cast, 0)
        else:
            settle(i - NFC)
            for p in range(DEV):
                for r in range(CW // LANES):
                    x = buf[slot, p, :, LANES * r:LANES * (r + 1)]
                    at = (slice(U * r, U * (r + 1)), slice(LANES * p, LANES * (p + 1)))
                    fbuf[(i % NFC,) + at] = x
                    fbbuf[(i % NFC,) + at] = x.astype(BF16)
        for d in stores(i):
            d.start()
        if i == AHEAD:
            for d in v_ins:
                d.wait()
            for d in v_outs:
                d.start()
            nf_in.wait()
            flatten_fc()
            nf_out.start()
        if i + AHEAD < TAIL0:
            settle(i + AHEAD - NBUF)
            for d in load(i + AHEAD):
                d.start()
    settle(TAIL0 - 1)
    nf_out.wait()
    for d in v_outs:
        d.wait()


def run_write(o, moments_new, so, sv, width):
    anyspec = pl.BlockSpec(memory_space=pl.ANY)
    vspec = pl.BlockSpec(memory_space=pltpu.VMEM)
    shapes = [dshape(*e, DEV) for e in TABLE[:2]] + [(CLASSES, DEV * LANES)]
    moments = [(e[1] * e[2] * LANES, LANES) for e in TABLE] + [(CLASSES, LANES)]
    tile = (SUB, LANES)
    dma = pltpu.SemaphoreType.DMA
    outs = [(s, F32) for s in shapes] + [(s, BF16) for s in shapes] + [(s, F32) for s in moments]
    outs += [((DEV,) + tile, F32), (tile, F32), ((1, CLASSES), F32), ((1, width), F32)]
    return pl.pallas_call(
        write_kernel,
        out_shape=[jax.ShapeDtypeStruct(*s) for s in outs],
        in_specs=[anyspec] * 7 + [vspec] * 2,
        out_specs=[anyspec] * 12 + [vspec] * 4,
        scratch_shapes=[
            pltpu.VMEM((NBUF, DEV, U, CW), F32), pltpu.VMEM((NBUF, DEV, U, CW), BF16),
            pltpu.VMEM((NFC, LANES, DEV * LANES), F32), pltpu.VMEM((NFC, LANES, DEV * LANES), BF16),
            pltpu.VMEM(((NCH - FCN) * LANES, LANES), F32), pltpu.VMEM((SUB * LANES, LANES), F32),
            pltpu.VMEM((SUB + 1, LANES, LANES), F32), pltpu.VMEM((SUB, SUB * LANES), F32),
            pltpu.VMEM((CLASSES, LANES), F32), dma((NBUF,)), dma((NBUF,)), dma((NBUF,)), dma, dma],
        compiler_params=pltpu.CompilerParams(vmem_limit_bytes=VMEM),
        cost_estimate=pl.CostEstimate(flops=WRITE_FLOPS, bytes_accessed=TAIL0 * 160 * U * CW, transcendentals=0),
        name='write_out',
    )(o, *moments_new, so, sv)


TBUF, TAHEAD = 16, 10


def tail_kernel(jobs, size, count, aliased, *refs):
    srcs, refs = refs[:count], refs[count + 7 * aliased:]
    fulls, halves, (token, buf, bbuf, in_sem, f_sem, b_sem) = refs[:3], refs[3:6], refs[6:]
    me = lax.axis_index('dp')
    mate = 1 - 2 * (me % 2)
    ring = buf.shape[0]
    token[...] = jnp.zeros_like(token)

    def load(n):
        return [pltpu.make_async_copy(srcs[src].at[k], buf.at[n % ring, pl.ds(4 * j, 4)], in_sem.at[n % ring])
                for j, (src, k, _, _) in enumerate(jobs[n][1])]

    def store(n):
        slot = n % ring
        c, parts = jobs[n]
        e = devices(me, strides(me // 2, c % 3))
        entry, full, half = [x for x in zip(TABLE[2:], fulls, halves) if c >= x[0][0]][-1]
        i, row, _ = unit_at(entry, c)
        for j, (_, _, base, other) in enumerate(parts):
            for q in range(4):
                p = e[base + q] + mate * other
                at = (i, p, pl.ds(row, U))
                pltpu.make_async_copy(buf.at[slot, 4 * j + q], full.at[at], f_sem.at[slot]).start()
                pltpu.make_async_copy(bbuf.at[slot, 4 * j + q], half.at[at], b_sem.at[slot]).start()

    def settled(n):
        for ref, sem in ((buf, f_sem), (bbuf, b_sem)):
            pltpu.make_async_copy(ref.at[n % ring], ref.at[n % ring], sem.at[n % ring]).wait()

    total = len(jobs)
    ahead = ring if ring == total else TAHEAD
    for n in range(ahead):
        for d in load(n):
            d.start()
    for n in range(total):
        slot = n % ring
        for d in load(n):
            d.wait()

        def cast(p, _):
            bbuf[slot, p] = buf[slot, p].astype(BF16)
            return 0

        lax.fori_loop(0, size, cast, 0)
        store(n)
        nxt = n + ahead
        if nxt < total:
            if nxt >= ring:
                settled(nxt - ring)
            for d in load(nxt):
                d.start()
    for n in range(max(0, total - ring), total):
        settled(n)


def run_tail(groups, sets, arrays):
    anyspec = pl.BlockSpec(memory_space=pl.ANY)
    dma = pltpu.SemaphoreType.DMA
    size = 4 * len(sets)
    srcs, jobs = [], []
    for g in groups:
        base = len(srcs)
        for arrs, _, _ in sets:
            srcs += arrs[3 * g:3 * g + 3]
        for n in range(GROUP):
            jobs.append((TAIL0 + g * GROUP + n, [(base + 3 * j + n % 3, n // 3, first, other)
                                                 for j, (_, first, other) in enumerate(sets)]))
    ring = min(len(jobs), TBUF)
    count = len(srcs)
    given = list(arrays or [])[:6]
    tokens = list(arrays or [])[6:]
    shapes = [dshape(*e, DEV) for e in TABLE[2:]]
    outs = [jax.ShapeDtypeStruct(s, t) for t in (F32, BF16) for s in shapes]
    return pl.pallas_call(
        functools.partial(tail_kernel, jobs, size, count, len(given) > 0),
        out_shape=outs + [jax.ShapeDtypeStruct((SUB, LANES), F32)],
        in_specs=[anyspec] * (count + len(given) + len(tokens)),
        out_specs=[anyspec] * 6 + [pl.BlockSpec(memory_space=pltpu.VMEM)],
        input_output_aliases={count + n: n for n in range(len(given))},
        scratch_shapes=[pltpu.VMEM((ring, size, U, CW), F32), pltpu.VMEM((ring, size, U, CW), BF16),
                        dma((ring,)), dma((ring,)), dma((ring,))],
        compiler_params=pltpu.CompilerParams(vmem_limit_bytes=VMEM),
        cost_estimate=pl.CostEstimate(flops=WRITE_FLOPS // 3, bytes_accessed=len(jobs) * size * 10 * U * CW,
                                      transcendentals=0),
    )(*srcs, *given, *tokens)


def solution(mesh):
    n_dev = mesh.shape['dp']
    assert n_dev == DEV
    full, lead, cols = P(), P('dp'), P(None, 'dp')
    moment_specs = (lead, lead, cols, cols, cols, lead, lead, lead)
    in_specs = (full,) * 8 + (lead,) * 8 + moment_specs + (full,)
    out_specs = (full,) * 14 + moment_specs

    def body(w_in0, w_short, w_in, w_mid, w_out, w_fc, w_bn, w_bias,
             g_in0, g_short, g_in, g_mid, g_out, g_bn, pooled, dlogits,
             v_in0, v_short, v_in, v_mid, v_out, v_fc, v_bn, v_bias, learn_rate):
        width = v_bias.shape[0]
        shapes = [dshape(*e, DEV) for e in TABLE]
        grads = [g.reshape(s) for g, s in zip((g_short, g_out, g_in, g_in0, g_mid), shapes)]
        weights = [w.reshape(s) for w, s in zip((w_short, w_out, w_in, w_in0, w_mid), shapes)] + [w_fc.T]

        def to_rows(v, entry):
            _, stack, _, blocks = entry
            return v.reshape(stack, -1, LANES).transpose(1, 0, 2).reshape(-1, blocks * CW // LANES, stack, 1, LANES)

        def from_rows(v, stack, like):
            return v.reshape(-1, stack, LANES).transpose(1, 0, 2).reshape(like.shape)

        olds = (v_short, v_out, v_in, v_in0, v_mid)
        moments = [to_rows(v, e) for v, e in zip(olds, TABLE)]
        moments.append(v_fc.reshape(LANES, CLASSES).T)
        tiles = (-1, SUB, LANES)
        small = [g_bn.reshape(tiles), w_bn.reshape(-1, LANES), v_bn.reshape(SUB, LANES),
                 w_bias.reshape(1, CLASSES), v_bias.reshape(1, width)]
        o, *made, so, sv = run_comm(
            learn_rate.reshape(1, 1), grads, pooled, dlogits.T, weights, moments, small)
        ts, us, made = made[:6], made[6:12], made[12:]

        def across(x, weight):
            return lax.ppermute(x, 'dp', [(i, i ^ weight) for i in range(DEV)])

        def to_mates(arrs, token):
            *held, token = lax.optimization_barrier((*arrs, token))
            return [across(r, 1) for r in held], token

        rs = []
        for n, t in enumerate(ts):
            rs.append(across(t, 2 << (n + 2) % 3))
        outs = run_write(o, [v.reshape(-1, LANES) for v in made], so, sv, width)
        short, out, fc, short_b, out_b, fc_b, vs, vo, vi, v0, vm, vf, bn, vbn, wb, vb = outs
        mates, vbn = to_mates(rs[:3], vbn)
        tail = run_tail((0, 1), [(ts, 0, False), (us, 0, True)], None)
        *tail, token = run_tail((0,), [(rs, 4, False), (mates, 4, True)], tail)
        last, token = to_mates(rs[3:], token)
        tail = run_tail((1,), [(rs, 4, False)], (*tail, token))
        *tail, _ = run_tail((1,), [(mates + last, 4, True)], tail)
        inn, in0, mid, inn_b, in0_b, mid_b = tail
        news = [from_rows(v, e[1], old) for v, e, old in zip((vs, vo, vi, v0, vm), TABLE, olds)]
        return (in0.reshape(w_in0.shape), short.reshape(w_short.shape), inn.reshape(w_in.shape),
                mid.reshape(w_mid.shape), out.reshape(w_out.shape), fc.T,
                bn.reshape(w_bn.shape), wb.reshape(w_bias.shape),
                in0_b.reshape(w_in0.shape), short_b.reshape(w_short.shape), inn_b.reshape(w_in.shape),
                mid_b.reshape(w_mid.shape), out_b.reshape(w_out.shape), fc_b.T,
                news[3], news[0], news[2], news[4], news[1], vf.reshape(v_fc.shape),
                vbn.reshape(v_bn.shape), vb.reshape(v_bias.shape))

    return jax.shard_map(body, mesh=mesh, in_specs=in_specs, out_specs=out_specs, check_vma=False)
```
